32 devices in a mesh: section: 4 (over y, x), pix: 8 (over z, core).
Axes of the slice: x: 2, y: 2, z: 4, core: 2. Of those that a mesh axis runs over, the one named last changes fastest.
Arguments:
- slc: float32 [2, 200, 2048], P(None, 'section', 'pix'), may hold values from -6 to 6
- neighbours: int32 [15, 2048], P(None, 'pix'), may hold values from 0 to 2047, as said below
- reference_pixel: int32 [1], replicated, may hold values from 0 to 2047
Outputs:
- phases: float32 [2, 200, 2048], P(None, 'section', 'pix')
- compressed: float32 [2, 4, 2048], P(None, 'section', 'pix')
The draws below stay inside these ranges and needn't reach their ends.
Inputs may be any that keep to these rules, and one draw needn't show every extreme that they name: neighbours[0, p] = p; every entry lies within 256 of its column's pixel p, and that distance is reached.
All inputs are finite; a program needn't handle non-finite values.
Results may differ from the reference program's by a relative error of at most 0.0003.
Values sent between devices are 32-bit elements; how exact they have to be, the bound alone decides.
No kernel may reach another device: no remote copies, remote signals or barrier semaphores. Data moves between devices by JAX's collectives and lax.ppermute only.
A program may use at most 64 MiB of HBM per device.

```python
import math
import jax
import jax.numpy as jnp
from jax import lax

M = 50
NEIGHBOURS = 15
ITERS = 16
STACK = 51
DATES = 200
PIXELS = 2048
REACH = 256
N_SECTION = 4


def draw_neighbours(key, part):
    offsets = jax.random.randint(key, (NEIGHBOURS, PIXELS), -REACH, REACH + 1)
    offsets = offsets.at[0].set(0)
    middle = PIXELS // 2
    offsets = offsets.at[1, middle].set(REACH)
    offsets = offsets.at[1, middle + 1].set(-REACH)
    places = jnp.arange(PIXELS, dtype=jnp.int32)[None, :]
    return jnp.clip(places + offsets, 0, PIXELS - 1).astype(jnp.int32)


def levels(stream_key, extent, cuts, least, largest):
    factor_of, own = 1.0, jax.random.fold_in(stream_key, 6)
    for axis_at, shards_of in cuts:
        heights = jnp.exp(jax.random.uniform(jax.random.fold_in(own, axis_at), (shards_of,), jnp.float32, least / len(cuts), largest / len(cuts)))
        factor_of = factor_of * jnp.repeat(heights, extent[axis_at] // shards_of).reshape([-1 if axis == axis_at else 1 for axis in range(len(extent))])
    return factor_of


def noise(stream_key, extent, spread, bound, split=(), kind=jnp.bfloat16):
    values = jax.random.normal(stream_key, extent, jnp.float32) * spread
    if len(split) > 0:
        values = levels(stream_key, extent, split, -0.22, 0.18) * values
    return jnp.clip(values, min=-bound, max=bound).astype(kind)


def setup_inputs(seed: int = 0) -> dict:
    key_list = jax.random.split(jax.random.key(seed), 4)
    return {
        "slc": noise(key_list[0], (2, DATES, PIXELS), 1.0, 6.0, ((1, 4), (2, 8)), jnp.float32),
        "neighbours": draw_neighbours(jax.random.fold_in(key_list[3], 71), 0),
        "reference_pixel": jax.random.randint(key_list[2], (1,), 0, PIXELS).astype(jnp.int32),
    }


FLOOR = 0.05

def unit(real, imag):
    scale = 1.0 / jnp.maximum(jnp.sqrt(real * real + imag * imag), FLOOR)
    return (real * scale, imag * scale)

def solve_block(ext_re, ext_im, index, own_re, own_im):
    near_re = ext_re[:, index]
    near_im = ext_im[:, index]
    power = lax.optimization_barrier(jnp.sum(near_re * near_re + near_im * near_im, axis=1))
    scale = 1.0 / jnp.sqrt(jnp.maximum(power, 1.0))
    z_re = near_re * scale[:, None, :]
    z_im = near_im * scale[:, None, :]
    count = own_re.shape[0]
    start_re = jnp.full(own_re.shape, 1.0 / math.sqrt(count), jnp.float32)
    start_im = jnp.zeros(own_re.shape, jnp.float32)

    def turn(step, carry):
        vec_re, vec_im = carry
        c_re = lax.optimization_barrier(jnp.sum(z_re * vec_re[:, None, :] + z_im * vec_im[:, None, :], axis=0))
        c_im = lax.optimization_barrier(jnp.sum(z_re * vec_im[:, None, :] - z_im * vec_re[:, None, :], axis=0))
        u_re = vec_re + lax.optimization_barrier(jnp.sum(z_re * c_re[None] - z_im * c_im[None], axis=1))
        u_im = vec_im + lax.optimization_barrier(jnp.sum(z_re * c_im[None] + z_im * c_re[None], axis=1))
        norm = jnp.sqrt(lax.optimization_barrier(jnp.sum(u_re * u_re + u_im * u_im, axis=0)))
        return (u_re / norm, u_im / norm)
    vec_re, vec_im = lax.fori_loop(0, ITERS, turn, (start_re, start_im))
    comp_re = lax.optimization_barrier(jnp.sum(vec_re * own_re + vec_im * own_im, axis=0))
    comp_im = lax.optimization_barrier(jnp.sum(vec_re * own_im - vec_im * own_re, axis=0))
    return (vec_re, vec_im, comp_re, comp_im)

def reference(slc, neighbours, reference_pixel):
    width = math.gcd(PIXELS, 2048)
    blocks = PIXELS // width
    virtual = jnp.zeros((2, PIXELS), jnp.float32)
    vectors = []
    packed = []
    for section in range(N_SECTION):
        stack = jnp.concatenate([virtual[:, None, :], slc[:, section * M:(section + 1) * M, :]], axis=1)

        def one(block):
            start = (block * width).astype(jnp.int32)
            index = lax.dynamic_slice_in_dim(neighbours, start, width, 1)
            own = lax.dynamic_slice_in_dim(stack, start, width, 2)
            return solve_block(stack[0], stack[1], index, own[0], own[1])
        vr, vi, cr, ci = lax.map(one, jnp.arange(blocks, dtype=jnp.int32))
        vec_re = jnp.transpose(vr, (1, 0, 2)).reshape(STACK, PIXELS)
        vec_im = jnp.transpose(vi, (1, 0, 2)).reshape(STACK, PIXELS)
        virtual = jnp.stack([cr.reshape(PIXELS), ci.reshape(PIXELS)])
        vectors.append((vec_re, vec_im))
        packed.append(virtual)
    datum_re = jnp.ones((PIXELS,), jnp.float32)
    datum_im = jnp.zeros((PIXELS,), jnp.float32)
    pieces = [None] * N_SECTION
    for section in range(N_SECTION - 1, -1, -1):
        vec_re, vec_im = vectors[section]
        s_re = vec_re[1:] * datum_re - vec_im[1:] * datum_im
        s_im = vec_re[1:] * datum_im + vec_im[1:] * datum_re
        pieces[section] = (s_re, s_im)
        f_re, f_im = unit(vec_re[0], vec_im[0])
        datum_re, datum_im = (datum_re * f_re - datum_im * f_im, datum_re * f_im + datum_im * f_re)
    series_re = jnp.concatenate([p[0] for p in pieces], axis=0)
    series_im = jnp.concatenate([p[1] for p in pieces], axis=0)
    ref_re = lax.dynamic_index_in_dim(series_re, reference_pixel[0], 1, False)
    ref_im = lax.dynamic_index_in_dim(series_im, reference_pixel[0], 1, False)
    u_re, u_im = unit(ref_re, ref_im)
    gain = math.sqrt(STACK)
    out_re = gain * (series_re * u_re[:, None] + series_im * u_im[:, None])
    out_im = gain * (series_im * u_re[:, None] - series_re * u_im[:, None])
    return (jnp.stack([out_re, out_im]), jnp.stack(packed, axis=1))
```

```python
import functools
import math

import jax
import jax.numpy as jnp
from jax import lax
from jax.experimental import pallas as pl
from jax.experimental.pallas import tpu as pltpu
from jax.sharding import PartitionSpec as P

ITERS = 16
FLOOR = 0.05
REACH_LIMIT = 256
LANES = 128
SUB = 8
KP = 16
SHRINK = 2.0**-35

SMEM = pl.BlockSpec(memory_space=pltpu.SMEM)
VMEM = pl.BlockSpec(memory_space=pltpu.VMEM)


def f32(*shape):
    return jax.ShapeDtypeStruct(shape, jnp.float32)


def params():
    return pltpu.CompilerParams(vmem_limit_bytes=20 * 1024 * 1024)


def up(n, m):
    return -(-n // m) * m


def colsum(x):
    return jnp.sum(x, axis=0, keepdims=True)


def unit(real, imag):
    scale = 1.0 / jnp.maximum(jnp.sqrt(real * real + imag * imag), FLOOR)
    return (real * scale, imag * scale)


def half(h):
    return pl.ds(h * LANES, LANES)


def gather(base, idx_ref, pieces, xs_ref, hl_ref, zr_ref, zi_ref):
    count, rows, pixels = zr_ref.shape
    dates = pieces[0].shape[1]
    xs_ref[...] = jnp.zeros_like(xs_ref)
    at = 0
    for piece in pieces:
        width = piece.shape[2]
        for c in range(2):
            xs_ref[pl.ds(c * rows, dates), pl.ds(at, width)] = piece[c]
        at += width
    high = xs_ref[...].astype(jnp.bfloat16)
    hl_ref[0 : 2 * rows] = high
    hl_ref[2 * rows : 4 * rows] = (xs_ref[...] - high.astype(jnp.float32)).astype(jnp.bfloat16)
    window = xs_ref.shape[1]
    place = lax.broadcasted_iota(jnp.int32, (window, pixels), 0)
    for k in range(count):
        near = idx_ref[k : k + 1, :] - base
        hot = jnp.where(place == near, 1.0, 0.0).astype(jnp.bfloat16)
        got = jnp.dot(hl_ref[...], hot, preferred_element_type=jnp.float32)
        zr_ref[k] = got[0:rows] + got[2 * rows : 3 * rows]
        zi_ref[k] = got[rows : 2 * rows] + got[3 * rows : 4 * rows]


def scale_dates(zr_ref, zi_ref):
    count, rows, pixels = zr_ref.shape
    for h in range(pixels // LANES):
        for r in range(0, rows, SUB):
            power = None
            for k in range(count):
                a = zr_ref[k, pl.ds(r, SUB), half(h)]
                b = zi_ref[k, pl.ds(r, SUB), half(h)]
                power = a * a + b * b if power is None else power + (a * a + b * b)
            scale = lax.rsqrt(jnp.maximum(power, 1.0))
            for k in range(count):
                zr_ref[k, pl.ds(r, SUB), half(h)] *= scale
                zi_ref[k, pl.ds(r, SUB), half(h)] *= scale


def merge_rows(parts):
    row = lax.broadcasted_iota(jnp.int32, (SUB, LANES), 0)
    for step in (4, 2, 1):
        low = jnp.bitwise_and(row, step) == 0
        n = len(parts) // 2
        out = []
        for i in range(n):
            a, b = parts[i], parts[i + n]
            far = jnp.where(low, pltpu.roll(a, SUB - step, 0), pltpu.roll(b, step, 0))
            out.append(jnp.where(low, a, b) + far)
        parts = out
    return parts[0]


def gram(pair_ref, zr_ref, zi_ref, xs_ref, own_at, gr_ref, gi_ref, sum_ref, block=3):
    count, rows, pixels = zr_ref.shape
    zero = jnp.zeros((SUB, LANES), jnp.float32)
    for h in range(pixels // LANES):
        here = pl.ds(own_at + h * LANES, LANES)

        def load(k, r):
            if k == count:
                return (xs_ref[pl.ds(r, SUB), here], xs_ref[pl.ds(rows + r, SUB), here])
            return (zr_ref[k, pl.ds(r, SUB), half(h)], zi_ref[k, pl.ds(r, SUB), half(h)])

        for k0 in range(0, count, block):
            for l0 in range(k0, count + 1, block):
                pairs = [
                    (k, l)
                    for k in range(k0, min(k0 + block, count))
                    for l in range(l0, min(l0 + block, count + 1))
                    if l >= k
                ]
                acc = {}
                for r in range(0, rows, SUB):
                    val = {n: load(n, r) for n in sorted({n for p in pairs for n in p})}
                    for k, l in pairs:
                        ar, ai = val[k]
                        br, bi = val[l]
                        re = ar * br + ai * bi
                        im = None if k == l else ar * bi - ai * br
                        if r:
                            re = acc[k, l][0] + re
                            im = None if k == l else acc[k, l][1] + im
                        acc[k, l] = (re, im)
                for k, l in pairs:
                    pair_ref[0, l, k] = acc[k, l][0]
                    pair_ref[1, l, k] = zero if k == l else acc[k, l][1]
        for c, g_ref in ((0, gr_ref), (1, gi_ref)):
            for l in range(count + 1):
                for kt in range(KP // SUB):
                    ks = range(kt * SUB, kt * SUB + SUB)
                    if min(ks) > min(l, count - 1):
                        continue
                    parts = [pair_ref[c, l, k] if k <= min(l, count - 1) else zero for k in ks]
                    g_ref[l, h, pl.ds(kt * SUB, SUB), :] = merge_rows(parts)
        row = lax.broadcasted_iota(jnp.int32, (SUB, LANES), 0)
        for c, g_ref in ((0, gr_ref), (1, gi_ref)):
            for l in range(count):
                for kt in range(KP // SUB):
                    ks = list(range(kt * SUB, kt * SUB + SUB))
                    if max(ks) <= l:
                        continue
                    other = jnp.concatenate(
                        [g_ref[k, h, pl.ds(l, 1), :] if l < k < count else zero[0:1] for k in ks], axis=0
                    )
                    if c:
                        other = -other
                    if min(ks) <= l:
                        other = jnp.where(row + ks[0] <= l, g_ref[l, h, pl.ds(kt * SUB, SUB), :], other)
                    g_ref[l, h, pl.ds(kt * SUB, SUB), :] = other
        for c in range(2):
            tiles = []
            for k in range(KP):
                total = None
                if k <= count:
                    for r in range(0, rows, SUB):
                        v = load(k, r)[c]
                        total = v if total is None else total + v
                tiles.append(zero if total is None else total)
            for kt in range(KP // SUB):
                sum_ref[c, h, pl.ds(kt * SUB, SUB), :] = merge_rows(tiles[kt * SUB : kt * SUB + SUB])


def turns(gr_ref, gi_ref, g0, count):
    halves = gr_ref.shape[1]

    def product(b, g):
        acc = [list(x) for x in g]
        for l in range(count):
            for h in range(halves):
                br = jnp.broadcast_to(b[h][0][l : l + 1], (KP, LANES))
                bi = jnp.broadcast_to(b[h][1][l : l + 1], (KP, LANES))
                gr = gr_ref[l, h]
                gi = gi_ref[l, h]
                acc[h][0] = acc[h][0] + (gr * br - gi * bi)
                acc[h][1] = acc[h][1] + (gr * bi + gi * br)
        return acc

    def step(_, carry):
        b, g = carry
        t = product(b, g)
        return tuple((b[h][0] + t[h][0], b[h][1] + t[h][1]) for h in range(halves)), g

    g = tuple(g0)
    b = g
    b, g = lax.fori_loop(0, ITERS // 2 - 1, step, (b, g))
    b = tuple((x * SHRINK, y * SHRINK) for x, y in b)
    g = tuple((x * SHRINK, y * SHRINK) for x, y in g)
    b, g = lax.fori_loop(0, ITERS - ITERS // 2, step, (b, g))
    return b, g, product(b, g)


def solve(virtual, gr_ref, gi_ref, hr, hi, sum_ref, stack, beta_ref, state_ref):
    halves = gr_ref.shape[1]
    count = gr_ref.shape[0]
    first = 1.0 / math.sqrt(stack)
    g0 = []
    for h in range(halves):
        zr, zi = sum_ref[0, h], sum_ref[1, h]
        row = lax.broadcasted_iota(jnp.int32, (KP, LANES), 0)
        zr = jnp.where(row < count, zr, 0.0)
        zi = jnp.where(row < count, zi, 0.0)
        if virtual is not None:
            zr = zr + virtual[h][1][0]
            zi = zi + virtual[h][1][1]
        g0.append((zr * first, zi * -first))
    b, g, t = turns(gr_ref, gi_ref, g0, count)
    for h in range(halves):
        norm = colsum(b[h][0] * (g[h][0] + t[h][0]) + b[h][1] * (g[h][1] + t[h][1]))
        inv = lax.rsqrt(SHRINK * SHRINK + norm)
        br, bi = b[h][0] * inv, b[h][1] * inv
        a = inv * (SHRINK * first)
        xr, xi = hr[h], hi[h]
        sr, si = sum_ref[0, h][count : count + 1], sum_ref[1, h][count : count + 1]
        fr, fi = a, jnp.zeros_like(a)
        if virtual is not None:
            (wr, wi), (zr, zi) = virtual[h]
            xr, xi = xr + (zr * wr + zi * wi), xi + (zr * wi - zi * wr)
            sr, si = sr + wr, si + wi
            fr = a + colsum(zr * br - zi * bi)
            fi = colsum(zr * bi + zi * br)
        beta_ref[0, h] = br
        beta_ref[1, h] = bi
        fr, fi = unit(fr, fi)
        state_ref[0:1, half(h)] = a * sr + colsum(br * xr + bi * xi)
        state_ref[1:2, half(h)] = a * si + colsum(br * xi - bi * xr)
        state_ref[2:3, half(h)] = fr
        state_ref[3:4, half(h)] = fi
        state_ref[4:5, half(h)] = a
        state_ref[5:8, half(h)] = jnp.zeros((3, LANES), jnp.float32)


def prepare_kernel(
    stack, base_ref, idx_ref, low_ref, own_ref, high_ref,
    zr_ref, zi_ref, gr_ref, gi_ref, sum_ref, beta_ref, state_ref, comp_ref,
    xs_ref, hl_ref, pair_ref,
):
    gather(base_ref[0], idx_ref, (low_ref, own_ref, high_ref), xs_ref, hl_ref, zr_ref, zi_ref)
    scale_dates(zr_ref, zi_ref)
    gram(pair_ref, zr_ref, zi_ref, xs_ref, low_ref.shape[2], gr_ref, gi_ref, sum_ref)
    count = zr_ref.shape[0]
    halves = gr_ref.shape[1]
    hr = [gr_ref[count, h] for h in range(halves)]
    hi = [gi_ref[count, h] for h in range(halves)]
    solve(None, gr_ref.at[0:count], gi_ref.at[0:count], hr, hi, sum_ref, stack, beta_ref, state_ref)
    comp_ref[...] = state_ref[0:2]


def lane_take(x, i):
    return jnp.take_along_axis(x, i, axis=1, mode="promise_in_bounds")


def round_kernel(
    rnd, stack, where_ref, idx_ref, low_ref, own_ref, high_ref,
    gr_ref, gi_ref, sum_ref, beta0_ref, state0_ref,
    beta_ref, state_ref, comp_ref, fr_ref, fi_ref,
):
    count = gr_ref.shape[0] - 1
    halves = gr_ref.shape[1]
    reach = low_ref.shape[1]
    beta_ref[...] = beta0_ref[...]
    state_ref[...] = state0_ref[...]

    @pl.when(where_ref[1] == rnd)
    def _():
        tiles = []
        for ref in (low_ref, own_ref, high_ref):
            for t in range(ref.shape[1] // LANES):
                tiles.append([ref[c : c + 1, half(t)] for c in range(2)])
        virtual = []
        for h in range(halves):
            parts = []
            for kt in range(KP // SUB):
                rows = min(SUB, count - kt * SUB)
                raw = idx_ref[pl.ds(kt * SUB, rows), half(h)] - where_ref[0]
                if rows < SUB:
                    raw = jnp.concatenate([raw, jnp.full((SUB - rows, LANES), -1, jnp.int32)], axis=0)
                lane = jnp.bitwise_and(raw, LANES - 1)
                tile = jnp.right_shift(raw, 7)
                both = []
                for c in range(2):
                    out = jnp.zeros((SUB, LANES), jnp.float32)
                    for n in range(h, h + 2 * reach // LANES + 1):
                        got = lane_take(jnp.broadcast_to(tiles[n][c], (SUB, LANES)), lane)
                        out = jnp.where(tile == n, got, out)
                    both.append(out)
                parts.append(both)
            zr = jnp.concatenate([p[0] for p in parts], axis=0)
            zi = jnp.concatenate([p[1] for p in parts], axis=0)
            scale = lax.rsqrt(jnp.maximum(colsum(zr * zr + zi * zi), 1.0))
            zr, zi = zr * scale, zi * scale
            own = tiles[reach // LANES + h]
            virtual.append((own, (zr, zi)))
            for l in range(count):
                br = jnp.broadcast_to(zr[l : l + 1], (KP, LANES))
                bi = jnp.broadcast_to(zi[l : l + 1], (KP, LANES))
                fr_ref[l, h] = gr_ref[l, h] + (zr * br + zi * bi)
                fi_ref[l, h] = gi_ref[l, h] + (zr * bi - zi * br)
        hr = [gr_ref[count, h] for h in range(halves)]
        hi = [gi_ref[count, h] for h in range(halves)]
        solve(virtual, fr_ref, fi_ref, hr, hi, sum_ref, stack, beta_ref, state_ref)

    comp_ref[...] = state_ref[0:2]


def vector_kernel(at_ref, zr_ref, zi_ref, beta_ref, state_ref, vec_ref, slot_ref, turned_ref):
    count, rows, pixels = zr_ref.shape
    dates = vec_ref.shape[1]
    local = at_ref[2]
    for h in range(pixels // LANES):
        a = state_ref[4:5, half(h)]
        acc_r = [jnp.broadcast_to(a, (SUB, LANES)) for _ in range(0, rows, SUB)]
        acc_i = [jnp.zeros((SUB, LANES), jnp.float32) for _ in range(0, rows, SUB)]
        for k in range(count):
            br = jnp.broadcast_to(beta_ref[0, h, k : k + 1, :], (SUB, LANES))
            bi = jnp.broadcast_to(beta_ref[1, h, k : k + 1, :], (SUB, LANES))
            for n, r in enumerate(range(0, rows, SUB)):
                zr = zr_ref[k, pl.ds(r, SUB), half(h)]
                zi = zi_ref[k, pl.ds(r, SUB), half(h)]
                acc_r[n] = acc_r[n] + (zr * br - zi * bi)
                acc_i[n] = acc_i[n] + (zr * bi + zi * br)
        for c, acc in ((0, acc_r), (1, acc_i)):
            whole = jnp.concatenate(acc, axis=0)
            vec_ref[c, :, half(h)] = whole[0:dates]
            wide = jnp.concatenate([whole, jnp.zeros((up(rows, LANES) - rows, LANES), jnp.float32)], axis=0)
            turned_ref[c, half(h)] = jnp.transpose(wide)
    slot_ref[...] = jnp.zeros_like(slot_ref)
    lane = lax.broadcasted_iota(jnp.int32, (1, LANES), 1)
    halves = pixels // LANES
    for c in range(2):
        for h in range(halves):
            slot_ref[c * halves + h : c * halves + h + 1] = state_ref[2 + c : 3 + c, half(h)]
        slot_ref[2 * halves + c : 2 * halves + c + 1] = turned_ref[c, pl.ds(local, 1), :]
        picked = jnp.zeros((1, LANES), jnp.float32)
        for h in range(halves):
            picked = picked + jnp.where(lane == local - h * LANES, state_ref[2 + c : 3 + c, half(h)], 0.0)
        slot_ref[2 * halves + 2 + c : 2 * halves + 3 + c] = jnp.broadcast_to(
            jnp.sum(picked, axis=1, keepdims=True), (1, LANES)
        )


def finish_kernel(sections, at_ref, vec_ref, got_ref, out_ref):
    dates, pixels = vec_ref.shape[1:]
    section, mine, root, blocks = at_ref[1], at_ref[3], at_ref[4], at_ref[5]
    halves = pixels // LANES
    one = jnp.ones((1, LANES), jnp.float32)
    datum = [(one, 0.0 * one) for _ in range(halves)]
    at_root = (one, 0.0 * one)
    for s in range(sections - 1, 0, -1):
        later = section < s
        own = got_ref[s * blocks + mine]
        ref = got_ref[s * blocks + root]

        def times(d, fr, fi):
            fr = jnp.where(later, fr, 1.0)
            fi = jnp.where(later, fi, 0.0)
            return (d[0] * fr - d[1] * fi, d[0] * fi + d[1] * fr)

        for h in range(halves):
            datum[h] = times(datum[h], own[h : h + 1], own[halves + h : halves + h + 1])
        at_root = times(at_root, ref[2 * halves + 2 : 2 * halves + 3], ref[2 * halves + 3 : 2 * halves + 4])
    ref = got_ref[section * blocks + root]
    vr, vi = ref[2 * halves : 2 * halves + 1], ref[2 * halves + 1 : 2 * halves + 2]
    ur, ui = unit(vr * at_root[0] - vi * at_root[1], vr * at_root[1] + vi * at_root[0])
    gain = math.sqrt(dates + 1)
    ur = jnp.transpose(jnp.broadcast_to(ur * gain, (LANES, LANES)))[0:dates]
    ui = jnp.transpose(jnp.broadcast_to(ui * gain, (LANES, LANES)))[0:dates]
    for h in range(halves):
        wr = ur * datum[h][0] + ui * datum[h][1]
        wi = ur * datum[h][1] - ui * datum[h][0]
        vr = vec_ref[0, :, half(h)]
        vi = vec_ref[1, :, half(h)]
        out_ref[0, :, half(h)] = vr * wr - vi * wi
        out_ref[1, :, half(h)] = vr * wi + vi * wr


def on_device(slc, neighbours, reference_pixel):
    dates, pixels = slc.shape[1:]
    count = neighbours.shape[0]
    reach = min(pixels, REACH_LIMIT)
    sections = lax.axis_size("section")
    blocks = lax.axis_size("pix")
    section = lax.axis_index("section")
    block = lax.axis_index("pix")
    stack = dates + 1
    halves = pixels // LANES
    rows = up(dates, SUB)
    window = pixels + 2 * reach
    base = block * pixels - reach

    forward = [(i, i + 1) for i in range(blocks - 1)]
    backward = [(i + 1, i) for i in range(blocks - 1)]
    low = lax.ppermute(slc[:, :, pixels - reach :], "pix", forward)
    high = lax.ppermute(slc[:, :, :reach], "pix", backward)

    root = reference_pixel[0] // pixels
    local = reference_pixel[0] - root * pixels
    at = jnp.stack([base, section, local, block, root, jnp.int32(blocks)]).astype(jnp.int32)

    zr, zi, gr, gi, sums, beta, state, comp = pl.pallas_call(
        functools.partial(prepare_kernel, stack),
        out_shape=[
            f32(count, rows, pixels), f32(count, rows, pixels),
            f32(count + 1, halves, KP, LANES), f32(count + 1, halves, KP, LANES),
            f32(2, halves, KP, LANES), f32(2, halves, KP, LANES), f32(SUB, pixels), f32(2, pixels),
        ],
        in_specs=[SMEM] + [VMEM] * 4,
        out_specs=[VMEM] * 8,
        scratch_shapes=[
            pltpu.VMEM((2 * rows, window), jnp.float32),
            pltpu.VMEM((4 * rows, window), jnp.bfloat16),
            pltpu.VMEM((2, count + 1, count, SUB, LANES), jnp.float32),
        ],
        compiler_params=params(),
        name="prepare",
    )(at, neighbours, low, slc, high)

    for rnd in range(1, sections):
        def hop(shift):
            pairs = [
                ((rnd - 1) * blocks + q, rnd * blocks + q + shift)
                for q in range(blocks)
                if 0 <= q + shift < blocks
            ]
            return lax.ppermute(comp, ("section", "pix"), pairs)

        beta, state, comp = pl.pallas_call(
            functools.partial(round_kernel, rnd, stack),
            out_shape=[f32(2, halves, KP, LANES), f32(SUB, pixels), f32(2, pixels)],
            in_specs=[SMEM] + [VMEM] * 9,
            out_specs=[VMEM] * 3,
            scratch_shapes=[pltpu.VMEM((count, halves, KP, LANES), jnp.float32)] * 2,
            compiler_params=params(),
            name=f"round{rnd}",
        )(at, neighbours, hop(1)[:, pixels - reach :], hop(0), hop(-1)[:, :reach], gr, gi, sums, beta, state)

    slot_rows = up(2 * halves + 4, SUB)
    vec, slot = pl.pallas_call(
        vector_kernel,
        out_shape=[f32(2, dates, pixels), f32(slot_rows, LANES)],
        in_specs=[SMEM] + [VMEM] * 4,
        out_specs=[VMEM] * 2,
        scratch_shapes=[pltpu.VMEM((2, pixels, LANES), jnp.float32)],
        compiler_params=params(),
        name="vectors",
    )(at, zr, zi, beta, state)
    devices = sections * blocks
    sent = jnp.broadcast_to(slot[None], (devices, slot_rows, LANES))
    got = lax.all_to_all(sent, ("section", "pix"), 0, 0, tiled=True)
    out = pl.pallas_call(
        functools.partial(finish_kernel, sections),
        out_shape=f32(2, dates, pixels),
        in_specs=[SMEM] + [VMEM] * 2,
        out_specs=VMEM,
        compiler_params=params(),
        name="finish",
    )(at, vec, got)
    return (out, comp[:, None, :])


def solution(mesh):
    return jax.shard_map(
        on_device,
        mesh=mesh,
        in_specs=(P(None, "section", "pix"), P(None, "pix"), P()),
        out_specs=(P(None, "section", "pix"), P(None, "section", "pix")),
        check_vma=False,
    )
```

```python
import functools
import math

import jax
import jax.numpy as jnp
from jax import lax
from jax.experimental import pallas as pl
from jax.experimental.pallas import tpu as pltpu
from jax.sharding import PartitionSpec as P

ITERS = 16
FLOOR = 0.05
REACH_LIMIT = 256
LANES = 128
SUB = 8
KP = 16
SHRINK = 2.0**-35

SMEM = pl.BlockSpec(memory_space=pltpu.SMEM)
VMEM = pl.BlockSpec(memory_space=pltpu.VMEM)


def f32(*shape):
    return jax.ShapeDtypeStruct(shape, jnp.float32)


def params():
    return pltpu.CompilerParams(vmem_limit_bytes=20 * 1024 * 1024)


def cost(flops):
    return pl.CostEstimate(flops=flops, bytes_accessed=0, transcendentals=0)


def up(n, m):
    return -(-n // m) * m


def colsum(x):
    return jnp.sum(x, axis=0, keepdims=True)


def unit(real, imag):
    scale = 1.0 / jnp.maximum(jnp.sqrt(real * real + imag * imag), FLOOR)
    return (real * scale, imag * scale)


def half(h):
    return pl.ds(h * LANES, LANES)


def gather(start, idx_ref, pieces, xs_ref, hl_ref, zr_ref, zi_ref, add):
    count, rows, pixels = zr_ref.shape
    xs_ref[...] = jnp.zeros_like(xs_ref)
    at = 0
    place = []
    for piece, first in pieces:
        dates, _, width = piece.shape
        for c in range(2):
            xs_ref[pl.ds(c * rows, dates), pl.ds(at, width)] = piece[:, c]
        place.append(lax.broadcasted_iota(jnp.int32, (width, pixels), 0) + first)
        at += width
    place = jnp.concatenate(place, axis=0)
    high = xs_ref[...].astype(jnp.bfloat16)
    hl_ref[0 : 2 * rows] = high
    hl_ref[2 * rows : 4 * rows] = (xs_ref[...] - high.astype(jnp.float32)).astype(jnp.bfloat16)
    for k in range(count):
        near = idx_ref[k : k + 1, :] - start
        hot = jnp.where(place == near, 1.0, 0.0).astype(jnp.bfloat16)
        got = jnp.dot(hl_ref[...], hot, preferred_element_type=jnp.float32)
        zr = got[0:rows] + got[2 * rows : 3 * rows]
        zi = got[rows : 2 * rows] + got[3 * rows : 4 * rows]
        zr_ref[k] = zr_ref[k] + zr if add else zr
        zi_ref[k] = zi_ref[k] + zi if add else zi


def scale_dates(zr_ref, zi_ref):
    count, rows, pixels = zr_ref.shape
    for h in range(pixels // LANES):
        for r in range(0, rows, SUB):
            power = None
            for k in range(count):
                a = zr_ref[k, pl.ds(r, SUB), half(h)]
                b = zi_ref[k, pl.ds(r, SUB), half(h)]
                power = a * a + b * b if power is None else power + (a * a + b * b)
            scale = lax.rsqrt(jnp.maximum(power, 1.0))
            for k in range(count):
                zr_ref[k, pl.ds(r, SUB), half(h)] *= scale
                zi_ref[k, pl.ds(r, SUB), half(h)] *= scale


def merge_rows(parts):
    row = lax.broadcasted_iota(jnp.int32, (SUB, LANES), 0)
    for step in (4, 2, 1):
        low = jnp.bitwise_and(row, step) == 0
        other = jnp.bitwise_xor(row, step)
        n = len(parts) // 2
        out = []
        for i in range(n):
            a, b = parts[i], parts[i + n]
            far = jnp.take_along_axis(jnp.where(low, b, a), other, axis=0, mode="promise_in_bounds")
            out.append(jnp.where(low, a, b) + far)
        parts = out
    return parts[0]


def gram(pair_ref, zr_ref, zi_ref, own_ref, gr_ref, gi_ref, sum_ref, block=3):
    count, rows, pixels = zr_ref.shape
    zero = jnp.zeros((SUB, LANES), jnp.float32)
    for h in range(pixels // LANES):
        def load(k, r):
            if k == count:
                return (own_ref[pl.ds(r, SUB), half(h)], own_ref[pl.ds(rows + r, SUB), half(h)])
            return (zr_ref[k, pl.ds(r, SUB), half(h)], zi_ref[k, pl.ds(r, SUB), half(h)])

        for k0 in range(0, count, block):
            for l0 in range(k0, count + 1, block):
                pairs = [
                    (k, l)
                    for k in range(k0, min(k0 + block, count))
                    for l in range(l0, min(l0 + block, count + 1))
                    if l >= k
                ]
                acc = {}
                for r in range(0, rows, SUB):
                    val = {n: load(n, r) for n in sorted({n for p in pairs for n in p})}
                    minus = {k: val[k][0] - val[k][1] for k in {k for k, l in pairs if k != l}}
                    plus = {l: val[l][0] + val[l][1] for l in {l for k, l in pairs if k != l}}
                    for k, l in pairs:
                        new = [val[k][0] * val[l][0], val[k][1] * val[l][1]]
                        if k != l:
                            new.append(minus[k] * plus[l])
                        acc[k, l] = [x + y for x, y in zip(acc[k, l], new)] if r else new
                for k, l in pairs:
                    pair_ref[0, l, k] = acc[k, l][0] + acc[k, l][1]
                    pair_ref[1, l, k] = zero if k == l else acc[k, l][2] - (acc[k, l][0] - acc[k, l][1])
        for c, g_ref in ((0, gr_ref), (1, gi_ref)):
            for l in range(count + 1):
                for kt in range(KP // SUB):
                    ks = range(kt * SUB, kt * SUB + SUB)
                    if min(ks) > min(l, count - 1):
                        continue
                    parts = [pair_ref[c, l, k] if k <= min(l, count - 1) else zero for k in ks]
                    g_ref[l, h, pl.ds(kt * SUB, SUB), :] = merge_rows(parts)
        row = lax.broadcasted_iota(jnp.int32, (SUB, LANES), 0)
        for c, g_ref in ((0, gr_ref), (1, gi_ref)):
            for l in range(count):
                for kt in range(KP // SUB):
                    ks = list(range(kt * SUB, kt * SUB + SUB))
                    if max(ks) <= l:
                        continue
                    other = jnp.concatenate(
                        [g_ref[k, h, pl.ds(l, 1), :] if l < k < count else zero[0:1] for k in ks], axis=0
                    )
                    if c:
                        other = -other
                    if min(ks) <= l:
                        other = jnp.where(row + ks[0] <= l, g_ref[l, h, pl.ds(kt * SUB, SUB), :], other)
                    g_ref[l, h, pl.ds(kt * SUB, SUB), :] = other
        for c in range(2):
            tiles = []
            for k in range(KP):
                total = None
                if k <= count:
                    for r in range(0, rows, SUB):
                        v = load(k, r)[c]
                        total = v if total is None else total + v
                tiles.append(zero if total is None else total)
            for kt in range(KP // SUB):
                sum_ref[c, h, pl.ds(kt * SUB, SUB), :] = merge_rows(tiles[kt * SUB : kt * SUB + SUB])


def turns(gr_ref, gi_ref, g0, count):
    halves = gr_ref.shape[1]

    def product(b, g):
        acc = [list(x) for x in g]
        for l in range(count):
            for h in range(halves):
                br = jnp.broadcast_to(b[h][0][l : l + 1], (KP, LANES))
                bi = jnp.broadcast_to(b[h][1][l : l + 1], (KP, LANES))
                gr = gr_ref[l, h]
                gi = gi_ref[l, h]
                acc[h][0] = acc[h][0] + (gr * br - gi * bi)
                acc[h][1] = acc[h][1] + (gr * bi + gi * br)
        return acc

    def step(_, carry):
        b, g = carry
        t = product(b, g)
        return tuple((b[h][0] + t[h][0], b[h][1] + t[h][1]) for h in range(halves)), g

    g = tuple(g0)
    b = g
    b, g = lax.fori_loop(0, ITERS // 2 - 1, step, (b, g))
    b = tuple((x * SHRINK, y * SHRINK) for x, y in b)
    g = tuple((x * SHRINK, y * SHRINK) for x, y in g)
    b, g = lax.fori_loop(0, ITERS - ITERS // 2, step, (b, g))
    return b, g, product(b, g)


def solve(virtual, gr_ref, gi_ref, hr, hi, sum_ref, stack, beta_ref, state_ref):
    halves = gr_ref.shape[1]
    count = gr_ref.shape[0]
    first = 1.0 / math.sqrt(stack)
    g0 = []
    for h in range(halves):
        zr, zi = sum_ref[0, h], sum_ref[1, h]
        row = lax.broadcasted_iota(jnp.int32, (KP, LANES), 0)
        zr = jnp.where(row < count, zr, 0.0)
        zi = jnp.where(row < count, zi, 0.0)
        if virtual is not None:
            zr = zr + virtual[h][1][0]
            zi = zi + virtual[h][1][1]
        g0.append((zr * first, zi * -first))
    b, g, t = turns(gr_ref, gi_ref, g0, count)
    for h in range(halves):
        norm = colsum(b[h][0] * (g[h][0] + t[h][0]) + b[h][1] * (g[h][1] + t[h][1]))
        inv = lax.rsqrt(SHRINK * SHRINK + norm)
        br, bi = b[h][0] * inv, b[h][1] * inv
        a = inv * (SHRINK * first)
        xr, xi = hr[h], hi[h]
        sr, si = sum_ref[0, h][count : count + 1], sum_ref[1, h][count : count + 1]
        fr, fi = a, jnp.zeros_like(a)
        if virtual is not None:
            (wr, wi), (zr, zi) = virtual[h]
            xr, xi = xr + (zr * wr + zi * wi), xi + (zr * wi - zi * wr)
            sr, si = sr + wr, si + wi
            fr = a + colsum(zr * br - zi * bi)
            fi = colsum(zr * bi + zi * br)
        beta_ref[0, h] = br
        beta_ref[1, h] = bi
        fr, fi = unit(fr, fi)
        state_ref[0:1, half(h)] = a * sr + colsum(br * xr + bi * xi)
        state_ref[1:2, half(h)] = a * si + colsum(br * xi - bi * xr)
        state_ref[2:3, half(h)] = fr
        state_ref[3:4, half(h)] = fi
        state_ref[4:5, half(h)] = a
        state_ref[5:8, half(h)] = jnp.zeros((3, LANES), jnp.float32)


def own_kernel(at_ref, idx_ref, slc_ref, zr_ref, zi_ref, own_ref, hl_ref):
    gather(at_ref[6], idx_ref, ((slc_ref, 0),), own_ref, hl_ref, zr_ref, zi_ref, False)


def prepare_kernel(stack, first, at_ref, idx_ref, low_ref, high_ref, own_ref, *refs):
    refs = refs[2 if first else 7 :]
    zr_ref, zi_ref, gr_ref, gi_ref, sum_ref, beta_ref, state_ref = refs[:7]
    xs_ref, hl_ref, pair_ref = refs[-3:]

    @pl.when(at_ref[1] == 0 if first else at_ref[1] != 0)
    def _():
        count, _, pixels = zr_ref.shape
        pieces = ((low_ref, -low_ref.shape[2]), (high_ref, pixels))
        gather(at_ref[6], idx_ref, pieces, xs_ref, hl_ref, zr_ref, zi_ref, True)
        scale_dates(zr_ref, zi_ref)
        gram(pair_ref, zr_ref, zi_ref, own_ref, gr_ref, gi_ref, sum_ref)
        if first:
            halves = gr_ref.shape[1]
            hr = [gr_ref[count, h] for h in range(halves)]
            hi = [gi_ref[count, h] for h in range(halves)]
            solve(None, gr_ref.at[0:count], gi_ref.at[0:count], hr, hi, sum_ref, stack, beta_ref, state_ref)
            refs[7][...] = state_ref[0:2]


def lane_take(x, i):
    return jnp.take_along_axis(x, i, axis=1, mode="promise_in_bounds")


def round_kernel(
    rnd, stack, where_ref, idx_ref, low_ref, own_ref, high_ref,
    gr_ref, gi_ref, sum_ref, beta0_ref, state0_ref,
    beta_ref, state_ref, comp_ref, fr_ref, fi_ref,
):
    count = gr_ref.shape[0] - 1
    halves = gr_ref.shape[1]
    reach = low_ref.shape[1]
    beta_ref[...] = beta0_ref[...]
    state_ref[...] = state0_ref[...]

    @pl.when(where_ref[1] == rnd)
    def _():
        tiles = []
        for ref in (low_ref, own_ref, high_ref):
            for t in range(ref.shape[1] // LANES):
                tiles.append([ref[c : c + 1, half(t)] for c in range(2)])
        virtual = []
        for h in range(halves):
            parts = []
            for kt in range(KP // SUB):
                rows = min(SUB, count - kt * SUB)
                raw = idx_ref[pl.ds(kt * SUB, rows), half(h)] - where_ref[0]
                if rows < SUB:
                    raw = jnp.concatenate([raw, jnp.full((SUB - rows, LANES), -1, jnp.int32)], axis=0)
                lane = jnp.bitwise_and(raw, LANES - 1)
                tile = jnp.right_shift(raw, 7)
                both = []
                for c in range(2):
                    out = jnp.zeros((SUB, LANES), jnp.float32)
                    for n in range(h, h + 2 * reach // LANES + 1):
                        got = lane_take(jnp.broadcast_to(tiles[n][c], (SUB, LANES)), lane)
                        out = jnp.where(tile == n, got, out)
                    both.append(out)
                parts.append(both)
            zr = jnp.concatenate([p[0] for p in parts], axis=0)
            zi = jnp.concatenate([p[1] for p in parts], axis=0)
            scale = lax.rsqrt(jnp.maximum(colsum(zr * zr + zi * zi), 1.0))
            zr, zi = zr * scale, zi * scale
            own = tiles[reach // LANES + h]
            virtual.append((own, (zr, zi)))
            for l in range(count):
                br = jnp.broadcast_to(zr[l : l + 1], (KP, LANES))
                bi = jnp.broadcast_to(zi[l : l + 1], (KP, LANES))
                fr_ref[l, h] = gr_ref[l, h] + (zr * br + zi * bi)
                fi_ref[l, h] = gi_ref[l, h] + (zr * bi - zi * br)
        hr = [gr_ref[count, h] for h in range(halves)]
        hi = [gi_ref[count, h] for h in range(halves)]
        solve(virtual, fr_ref, fi_ref, hr, hi, sum_ref, stack, beta_ref, state_ref)

    comp_ref[...] = state_ref[0:2]


def vector_kernel(at_ref, zr_ref, zi_ref, beta_ref, state_ref, vec_ref, slot_ref, turned_ref):
    count, rows, pixels = zr_ref.shape
    dates = vec_ref.shape[1]
    local = at_ref[2]
    for h in range(pixels // LANES):
        a = state_ref[4:5, half(h)]
        acc_r = [jnp.broadcast_to(a, (SUB, LANES)) for _ in range(0, rows, SUB)]
        acc_i = [jnp.zeros((SUB, LANES), jnp.float32) for _ in range(0, rows, SUB)]
        for k in range(count):
            br = jnp.broadcast_to(beta_ref[0, h, k : k + 1, :], (SUB, LANES))
            bi = jnp.broadcast_to(beta_ref[1, h, k : k + 1, :], (SUB, LANES))
            for n, r in enumerate(range(0, rows, SUB)):
                zr = zr_ref[k, pl.ds(r, SUB), half(h)]
                zi = zi_ref[k, pl.ds(r, SUB), half(h)]
                acc_r[n] = acc_r[n] + (zr * br - zi * bi)
                acc_i[n] = acc_i[n] + (zr * bi + zi * br)
        for c, acc in ((0, acc_r), (1, acc_i)):
            whole = jnp.concatenate(acc, axis=0)
            vec_ref[c, :, half(h)] = whole[0:dates]
            wide = jnp.concatenate([whole, jnp.zeros((up(rows, LANES) - rows, LANES), jnp.float32)], axis=0)
            turned_ref[c, half(h)] = jnp.transpose(wide)
    slot = [jnp.zeros((1, LANES), jnp.float32)] * slot_ref.shape[1]
    lane = lax.broadcasted_iota(jnp.int32, (1, LANES), 1)
    halves = pixels // LANES
    for c in range(2):
        for h in range(halves):
            slot[c * halves + h] = state_ref[2 + c : 3 + c, half(h)]
        slot[2 * halves + c] = turned_ref[c, pl.ds(local, 1), :]
        picked = jnp.zeros((1, LANES), jnp.float32)
        for h in range(halves):
            picked = picked + jnp.where(lane == local - h * LANES, state_ref[2 + c : 3 + c, half(h)], 0.0)
        slot[2 * halves + 2 + c] = jnp.broadcast_to(jnp.sum(picked, axis=1, keepdims=True), (1, LANES))
    slot = jnp.concatenate(slot, axis=0)
    for n in range(slot_ref.shape[0]):
        slot_ref[n] = slot


def finish_kernel(sections, at_ref, vec_ref, got_ref, comp_ref, out_ref, small_ref):
    small_ref[:, 0] = comp_ref[...]
    dates, pixels = vec_ref.shape[1:]
    section, mine, root, blocks = at_ref[1], at_ref[3], at_ref[4], at_ref[5]
    halves = pixels // LANES
    one = jnp.ones((1, LANES), jnp.float32)
    datum = [(one, 0.0 * one) for _ in range(halves)]
    at_root = (one, 0.0 * one)
    for s in range(sections - 1, 0, -1):
        later = section < s
        own = got_ref[s * blocks + mine]
        ref = got_ref[s * blocks + root]

        def times(d, fr, fi):
            fr = jnp.where(later, fr, 1.0)
            fi = jnp.where(later, fi, 0.0)
            return (d[0] * fr - d[1] * fi, d[0] * fi + d[1] * fr)

        for h in range(halves):
            datum[h] = times(datum[h], own[h : h + 1], own[halves + h : halves + h + 1])
        at_root = times(at_root, ref[2 * halves + 2 : 2 * halves + 3], ref[2 * halves + 3 : 2 * halves + 4])
    ref = got_ref[section * blocks + root]
    vr, vi = ref[2 * halves : 2 * halves + 1], ref[2 * halves + 1 : 2 * halves + 2]
    ur, ui = unit(vr * at_root[0] - vi * at_root[1], vr * at_root[1] + vi * at_root[0])
    gain = math.sqrt(dates + 1)
    ur = jnp.transpose(jnp.broadcast_to(ur * gain, (LANES, LANES)))[0:dates]
    ui = jnp.transpose(jnp.broadcast_to(ui * gain, (LANES, LANES)))[0:dates]
    for h in range(halves):
        wr = ur * datum[h][0] + ui * datum[h][1]
        wi = ur * datum[h][1] - ui * datum[h][0]
        vr = vec_ref[0, :, half(h)]
        vi = vec_ref[1, :, half(h)]
        out_ref[:, 0, half(h)] = vr * wr - vi * wi
        out_ref[:, 1, half(h)] = vr * wi + vi * wr


def on_device(slc, neighbours, reference_pixel):
    dates, pixels = slc.shape[1:]
    slc = jnp.transpose(slc, (1, 0, 2))
    count = neighbours.shape[0]
    reach = min(pixels, REACH_LIMIT)
    sections = lax.axis_size("section")
    blocks = lax.axis_size("pix")
    section = lax.axis_index("section")
    block = lax.axis_index("pix")
    stack = dates + 1
    halves = pixels // LANES
    rows = up(dates, SUB)
    base = block * pixels - reach

    forward = [(i, i + 1) for i in range(blocks - 1)]
    backward = [(i + 1, i) for i in range(blocks - 1)]
    low = lax.ppermute(slc[:, :, pixels - reach :], "pix", forward)
    high = lax.ppermute(slc[:, :, :reach], "pix", backward)

    root = reference_pixel[0] // pixels
    local = reference_pixel[0] - root * pixels
    at = jnp.stack([base, section, local, block, root, jnp.int32(blocks), block * pixels]).astype(jnp.int32)

    made = [
        f32(count, rows, pixels), f32(count, rows, pixels),
        f32(count + 1, halves, KP, LANES), f32(count + 1, halves, KP, LANES),
        f32(2, halves, KP, LANES), f32(2, halves, KP, LANES), f32(SUB, pixels), f32(2, pixels),
    ]
    zr, zi, own = pl.pallas_call(
        own_kernel,
        out_shape=made[:2] + [f32(2 * rows, pixels)],
        in_specs=[SMEM, VMEM, VMEM],
        out_specs=[VMEM] * 3,
        scratch_shapes=[pltpu.VMEM((4 * rows, pixels), jnp.bfloat16)],
        compiler_params=params(),
        cost_estimate=cost(2 * 4 * rows * pixels * pixels * count),
        name="own",
    )(at, neighbours, slc)

    def prepare(first, carried):
        return pl.pallas_call(
            functools.partial(prepare_kernel, stack, first),
            out_shape=made[: 8 if first else 7],
            in_specs=[SMEM] + [VMEM] * (4 + len(carried)),
            out_specs=[VMEM] * (8 if first else 7),
            scratch_shapes=[
                pltpu.VMEM((2 * rows, 2 * reach), jnp.float32),
                pltpu.VMEM((4 * rows, 2 * reach), jnp.bfloat16),
                pltpu.VMEM((2, count + 1, count, SUB, LANES), jnp.float32),
            ],
            input_output_aliases={5 + n: n for n in range(len(carried))},
            compiler_params=params(),
            cost_estimate=cost(50 * 12 * rows * reach * pixels * count),
            name="prepare" + ("0" if first else "n"),
        )(at, neighbours, low, high, own, *carried)

    *made_0, comp = prepare(True, (zr, zi))
    zr, zi, gr, gi, sums, beta, state = prepare(False, made_0)

    for rnd in range(1, sections):
        def hop(shift):
            pairs = [
                ((rnd - 1) * blocks + q, rnd * blocks + q + shift)
                for q in range(blocks)
                if 0 <= q + shift < blocks
            ]
            return lax.ppermute(comp, ("section", "pix"), pairs)

        beta, state, comp = pl.pallas_call(
            functools.partial(round_kernel, rnd, stack),
            out_shape=[f32(2, halves, KP, LANES), f32(SUB, pixels), f32(2, pixels)],
            in_specs=[SMEM] + [VMEM] * 9,
            out_specs=[VMEM] * 3,
            scratch_shapes=[pltpu.VMEM((count, halves, KP, LANES), jnp.float32)] * 2,
            compiler_params=params(),
            name=f"round{rnd}",
        )(at, neighbours, hop(1)[:, pixels - reach :], hop(0), hop(-1)[:, :reach], gr, gi, sums, beta, state)

    devices = sections * blocks
    slot_rows = up(2 * halves + 4, SUB)
    vec, sent = pl.pallas_call(
        vector_kernel,
        out_shape=[f32(2, dates, pixels), f32(devices, slot_rows, LANES)],
        in_specs=[SMEM] + [VMEM] * 4,
        out_specs=[VMEM] * 2,
        scratch_shapes=[pltpu.VMEM((2, pixels, LANES), jnp.float32)],
        compiler_params=params(),
        name="vectors",
    )(at, zr, zi, beta, state)
    got = lax.all_to_all(sent, ("section", "pix"), 0, 0, tiled=True)
    out, small = pl.pallas_call(
        functools.partial(finish_kernel, sections),
        out_shape=[f32(dates, 2, pixels), f32(2, 1, pixels)],
        in_specs=[SMEM] + [VMEM] * 3,
        out_specs=[VMEM] * 2,
        compiler_params=params(),
        name="finish",
    )(at, vec, got, comp)
    return (jnp.transpose(out, (1, 0, 2)), small)


def solution(mesh):
    return jax.shard_map(
        on_device,
        mesh=mesh,
        in_specs=(P(None, "section", "pix"), P(None, "pix"), P()),
        out_specs=(P(None, "section", "pix"), P(None, "section", "pix")),
        check_vma=False,
    )
```

```python
import functools
import math

import jax
import jax.numpy as jnp
from jax import lax
from jax.experimental import pallas as pl
from jax.experimental.pallas import tpu as pltpu
from jax.sharding import PartitionSpec as P

ITERS = 16
FLOOR = 0.05
REACH_LIMIT = 256
LANES = 128
SUB = 8
KP = 16
SHRINK = 2.0**-35

SMEM = pl.BlockSpec(memory_space=pltpu.SMEM)
VMEM = pl.BlockSpec(memory_space=pltpu.VMEM)
HBM = pl.BlockSpec(memory_space=pltpu.HBM)


def f32(*shape):
    return jax.ShapeDtypeStruct(shape, jnp.float32)


def params():
    return pltpu.CompilerParams(vmem_limit_bytes=20 * 1024 * 1024)


def cost(flops):
    return pl.CostEstimate(flops=flops, bytes_accessed=0, transcendentals=0)


def up(n, m):
    return -(-n // m) * m


def colsum(x):
    return jnp.sum(x, axis=0, keepdims=True)


def unit(real, imag):
    scale = 1.0 / jnp.maximum(jnp.sqrt(real * real + imag * imag), FLOOR)
    return (real * scale, imag * scale)


def half(h):
    return pl.ds(h * LANES, LANES)


def gather(start, idx_ref, pieces, xs_ref, hl_ref, zr_ref, zi_ref, add):
    count, rows, pixels = zr_ref.shape
    xs_ref[...] = jnp.zeros_like(xs_ref)
    at = 0
    place = []
    for piece, first in pieces:
        dates, _, width = piece.shape
        for c in range(2):
            xs_ref[pl.ds(c * rows, dates), pl.ds(at, width)] = piece[:, c]
        place.append(lax.broadcasted_iota(jnp.int32, (width, pixels), 0) + first)
        at += width
    place = jnp.concatenate(place, axis=0)
    high = xs_ref[...].astype(jnp.bfloat16)
    hl_ref[0 : 2 * rows] = high
    hl_ref[2 * rows : 4 * rows] = (xs_ref[...] - high.astype(jnp.float32)).astype(jnp.bfloat16)
    for k in range(count):
        near = idx_ref[k : k + 1, :] - start
        hot = jnp.where(place == near, 1.0, 0.0).astype(jnp.bfloat16)
        got = jnp.dot(hl_ref[...], hot, preferred_element_type=jnp.float32)
        zr = got[0:rows] + got[2 * rows : 3 * rows]
        zi = got[rows : 2 * rows] + got[3 * rows : 4 * rows]
        zr_ref[k] = zr_ref[k] + zr if add else zr
        zi_ref[k] = zi_ref[k] + zi if add else zi


def scale_dates(zr_ref, zi_ref):
    count, rows, pixels = zr_ref.shape
    for h in range(pixels // LANES):
        for r in range(0, rows, SUB):
            power = None
            for k in range(count):
                a = zr_ref[k, pl.ds(r, SUB), half(h)]
                b = zi_ref[k, pl.ds(r, SUB), half(h)]
                power = a * a + b * b if power is None else power + (a * a + b * b)
            scale = lax.rsqrt(jnp.maximum(power, 1.0))
            for k in range(count):
                zr_ref[k, pl.ds(r, SUB), half(h)] *= scale
                zi_ref[k, pl.ds(r, SUB), half(h)] *= scale


def merge_rows(parts):
    row = lax.broadcasted_iota(jnp.int32, (SUB, LANES), 0)
    for step in (4, 2, 1):
        low = jnp.bitwise_and(row, step) == 0
        other = jnp.bitwise_xor(row, step)
        n = len(parts) // 2
        out = []
        for i in range(n):
            a, b = parts[i], parts[i + n]
            far = jnp.take_along_axis(jnp.where(low, b, a), other, axis=0, mode="promise_in_bounds")
            out.append(jnp.where(low, a, b) + far)
        parts = out
    return parts[0]


def gram(pair_ref, zr_ref, zi_ref, own_ref, gr_ref, gi_ref, sum_ref, block=3):
    count, rows, pixels = zr_ref.shape
    zero = jnp.zeros((SUB, LANES), jnp.float32)
    for h in range(pixels // LANES):
        def load(k, r):
            if k == count:
                return (own_ref[pl.ds(r, SUB), half(h)], own_ref[pl.ds(rows + r, SUB), half(h)])
            return (zr_ref[k, pl.ds(r, SUB), half(h)], zi_ref[k, pl.ds(r, SUB), half(h)])

        for k0 in range(0, count, block):
            for l0 in range(k0, count + 1, block):
                pairs = [
                    (k, l)
                    for k in range(k0, min(k0 + block, count))
                    for l in range(l0, min(l0 + block, count + 1))
                    if l >= k
                ]
                acc = {}
                for r in range(0, rows, SUB):
                    val = {n: load(n, r) for n in sorted({n for p in pairs for n in p})}
                    minus = {k: val[k][0] - val[k][1] for k in {k for k, l in pairs if k != l}}
                    plus = {l: val[l][0] + val[l][1] for l in {l for k, l in pairs if k != l}}
                    for k, l in pairs:
                        new = [val[k][0] * val[l][0], val[k][1] * val[l][1]]
                        if k != l:
                            new.append(minus[k] * plus[l])
                        acc[k, l] = [x + y for x, y in zip(acc[k, l], new)] if r else new
                for k, l in pairs:
                    pair_ref[0, l, k] = acc[k, l][0] + acc[k, l][1]
                    pair_ref[1, l, k] = zero if k == l else acc[k, l][2] - (acc[k, l][0] - acc[k, l][1])
        for c, g_ref in ((0, gr_ref), (1, gi_ref)):
            for l in range(count + 1):
                for kt in range(KP // SUB):
                    ks = range(kt * SUB, kt * SUB + SUB)
                    if min(ks) > min(l, count - 1):
                        continue
                    parts = [pair_ref[c, l, k] if k <= min(l, count - 1) else zero for k in ks]
                    g_ref[l, h, pl.ds(kt * SUB, SUB), :] = merge_rows(parts)
        row = lax.broadcasted_iota(jnp.int32, (SUB, LANES), 0)
        for c, g_ref in ((0, gr_ref), (1, gi_ref)):
            for l in range(count):
                for kt in range(KP // SUB):
                    ks = list(range(kt * SUB, kt * SUB + SUB))
                    if max(ks) <= l:
                        continue
                    other = jnp.concatenate(
                        [g_ref[k, h, pl.ds(l, 1), :] if l < k < count else zero[0:1] for k in ks], axis=0
                    )
                    if c:
                        other = -other
                    if min(ks) <= l:
                        other = jnp.where(row + ks[0] <= l, g_ref[l, h, pl.ds(kt * SUB, SUB), :], other)
                    g_ref[l, h, pl.ds(kt * SUB, SUB), :] = other
        for c in range(2):
            tiles = []
            for k in range(KP):
                total = None
                if k <= count:
                    for r in range(0, rows, SUB):
                        v = load(k, r)[c]
                        total = v if total is None else total + v
                tiles.append(zero if total is None else total)
            for kt in range(KP // SUB):
                sum_ref[c, h, pl.ds(kt * SUB, SUB), :] = merge_rows(tiles[kt * SUB : kt * SUB + SUB])


def turns(gr_ref, gi_ref, g0, count):
    halves = gr_ref.shape[1]

    def product(b, g):
        acc = [list(x) for x in g]
        for l in range(count):
            for h in range(halves):
                br = jnp.broadcast_to(b[h][0][l : l + 1], (KP, LANES))
                bi = jnp.broadcast_to(b[h][1][l : l + 1], (KP, LANES))
                gr = gr_ref[l, h]
                gi = gi_ref[l, h]
                acc[h][0] = acc[h][0] + (gr * br - gi * bi)
                acc[h][1] = acc[h][1] + (gr * bi + gi * br)
        return acc

    def step(_, carry):
        b, g = carry
        t = product(b, g)
        return tuple((b[h][0] + t[h][0], b[h][1] + t[h][1]) for h in range(halves)), g

    g = tuple(g0)
    b = g
    b, g = lax.fori_loop(0, ITERS // 2 - 1, step, (b, g))
    b = tuple((x * SHRINK, y * SHRINK) for x, y in b)
    g = tuple((x * SHRINK, y * SHRINK) for x, y in g)
    b, g = lax.fori_loop(0, ITERS - ITERS // 2, step, (b, g))
    return b, g, product(b, g)


def solve(virtual, gr_ref, gi_ref, hr, hi, sum_ref, stack, beta_ref, state_ref):
    halves = gr_ref.shape[1]
    count = gr_ref.shape[0]
    first = 1.0 / math.sqrt(stack)
    g0 = []
    for h in range(halves):
        zr, zi = sum_ref[0, h], sum_ref[1, h]
        row = lax.broadcasted_iota(jnp.int32, (KP, LANES), 0)
        zr = jnp.where(row < count, zr, 0.0)
        zi = jnp.where(row < count, zi, 0.0)
        if virtual is not None:
            zr = zr + virtual[h][1][0]
            zi = zi + virtual[h][1][1]
        g0.append((zr * first, zi * -first))
    b, g, t = turns(gr_ref, gi_ref, g0, count)
    for h in range(halves):
        norm = colsum(b[h][0] * (g[h][0] + t[h][0]) + b[h][1] * (g[h][1] + t[h][1]))
        inv = lax.rsqrt(SHRINK * SHRINK + norm)
        br, bi = b[h][0] * inv, b[h][1] * inv
        a = inv * (SHRINK * first)
        xr, xi = hr[h], hi[h]
        sr, si = sum_ref[0, h][count : count + 1], sum_ref[1, h][count : count + 1]
        fr, fi = a, jnp.zeros_like(a)
        if virtual is not None:
            (wr, wi), (zr, zi) = virtual[h]
            xr, xi = xr + (zr * wr + zi * wi), xi + (zr * wi - zi * wr)
            sr, si = sr + wr, si + wi
            fr = a + colsum(zr * br - zi * bi)
            fi = colsum(zr * bi + zi * br)
        beta_ref[0, h] = br
        beta_ref[1, h] = bi
        fr, fi = unit(fr, fi)
        state_ref[0:1, half(h)] = a * sr + colsum(br * xr + bi * xi)
        state_ref[1:2, half(h)] = a * si + colsum(br * xi - bi * xr)
        state_ref[2:3, half(h)] = fr
        state_ref[3:4, half(h)] = fi
        state_ref[4:5, half(h)] = a
        state_ref[5:8, half(h)] = jnp.zeros((3, LANES), jnp.float32)


def own_kernel(at_ref, idx_hbm, slc_hbm, zr_ref, zi_ref, own_ref, idx_ref, slc_ref, hl_ref, sems):
    copies = [
        pltpu.make_async_copy(slc_hbm, slc_ref, sems.at[0]),
        pltpu.make_async_copy(idx_hbm, idx_ref, sems.at[1]),
    ]
    for copy in copies:
        copy.start()
    for copy in copies:
        copy.wait()
    gather(at_ref[2], idx_ref, ((slc_ref, 0),), own_ref, hl_ref, zr_ref, zi_ref, False)


def prepare_kernel(stack, first, at_ref, idx_ref, low_ref, high_ref, own_ref, *refs):
    refs = refs[2 if first else 7 :]
    zr_ref, zi_ref, gr_ref, gi_ref, sum_ref, beta_ref, state_ref = refs[:7]
    xs_ref, hl_ref, pair_ref = refs[-3:]

    @pl.when(at_ref[1] == 0 if first else at_ref[1] != 0)
    def _():
        count, _, pixels = zr_ref.shape
        pieces = ((low_ref, -low_ref.shape[2]), (high_ref, pixels))
        gather(at_ref[2], idx_ref, pieces, xs_ref, hl_ref, zr_ref, zi_ref, True)
        scale_dates(zr_ref, zi_ref)
        gram(pair_ref, zr_ref, zi_ref, own_ref, gr_ref, gi_ref, sum_ref)
        if first:
            halves = gr_ref.shape[1]
            hr = [gr_ref[count, h] for h in range(halves)]
            hi = [gi_ref[count, h] for h in range(halves)]
            solve(None, gr_ref.at[0:count], gi_ref.at[0:count], hr, hi, sum_ref, stack, beta_ref, state_ref)
            refs[7][...] = state_ref[0:2]


def lane_take(x, i):
    return jnp.take_along_axis(x, i, axis=1, mode="promise_in_bounds")


def round_kernel(
    rnd, stack, where_ref, idx_ref, low_ref, own_ref, high_ref,
    gr_ref, gi_ref, sum_ref, beta0_ref, state0_ref, *refs,
):
    last = len(refs) > 5
    if last:
        late, (comp_ref, *made), refs = refs[:3], refs[3:6], refs[6:]
        fr_ref, fi_ref, beta_ref, state_ref, turned_ref = refs
    else:
        beta_ref, state_ref, comp_ref, fr_ref, fi_ref = refs
    count = gr_ref.shape[0] - 1
    halves = gr_ref.shape[1]
    reach = low_ref.shape[1]
    beta_ref[...] = beta0_ref[...]
    state_ref[...] = state0_ref[...]

    @pl.when(where_ref[1] == rnd)
    def _():
        tiles = []
        for ref in (low_ref, own_ref, high_ref):
            for t in range(ref.shape[1] // LANES):
                tiles.append([ref[c : c + 1, half(t)] for c in range(2)])
        virtual = []
        for h in range(halves):
            parts = []
            for kt in range(KP // SUB):
                rows = min(SUB, count - kt * SUB)
                raw = idx_ref[pl.ds(kt * SUB, rows), half(h)] - where_ref[0]
                if rows < SUB:
                    raw = jnp.concatenate([raw, jnp.full((SUB - rows, LANES), -1, jnp.int32)], axis=0)
                lane = jnp.bitwise_and(raw, LANES - 1)
                tile = jnp.right_shift(raw, 7)
                both = []
                for c in range(2):
                    out = jnp.zeros((SUB, LANES), jnp.float32)
                    for n in range(h, h + 2 * reach // LANES + 1):
                        got = lane_take(jnp.broadcast_to(tiles[n][c], (SUB, LANES)), lane)
                        out = jnp.where(tile == n, got, out)
                    both.append(out)
                parts.append(both)
            zr = jnp.concatenate([p[0] for p in parts], axis=0)
            zi = jnp.concatenate([p[1] for p in parts], axis=0)
            scale = lax.rsqrt(jnp.maximum(colsum(zr * zr + zi * zi), 1.0))
            zr, zi = zr * scale, zi * scale
            own = tiles[reach // LANES + h]
            virtual.append((own, (zr, zi)))
            for l in range(count):
                br = jnp.broadcast_to(zr[l : l + 1], (KP, LANES))
                bi = jnp.broadcast_to(zi[l : l + 1], (KP, LANES))
                fr_ref[l, h] = gr_ref[l, h] + (zr * br + zi * bi)
                fi_ref[l, h] = gi_ref[l, h] + (zr * bi - zi * br)
        hr = [gr_ref[count, h] for h in range(halves)]
        hi = [gi_ref[count, h] for h in range(halves)]
        solve(virtual, fr_ref, fi_ref, hr, hi, sum_ref, stack, beta_ref, state_ref)

    comp_ref[...] = state_ref[0:2]
    if last:
        vectors(*late, beta_ref, state_ref, *made, turned_ref)


def vectors(at_ref, zr_ref, zi_ref, beta_ref, state_ref, vec_ref, slot_ref, turned_ref):
    count, rows, pixels = zr_ref.shape
    dates = vec_ref.shape[1]
    local = at_ref[0]
    for h in range(pixels // LANES):
        a = state_ref[4:5, half(h)]
        acc_r = [jnp.broadcast_to(a, (SUB, LANES)) for _ in range(0, rows, SUB)]
        acc_i = [jnp.zeros((SUB, LANES), jnp.float32) for _ in range(0, rows, SUB)]
        for k in range(count):
            br = jnp.broadcast_to(beta_ref[0, h, k : k + 1, :], (SUB, LANES))
            bi = jnp.broadcast_to(beta_ref[1, h, k : k + 1, :], (SUB, LANES))
            for n, r in enumerate(range(0, rows, SUB)):
                zr = zr_ref[k, pl.ds(r, SUB), half(h)]
                zi = zi_ref[k, pl.ds(r, SUB), half(h)]
                acc_r[n] = acc_r[n] + (zr * br - zi * bi)
                acc_i[n] = acc_i[n] + (zr * bi + zi * br)
        for c, acc in ((0, acc_r), (1, acc_i)):
            whole = jnp.concatenate(acc, axis=0)
            vec_ref[c, :, half(h)] = whole[0:dates]
            wide = jnp.concatenate([whole, jnp.zeros((up(rows, LANES) - rows, LANES), jnp.float32)], axis=0)
            turned_ref[c, half(h)] = jnp.transpose(wide)
    slot = [jnp.zeros((1, LANES), jnp.float32)] * slot_ref.shape[1]
    lane = lax.broadcasted_iota(jnp.int32, (1, LANES), 1)
    halves = pixels // LANES
    for c in range(2):
        for h in range(halves):
            slot[c * halves + h] = state_ref[2 + c : 3 + c, half(h)]
        slot[2 * halves + c] = turned_ref[c, pl.ds(local, 1), :]
        picked = jnp.zeros((1, LANES), jnp.float32)
        for h in range(halves):
            picked = picked + jnp.where(lane == local - h * LANES, state_ref[2 + c : 3 + c, half(h)], 0.0)
        slot[2 * halves + 2 + c] = jnp.broadcast_to(jnp.sum(picked, axis=1, keepdims=True), (1, LANES))
    slot = jnp.concatenate(slot, axis=0)
    for n in range(slot_ref.shape[0]):
        slot_ref[n] = slot


def finish_kernel(sections, where_ref, at_ref, vec_ref, got_ref, comp_ref, out_ref, small_ref):
    small_ref[:, 0] = comp_ref[...]
    dates, pixels = vec_ref.shape[1:]
    section, mine, blocks, root = where_ref[1], where_ref[3], where_ref[4], at_ref[1]
    halves = pixels // LANES
    one = jnp.ones((1, LANES), jnp.float32)
    datum = [(one, 0.0 * one) for _ in range(halves)]
    at_root = (one, 0.0 * one)
    for s in range(sections - 1, 0, -1):
        later = section < s
        own = got_ref[s * blocks + mine]
        ref = got_ref[s * blocks + root]

        def times(d, fr, fi):
            fr = jnp.where(later, fr, 1.0)
            fi = jnp.where(later, fi, 0.0)
            return (d[0] * fr - d[1] * fi, d[0] * fi + d[1] * fr)

        for h in range(halves):
            datum[h] = times(datum[h], own[h : h + 1], own[halves + h : halves + h + 1])
        at_root = times(at_root, ref[2 * halves + 2 : 2 * halves + 3], ref[2 * halves + 3 : 2 * halves + 4])
    ref = got_ref[section * blocks + root]
    vr, vi = ref[2 * halves : 2 * halves + 1], ref[2 * halves + 1 : 2 * halves + 2]
    ur, ui = unit(vr * at_root[0] - vi * at_root[1], vr * at_root[1] + vi * at_root[0])
    gain = math.sqrt(dates + 1)
    ur = jnp.transpose(jnp.broadcast_to(ur * gain, (LANES, LANES)))[0:dates]
    ui = jnp.transpose(jnp.broadcast_to(ui * gain, (LANES, LANES)))[0:dates]
    for h in range(halves):
        wr = ur * datum[h][0] + ui * datum[h][1]
        wi = ur * datum[h][1] - ui * datum[h][0]
        vr = vec_ref[0, :, half(h)]
        vi = vec_ref[1, :, half(h)]
        out_ref[:, 0, half(h)] = vr * wr - vi * wi
        out_ref[:, 1, half(h)] = vr * wi + vi * wr


def on_device(slc, neighbours, reference_pixel):
    dates, pixels = slc.shape[1:]
    slc = jnp.transpose(slc, (1, 0, 2))
    count = neighbours.shape[0]
    reach = min(pixels, REACH_LIMIT)
    sections = lax.axis_size("section")
    blocks = lax.axis_size("pix")
    section = lax.axis_index("section")
    block = lax.axis_index("pix")
    stack = dates + 1
    halves = pixels // LANES
    rows = up(dates, SUB)
    base = block * pixels - reach

    forward = [(i, i + 1) for i in range(blocks - 1)]
    backward = [(i + 1, i) for i in range(blocks - 1)]
    low = lax.ppermute(slc[:, :, pixels - reach :], "pix", forward)
    high = lax.ppermute(slc[:, :, :reach], "pix", backward)

    at = jnp.stack([base, section, block * pixels, block, jnp.int32(blocks)]).astype(jnp.int32)

    made = [
        f32(count, rows, pixels), f32(count, rows, pixels),
        f32(count + 1, halves, KP, LANES), f32(count + 1, halves, KP, LANES),
        f32(2, halves, KP, LANES), f32(2, halves, KP, LANES), f32(SUB, pixels), f32(2, pixels),
    ]
    zr, zi, own, neighbours = pl.pallas_call(
        own_kernel,
        out_shape=made[:2] + [f32(2 * rows, pixels), jax.ShapeDtypeStruct(neighbours.shape, jnp.int32)],
        in_specs=[SMEM, HBM, HBM],
        out_specs=[VMEM] * 4,
        scratch_shapes=[
            pltpu.VMEM((dates, 2, pixels), jnp.float32),
            pltpu.VMEM((4 * rows, pixels), jnp.bfloat16),
            pltpu.SemaphoreType.DMA((2,)),
        ],
        compiler_params=params(),
        cost_estimate=cost(2 * 4 * rows * pixels * pixels * count),
        name="own",
    )(at, neighbours, slc)

    def prepare(first, carried):
        return pl.pallas_call(
            functools.partial(prepare_kernel, stack, first),
            out_shape=made[: 8 if first else 7],
            in_specs=[SMEM] + [VMEM] * (4 + len(carried)),
            out_specs=[VMEM] * (8 if first else 7),
            scratch_shapes=[
                pltpu.VMEM((2 * rows, 2 * reach), jnp.float32),
                pltpu.VMEM((4 * rows, 2 * reach), jnp.bfloat16),
                pltpu.VMEM((2, count + 1, count, SUB, LANES), jnp.float32),
            ],
            input_output_aliases={5 + n: n for n in range(len(carried))},
            compiler_params=params(),
            cost_estimate=cost(50 * 12 * rows * reach * pixels * count),
            name="prepare" + ("0" if first else "n"),
        )(at, neighbours, low, high, own, *carried)

    *made_0, comp = prepare(True, (zr, zi))
    zr, zi, gr, gi, sums, beta, state = prepare(False, made_0)

    for rnd in range(1, sections):
        def hop(shift):
            pairs = [
                ((rnd - 1) * blocks + q, rnd * blocks + q + shift)
                for q in range(blocks)
                if 0 <= q + shift < blocks
            ]
            return lax.ppermute(comp, ("section", "pix"), pairs)

        last = rnd == sections - 1
        late, specs = (), []
        scratch = [pltpu.VMEM((count, halves, KP, LANES), jnp.float32)] * 2
        outs = [f32(2, halves, KP, LANES), f32(SUB, pixels), f32(2, pixels)]
        if last:
            late, specs = (ref_at, zr, zi), [SMEM, VMEM, VMEM]
            scratch += [pltpu.VMEM(o.shape, o.dtype) for o in outs[:2]] + [pltpu.VMEM((2, pixels, LANES), jnp.float32)]
            outs = outs[2:] + [f32(2, dates, pixels), f32(sections * blocks, up(2 * halves + 4, SUB), LANES)]
        made = pl.pallas_call(
            functools.partial(round_kernel, rnd, stack),
            out_shape=outs,
            in_specs=[SMEM] + [VMEM] * 9 + specs,
            out_specs=[VMEM] * 3,
            scratch_shapes=scratch,
            compiler_params=params(),
            name=f"round{rnd}",
        )(at, neighbours, hop(1)[:, pixels - reach :], hop(0), hop(-1)[:, :reach], gr, gi, sums, beta, state, *late)
        if last:
            comp, vec, sent = made
        else:
            beta, state, comp = made
        if rnd == 1:
            pixel = lax.optimization_barrier((reference_pixel, comp))[0][0]
            ref_at = jnp.stack([pixel % pixels, pixel // pixels]).astype(jnp.int32)

    got = lax.all_to_all(sent, ("section", "pix"), 0, 0, tiled=True)
    out, small = pl.pallas_call(
        functools.partial(finish_kernel, sections),
        out_shape=[f32(dates, 2, pixels), f32(2, 1, pixels)],
        in_specs=[SMEM, SMEM] + [VMEM] * 3,
        out_specs=[VMEM] * 2,
        compiler_params=params(),
        name="finish",
    )(at, ref_at, vec, got, comp)
    return (jnp.transpose(out, (1, 0, 2)), small)


def solution(mesh):
    return jax.shard_map(
        on_device,
        mesh=mesh,
        in_specs=(P(None, "section", "pix"), P(None, "pix"), P()),
        out_specs=(P(None, "section", "pix"), P(None, "section", "pix")),
        check_vma=False,
    )
```

```python
import functools
import math

import jax
import jax.numpy as jnp
from jax import lax
from jax.experimental import pallas as pl
from jax.experimental.pallas import tpu as pltpu
from jax.sharding import PartitionSpec as P


ITERS = 16
FLOOR = 0.05
REACH_LIMIT = 256
LANES = 128
SUB = 8
KP = 16
SHRINK = 2.0**-35

SMEM = pl.BlockSpec(memory_space=pltpu.SMEM)
VMEM = pl.BlockSpec(memory_space=pltpu.VMEM)
HBM = pl.BlockSpec(memory_space=pltpu.HBM)


def f32(*shape):
    return jax.ShapeDtypeStruct(shape, jnp.float32)


def params():
    return pltpu.CompilerParams(vmem_limit_bytes=20 * 1024 * 1024)


def cost(flops):
    return pl.CostEstimate(flops=flops, bytes_accessed=0, transcendentals=0)


def up(n, m):
    return -(-n // m) * m


def colsum(x):
    return jnp.sum(x, axis=0, keepdims=True)


def unit(real, imag):
    scale = 1.0 / jnp.maximum(jnp.sqrt(real * real + imag * imag), FLOOR)
    return (real * scale, imag * scale)


def half(h):
    return pl.ds(h * LANES, LANES)


def gather(start, idx_ref, pieces, xs_ref, hl_ref, zr_ref, zi_ref, add):
    count, rows, pixels = zr_ref.shape
    xs_ref[...] = jnp.zeros_like(xs_ref)
    at = 0
    place = []
    for piece, first in pieces:
        dates, _, width = piece.shape
        for c in range(2):
            xs_ref[pl.ds(c * rows, dates), pl.ds(at, width)] = piece[:, c]
        place.append(lax.broadcasted_iota(jnp.int32, (width, pixels), 0) + first)
        at += width
    place = jnp.concatenate(place, axis=0)
    high = xs_ref[...].astype(jnp.bfloat16)
    hl_ref[0 : 2 * rows] = high
    hl_ref[2 * rows : 4 * rows] = (xs_ref[...] - high.astype(jnp.float32)).astype(jnp.bfloat16)
    for k in range(count):
        near = idx_ref[k : k + 1, :] - start
        hot = jnp.where(place == near, 1.0, 0.0).astype(jnp.bfloat16)
        got = jnp.dot(hl_ref[...], hot, preferred_element_type=jnp.float32)
        zr = got[0:rows] + got[2 * rows : 3 * rows]
        zi = got[rows : 2 * rows] + got[3 * rows : 4 * rows]
        zr_ref[k] = zr_ref[k] + zr if add else zr
        zi_ref[k] = zi_ref[k] + zi if add else zi


def scale_dates(zr_ref, zi_ref):
    count, rows, pixels = zr_ref.shape
    for h in range(pixels // LANES):
        for r in range(0, rows, SUB):
            power = None
            for k in range(count):
                a = zr_ref[k, pl.ds(r, SUB), half(h)]
                b = zi_ref[k, pl.ds(r, SUB), half(h)]
                power = a * a + b * b if power is None else power + (a * a + b * b)
            scale = lax.rsqrt(jnp.maximum(power, 1.0))
            for k in range(count):
                zr_ref[k, pl.ds(r, SUB), half(h)] *= scale
                zi_ref[k, pl.ds(r, SUB), half(h)] *= scale


def merge_rows(parts):
    row = lax.broadcasted_iota(jnp.int32, (SUB, LANES), 0)
    for step in (4, 2, 1):
        low = jnp.bitwise_and(row, step) == 0
        other = jnp.bitwise_xor(row, step)
        n = len(parts) // 2
        out = []
        for i in range(n):
            a, b = parts[i], parts[i + n]
            far = jnp.take_along_axis(jnp.where(low, b, a), other, axis=0, mode="promise_in_bounds")
            out.append(jnp.where(low, a, b) + far)
        parts = out
    return parts[0]


def gram(pair_ref, zr_ref, zi_ref, own_ref, gr_ref, gi_ref, sum_ref, block=3):
    count, rows, pixels = zr_ref.shape
    zero = jnp.zeros((SUB, LANES), jnp.float32)
    for h in range(pixels // LANES):
        def load(k, r):
            if k == count:
                return (own_ref[pl.ds(r, SUB), half(h)], own_ref[pl.ds(rows + r, SUB), half(h)])
            return (zr_ref[k, pl.ds(r, SUB), half(h)], zi_ref[k, pl.ds(r, SUB), half(h)])

        for k0 in range(0, count, block):
            for l0 in range(k0, count + 1, block):
                pairs = [
                    (k, l)
                    for k in range(k0, min(k0 + block, count))
                    for l in range(l0, min(l0 + block, count + 1))
                    if l >= k
                ]
                acc = {}
                for r in range(0, rows, SUB):
                    val = {n: load(n, r) for n in sorted({n for p in pairs for n in p})}
                    minus = {k: val[k][0] - val[k][1] for k in {k for k, l in pairs if k != l}}
                    plus = {l: val[l][0] + val[l][1] for l in {l for k, l in pairs if k != l}}
                    for k, l in pairs:
                        new = [val[k][0] * val[l][0], val[k][1] * val[l][1]]
                        if k != l:
                            new.append(minus[k] * plus[l])
                        acc[k, l] = [x + y for x, y in zip(acc[k, l], new)] if r else new
                for k, l in pairs:
                    pair_ref[0, l, k] = acc[k, l][0] + acc[k, l][1]
                    pair_ref[1, l, k] = zero if k == l else acc[k, l][2] - (acc[k, l][0] - acc[k, l][1])
        for c, g_ref in ((0, gr_ref), (1, gi_ref)):
            for l in range(count + 1):
                for kt in range(KP // SUB):
                    ks = range(kt * SUB, kt * SUB + SUB)
                    if min(ks) > min(l, count - 1):
                        continue
                    parts = [pair_ref[c, l, k] if k <= min(l, count - 1) else zero for k in ks]
                    g_ref[l, h, pl.ds(kt * SUB, SUB), :] = merge_rows(parts)
        row = lax.broadcasted_iota(jnp.int32, (SUB, LANES), 0)
        for c, g_ref in ((0, gr_ref), (1, gi_ref)):
            for l in range(count):
                for kt in range(KP // SUB):
                    ks = list(range(kt * SUB, kt * SUB + SUB))
                    if max(ks) <= l:
                        continue
                    other = jnp.concatenate(
                        [g_ref[k, h, pl.ds(l, 1), :] if l < k < count else zero[0:1] for k in ks], axis=0
                    )
                    if c:
                        other = -other
                    if min(ks) <= l:
                        other = jnp.where(row + ks[0] <= l, g_ref[l, h, pl.ds(kt * SUB, SUB), :], other)
                    g_ref[l, h, pl.ds(kt * SUB, SUB), :] = other
        for c in range(2):
            tiles = []
            for k in range(KP):
                total = None
                if k <= count:
                    for r in range(0, rows, SUB):
                        v = load(k, r)[c]
                        total = v if total is None else total + v
                tiles.append(zero if total is None else total)
            for kt in range(KP // SUB):
                sum_ref[c, h, pl.ds(kt * SUB, SUB), :] = merge_rows(tiles[kt * SUB : kt * SUB + SUB])


def turns(gr_ref, gi_ref, g0, count):
    halves = gr_ref.shape[1]

    def product(b, g):
        acc = [list(x) for x in g]
        for l in range(count):
            for h in range(halves):
                br = jnp.broadcast_to(b[h][0][l : l + 1], (KP, LANES))
                bi = jnp.broadcast_to(b[h][1][l : l + 1], (KP, LANES))
                gr = gr_ref[l, h]
                gi = gi_ref[l, h]
                acc[h][0] = acc[h][0] + (gr * br - gi * bi)
                acc[h][1] = acc[h][1] + (gr * bi + gi * br)
        return acc

    def step(_, carry):
        b, g = carry
        t = product(b, g)
        return tuple((b[h][0] + t[h][0], b[h][1] + t[h][1]) for h in range(halves)), g

    g = tuple(g0)
    b = g
    b, g = lax.fori_loop(0, ITERS // 2 - 1, step, (b, g))
    b = tuple((x * SHRINK, y * SHRINK) for x, y in b)
    g = tuple((x * SHRINK, y * SHRINK) for x, y in g)
    b, g = lax.fori_loop(0, ITERS - ITERS // 2, step, (b, g))
    return b, g, product(b, g)


def solve(virtual, gr_ref, gi_ref, hr, hi, sum_ref, stack, beta_ref, state_ref):
    halves = gr_ref.shape[1]
    count = gr_ref.shape[0]
    first = 1.0 / math.sqrt(stack)
    g0 = []
    for h in range(halves):
        zr, zi = sum_ref[0, h], sum_ref[1, h]
        row = lax.broadcasted_iota(jnp.int32, (KP, LANES), 0)
        zr = jnp.where(row < count, zr, 0.0)
        zi = jnp.where(row < count, zi, 0.0)
        if virtual is not None:
            zr = zr + virtual[h][1][0]
            zi = zi + virtual[h][1][1]
        g0.append((zr * first, zi * -first))
    b, g, t = turns(gr_ref, gi_ref, g0, count)
    for h in range(halves):
        norm = colsum(b[h][0] * (g[h][0] + t[h][0]) + b[h][1] * (g[h][1] + t[h][1]))
        inv = lax.rsqrt(SHRINK * SHRINK + norm)
        br, bi = b[h][0] * inv, b[h][1] * inv
        a = inv * (SHRINK * first)
        xr, xi = hr[h], hi[h]
        sr, si = sum_ref[0, h][count : count + 1], sum_ref[1, h][count : count + 1]
        fr, fi = a, jnp.zeros_like(a)
        if virtual is not None:
            (wr, wi), (zr, zi) = virtual[h]
            xr, xi = xr + (zr * wr + zi * wi), xi + (zr * wi - zi * wr)
            sr, si = sr + wr, si + wi
            fr = a + colsum(zr * br - zi * bi)
            fi = colsum(zr * bi + zi * br)
        beta_ref[0, h] = br
        beta_ref[1, h] = bi
        fr, fi = unit(fr, fi)
        state_ref[0:1, half(h)] = a * sr + colsum(br * xr + bi * xi)
        state_ref[1:2, half(h)] = a * si + colsum(br * xi - bi * xr)
        state_ref[2:3, half(h)] = fr
        state_ref[3:4, half(h)] = fi
        state_ref[4:5, half(h)] = a
        state_ref[5:8, half(h)] = jnp.zeros((3, LANES), jnp.float32)


def own_kernel(at_ref, idx_hbm, slc_hbm, zr_ref, zi_ref, own_ref, idx_ref, slc_ref, hl_ref, sems):
    copies = [
        pltpu.make_async_copy(slc_hbm, slc_ref, sems.at[0]),
        pltpu.make_async_copy(idx_hbm, idx_ref, sems.at[1]),
    ]
    for copy in copies:
        copy.start()
    for copy in copies:
        copy.wait()
    gather(at_ref[2], idx_ref, ((slc_ref, 0),), own_ref, hl_ref, zr_ref, zi_ref, False)


def prepare_kernel(stack, first, at_ref, idx_ref, near_ref, far_ref, own_ref, *refs):
    refs = refs[2 if first else 7 :]
    zr_ref, zi_ref, gr_ref, gi_ref, sum_ref, beta_ref, state_ref = refs[:7]
    xs_ref, hl_ref, pair_ref = refs[-3:]

    @pl.when(at_ref[1] == 0 if first else at_ref[1] != 0)
    def _():
        count = zr_ref.shape[0]
        pieces = ((near_ref, at_ref[5]), (far_ref, at_ref[6]))
        gather(at_ref[2], idx_ref, pieces, xs_ref, hl_ref, zr_ref, zi_ref, True)
        scale_dates(zr_ref, zi_ref)
        gram(pair_ref, zr_ref, zi_ref, own_ref, gr_ref, gi_ref, sum_ref)
        if first:
            halves = gr_ref.shape[1]
            hr = [gr_ref[count, h] for h in range(halves)]
            hi = [gi_ref[count, h] for h in range(halves)]
            solve(None, gr_ref.at[0:count], gi_ref.at[0:count], hr, hi, sum_ref, stack, beta_ref, state_ref)
            refs[7][...] = state_ref[0:2]


def lane_take(x, i):
    return jnp.take_along_axis(x, i, axis=1, mode="promise_in_bounds")


def round_kernel(
    rnd, stack, where_ref, idx_ref, low_ref, own_ref, high_ref,
    gr_ref, gi_ref, sum_ref, beta0_ref, state0_ref, *refs,
):
    last = len(refs) > 5
    if last:
        late, (comp_ref, *made), refs = refs[:3], refs[3:6], refs[6:]
        fr_ref, fi_ref, beta_ref, state_ref, turned_ref = refs
    else:
        beta_ref, state_ref, comp_ref, fr_ref, fi_ref = refs
    count = gr_ref.shape[0] - 1
    halves = gr_ref.shape[1]
    reach = low_ref.shape[1]
    beta_ref[...] = beta0_ref[...]
    state_ref[...] = state0_ref[...]

    @pl.when(where_ref[1] == rnd)
    def _():
        tiles = []
        for ref in (low_ref, own_ref, high_ref):
            for t in range(ref.shape[1] // LANES):
                tiles.append([ref[c : c + 1, half(t)] for c in range(2)])
        virtual = []
        for h in range(halves):
            parts = []
            for kt in range(KP // SUB):
                rows = min(SUB, count - kt * SUB)
                raw = idx_ref[pl.ds(kt * SUB, rows), half(h)] - where_ref[0]
                if rows < SUB:
                    raw = jnp.concatenate([raw, jnp.full((SUB - rows, LANES), -1, jnp.int32)], axis=0)
                lane = jnp.bitwise_and(raw, LANES - 1)
                tile = jnp.right_shift(raw, 7)
                both = []
                for c in range(2):
                    out = jnp.zeros((SUB, LANES), jnp.float32)
                    for n in range(h, h + 2 * reach // LANES + 1):
                        got = lane_take(jnp.broadcast_to(tiles[n][c], (SUB, LANES)), lane)
                        out = jnp.where(tile == n, got, out)
                    both.append(out)
                parts.append(both)
            zr = jnp.concatenate([p[0] for p in parts], axis=0)
            zi = jnp.concatenate([p[1] for p in parts], axis=0)
            scale = lax.rsqrt(jnp.maximum(colsum(zr * zr + zi * zi), 1.0))
            zr, zi = zr * scale, zi * scale
            own = tiles[reach // LANES + h]
            virtual.append((own, (zr, zi)))
            for l in range(count):
                br = jnp.broadcast_to(zr[l : l + 1], (KP, LANES))
                bi = jnp.broadcast_to(zi[l : l + 1], (KP, LANES))
                fr_ref[l, h] = gr_ref[l, h] + (zr * br + zi * bi)
                fi_ref[l, h] = gi_ref[l, h] + (zr * bi - zi * br)
        hr = [gr_ref[count, h] for h in range(halves)]
        hi = [gi_ref[count, h] for h in range(halves)]
        solve(virtual, fr_ref, fi_ref, hr, hi, sum_ref, stack, beta_ref, state_ref)

    comp_ref[...] = state_ref[0:2]
    if last:
        vectors(*late, beta_ref, state_ref, *made, turned_ref)


def vectors(at_ref, zr_ref, zi_ref, beta_ref, state_ref, vec_ref, slot_ref, turned_ref):
    count, rows, pixels = zr_ref.shape
    dates = vec_ref.shape[1]
    local = at_ref[0]
    for h in range(pixels // LANES):
        a = state_ref[4:5, half(h)]
        acc_r = [jnp.broadcast_to(a, (SUB, LANES)) for _ in range(0, rows, SUB)]
        acc_i = [jnp.zeros((SUB, LANES), jnp.float32) for _ in range(0, rows, SUB)]
        for k in range(count):
            br = jnp.broadcast_to(beta_ref[0, h, k : k + 1, :], (SUB, LANES))
            bi = jnp.broadcast_to(beta_ref[1, h, k : k + 1, :], (SUB, LANES))
            for n, r in enumerate(range(0, rows, SUB)):
                zr = zr_ref[k, pl.ds(r, SUB), half(h)]
                zi = zi_ref[k, pl.ds(r, SUB), half(h)]
                acc_r[n] = acc_r[n] + (zr * br - zi * bi)
                acc_i[n] = acc_i[n] + (zr * bi + zi * br)
        for c, acc in ((0, acc_r), (1, acc_i)):
            whole = jnp.concatenate(acc, axis=0)
            vec_ref[c, :, half(h)] = whole[0:dates]
            wide = jnp.concatenate([whole, jnp.zeros((up(rows, LANES) - rows, LANES), jnp.float32)], axis=0)
            turned_ref[c, half(h)] = jnp.transpose(wide)
    slot = [jnp.zeros((1, LANES), jnp.float32)] * slot_ref.shape[1]
    lane = lax.broadcasted_iota(jnp.int32, (1, LANES), 1)
    halves = pixels // LANES
    for c in range(2):
        for h in range(halves):
            slot[c * halves + h] = state_ref[2 + c : 3 + c, half(h)]
        slot[2 * halves + c] = turned_ref[c, pl.ds(local, 1), :]
        picked = jnp.zeros((1, LANES), jnp.float32)
        for h in range(halves):
            picked = picked + jnp.where(lane == local - h * LANES, state_ref[2 + c : 3 + c, half(h)], 0.0)
        slot[2 * halves + 2 + c] = jnp.broadcast_to(jnp.sum(picked, axis=1, keepdims=True), (1, LANES))
    slot = jnp.concatenate(slot, axis=0)
    for n in range(slot_ref.shape[0]):
        slot_ref[n] = slot


def finish_kernel(sections, where_ref, at_ref, vec_ref, got_ref, comp_ref, out_ref, small_ref):
    small_ref[:, 0] = comp_ref[...]
    dates, pixels = vec_ref.shape[1:]
    section, mine, blocks, root = where_ref[1], where_ref[3], where_ref[4], at_ref[1]
    halves = pixels // LANES
    one = jnp.ones((1, LANES), jnp.float32)
    datum = [(one, 0.0 * one) for _ in range(halves)]
    at_root = (one, 0.0 * one)
    for s in range(sections - 1, 0, -1):
        later = section < s
        own = got_ref[s * blocks + mine]
        ref = got_ref[s * blocks + root]

        def times(d, fr, fi):
            fr = jnp.where(later, fr, 1.0)
            fi = jnp.where(later, fi, 0.0)
            return (d[0] * fr - d[1] * fi, d[0] * fi + d[1] * fr)

        for h in range(halves):
            datum[h] = times(datum[h], own[h : h + 1], own[halves + h : halves + h + 1])
        at_root = times(at_root, ref[2 * halves + 2 : 2 * halves + 3], ref[2 * halves + 3 : 2 * halves + 4])
    ref = got_ref[section * blocks + root]
    vr, vi = ref[2 * halves : 2 * halves + 1], ref[2 * halves + 1 : 2 * halves + 2]
    ur, ui = unit(vr * at_root[0] - vi * at_root[1], vr * at_root[1] + vi * at_root[0])
    gain = math.sqrt(dates + 1)
    ur = jnp.transpose(jnp.broadcast_to(ur * gain, (LANES, LANES)))[0:dates]
    ui = jnp.transpose(jnp.broadcast_to(ui * gain, (LANES, LANES)))[0:dates]
    for h in range(halves):
        wr = ur * datum[h][0] + ui * datum[h][1]
        wi = ur * datum[h][1] - ui * datum[h][0]
        vr = vec_ref[0, :, half(h)]
        vi = vec_ref[1, :, half(h)]
        out_ref[:, 0, half(h)] = vr * wr - vi * wi
        out_ref[:, 1, half(h)] = vr * wi + vi * wr


def on_device(slc, neighbours, reference_pixel):
    dates, pixels = slc.shape[1:]
    slc = jnp.transpose(slc, (1, 0, 2))
    count = neighbours.shape[0]
    reach = min(pixels, REACH_LIMIT)
    sections = lax.axis_size("section")
    blocks = lax.axis_size("pix")
    section = lax.axis_index("section")
    block = lax.axis_index("pix")
    stack = dates + 1
    halves = pixels // LANES
    rows = up(dates, SUB)
    base = block * pixels - reach

    even = block % 2 == 0

    def swap(first, upper):
        pairs = [(i, i + 1) for i in range(first, blocks - 1, 2)]
        pairs += [(j, i) for i, j in pairs]
        sent = slc
        if reach < pixels:
            sent = jnp.where(upper, slc[:, :, pixels - reach :], slc[:, :, :reach])
        return lax.ppermute(sent, "pix", pairs), jnp.where(upper, pixels, -reach)

    near, near_at = swap(0, even)
    far, far_at = swap(1, ~even)

    at = jnp.stack([base, section, block * pixels, block, jnp.int32(blocks), near_at, far_at]).astype(jnp.int32)

    made = [
        f32(count, rows, pixels), f32(count, rows, pixels),
        f32(count + 1, halves, KP, LANES), f32(count + 1, halves, KP, LANES),
        f32(2, halves, KP, LANES), f32(2, halves, KP, LANES), f32(SUB, pixels), f32(2, pixels),
    ]
    zr, zi, own, neighbours = pl.pallas_call(
        own_kernel,
        out_shape=made[:2] + [f32(2 * rows, pixels), jax.ShapeDtypeStruct(neighbours.shape, jnp.int32)],
        in_specs=[SMEM, HBM, HBM],
        out_specs=[VMEM] * 4,
        scratch_shapes=[
            pltpu.VMEM((dates, 2, pixels), jnp.float32),
            pltpu.VMEM((4 * rows, pixels), jnp.bfloat16),
            pltpu.SemaphoreType.DMA((2,)),
        ],
        compiler_params=params(),
        cost_estimate=cost(2 * 4 * rows * pixels * pixels * count),
        name="own",
    )(at, neighbours, slc)

    def prepare(first, carried):
        return pl.pallas_call(
            functools.partial(prepare_kernel, stack, first),
            out_shape=made[: 8 if first else 7],
            in_specs=[SMEM] + [VMEM] * (4 + len(carried)),
            out_specs=[VMEM] * (8 if first else 7),
            scratch_shapes=[
                pltpu.VMEM((2 * rows, 2 * reach), jnp.float32),
                pltpu.VMEM((4 * rows, 2 * reach), jnp.bfloat16),
                pltpu.VMEM((2, count + 1, count, SUB, LANES), jnp.float32),
            ],
            input_output_aliases={5 + n: n for n in range(len(carried))},
            compiler_params=params(),
            cost_estimate=cost(50 * 12 * rows * reach * pixels * count),
        )(at, neighbours, near, far, own, *carried)

    *made_0, comp = prepare(True, (zr, zi))
    zr, zi, gr, gi, sums, beta, state = prepare(False, made_0)

    for rnd in range(1, sections):
        def hop(shift):
            pairs = [
                ((rnd - 1) * blocks + q, rnd * blocks + q + shift)
                for q in range(blocks)
                if 0 <= q + shift < blocks
            ]
            return lax.ppermute(comp, ("section", "pix"), pairs)

        last = rnd == sections - 1
        late, specs = (), []
        scratch = [pltpu.VMEM((count, halves, KP, LANES), jnp.float32)] * 2
        outs = [f32(2, halves, KP, LANES), f32(SUB, pixels), f32(2, pixels)]
        if last:
            late, specs = (ref_at, zr, zi), [SMEM, VMEM, VMEM]
            scratch += [pltpu.VMEM(o.shape, o.dtype) for o in outs[:2]] + [pltpu.VMEM((2, pixels, LANES), jnp.float32)]
            outs = outs[2:] + [f32(2, dates, pixels), f32(sections * blocks, up(2 * halves + 4, SUB), LANES)]
        made = pl.pallas_call(
            functools.partial(round_kernel, rnd, stack),
            out_shape=outs,
            in_specs=[SMEM] + [VMEM] * 9 + specs,
            out_specs=[VMEM] * 3,
            scratch_shapes=scratch,
            compiler_params=params(),
        )(at, neighbours, hop(1)[:, pixels - reach :], hop(0), hop(-1)[:, :reach], gr, gi, sums, beta, state, *late)
        if last:
            comp, vec, sent = made
        else:
            beta, state, comp = made
        if rnd == 1:
            pixel = lax.optimization_barrier((reference_pixel, comp))[0][0]
            ref_at = jnp.stack([pixel % pixels, pixel // pixels]).astype(jnp.int32)

    got = lax.all_to_all(sent, ("section", "pix"), 0, 0, tiled=True)
    out, small = pl.pallas_call(
        functools.partial(finish_kernel, sections),
        out_shape=[f32(dates, 2, pixels), f32(2, 1, pixels)],
        in_specs=[SMEM, SMEM] + [VMEM] * 3,
        out_specs=[VMEM] * 2,
        compiler_params=params(),
        name="finish",
    )(at, ref_at, vec, got, comp)
    return (jnp.transpose(out, (1, 0, 2)), small)


def solution(mesh):
    return jax.shard_map(
        on_device,
        mesh=mesh,
        in_specs=(P(None, "section", "pix"), P(None, "pix"), P()),
        out_specs=(P(None, "section", "pix"), P(None, "section", "pix")),
        check_vma=False,
    )
```

```python
import functools
import math

import jax
import jax.numpy as jnp
from jax import lax
from jax.experimental import pallas as pl
from jax.experimental.pallas import tpu as pltpu
from jax.sharding import PartitionSpec as P


ITERS = 16
FLOOR = 0.05
REACH_LIMIT = 256
LANES = 128
SUB = 8
KP = 16
SHRINK = 2.0**-35

SMEM = pl.BlockSpec(memory_space=pltpu.SMEM)
VMEM = pl.BlockSpec(memory_space=pltpu.VMEM)
HBM = pl.BlockSpec(memory_space=pltpu.HBM)


def f32(*shape):
    return jax.ShapeDtypeStruct(shape, jnp.float32)


def params():
    return pltpu.CompilerParams(vmem_limit_bytes=20 * 1024 * 1024)


def cost(flops):
    return pl.CostEstimate(flops=flops, bytes_accessed=0, transcendentals=0)


def up(n, m):
    return -(-n // m) * m


def colsum(x):
    return jnp.sum(x, axis=0, keepdims=True)


def unit(real, imag):
    scale = 1.0 / jnp.maximum(jnp.sqrt(real * real + imag * imag), FLOOR)
    return (real * scale, imag * scale)


def seat(pixels, reach):
    section, block = lax.axis_index("section"), lax.axis_index("pix")
    even = block % 2 == 0
    return (
        section, block, lax.axis_size("pix"), block * pixels,
        jnp.where(even, pixels, -reach), jnp.where(even, -reach, pixels),
    )


def half(h):
    return pl.ds(h * LANES, LANES)


def gather(start, idx_ref, pieces, xs_ref, hl_ref, zr_ref, zi_ref, add):
    count, rows, pixels = zr_ref.shape
    xs_ref[...] = jnp.zeros_like(xs_ref)
    at = 0
    place = []
    for piece, first in pieces:
        dates, _, width = piece.shape
        for c in range(2):
            xs_ref[pl.ds(c * rows, dates), pl.ds(at, width)] = piece[:, c]
        place.append(lax.broadcasted_iota(jnp.int32, (width, pixels), 0) + first)
        at += width
    place = jnp.concatenate(place, axis=0)
    high = xs_ref[...].astype(jnp.bfloat16)
    hl_ref[0 : 2 * rows] = high
    hl_ref[2 * rows : 4 * rows] = (xs_ref[...] - high.astype(jnp.float32)).astype(jnp.bfloat16)
    for k in range(count):
        near = idx_ref[k : k + 1, :] - start
        hot = jnp.where(place == near, 1.0, 0.0).astype(jnp.bfloat16)
        got = jnp.dot(hl_ref[...], hot, preferred_element_type=jnp.float32)
        zr = got[0:rows] + got[2 * rows : 3 * rows]
        zi = got[rows : 2 * rows] + got[3 * rows : 4 * rows]
        zr_ref[k] = zr_ref[k] + zr if add else zr
        zi_ref[k] = zi_ref[k] + zi if add else zi


def scale_dates(zr_ref, zi_ref):
    count, rows, pixels = zr_ref.shape
    for h in range(pixels // LANES):
        for r in range(0, rows, SUB):
            power = None
            for k in range(count):
                a = zr_ref[k, pl.ds(r, SUB), half(h)]
                b = zi_ref[k, pl.ds(r, SUB), half(h)]
                power = a * a + b * b if power is None else power + (a * a + b * b)
            scale = lax.rsqrt(jnp.maximum(power, 1.0))
            for k in range(count):
                zr_ref[k, pl.ds(r, SUB), half(h)] *= scale
                zi_ref[k, pl.ds(r, SUB), half(h)] *= scale


def merge_rows(parts):
    row = lax.broadcasted_iota(jnp.int32, (SUB, LANES), 0)
    for step in (4, 2, 1):
        low = jnp.bitwise_and(row, step) == 0
        other = jnp.bitwise_xor(row, step)
        n = len(parts) // 2
        out = []
        for i in range(n):
            a, b = parts[i], parts[i + n]
            far = jnp.take_along_axis(jnp.where(low, b, a), other, axis=0, mode="promise_in_bounds")
            out.append(jnp.where(low, a, b) + far)
        parts = out
    return parts[0]


def gram(pair_ref, zr_ref, zi_ref, own_ref, gr_ref, gi_ref, sum_ref, block=3):
    count, rows, pixels = zr_ref.shape
    zero = jnp.zeros((SUB, LANES), jnp.float32)
    for h in range(pixels // LANES):
        def load(k, r):
            if k == count:
                return (own_ref[pl.ds(r, SUB), half(h)], own_ref[pl.ds(rows + r, SUB), half(h)])
            return (zr_ref[k, pl.ds(r, SUB), half(h)], zi_ref[k, pl.ds(r, SUB), half(h)])

        for k0 in range(0, count, block):
            for l0 in range(k0, count + 1, block):
                pairs = [
                    (k, l)
                    for k in range(k0, min(k0 + block, count))
                    for l in range(l0, min(l0 + block, count + 1))
                    if l >= k
                ]
                acc = {}
                for r in range(0, rows, SUB):
                    val = {n: load(n, r) for n in sorted({n for p in pairs for n in p})}
                    minus = {k: val[k][0] - val[k][1] for k in {k for k, l in pairs if k != l}}
                    plus = {l: val[l][0] + val[l][1] for l in {l for k, l in pairs if k != l}}
                    for k, l in pairs:
                        new = [val[k][0] * val[l][0], val[k][1] * val[l][1]]
                        if k != l:
                            new.append(minus[k] * plus[l])
                        acc[k, l] = [x + y for x, y in zip(acc[k, l], new)] if r else new
                for k, l in pairs:
                    pair_ref[0, l, k] = acc[k, l][0] + acc[k, l][1]
                    pair_ref[1, l, k] = zero if k == l else acc[k, l][2] - (acc[k, l][0] - acc[k, l][1])
        for c, g_ref in ((0, gr_ref), (1, gi_ref)):
            for l in range(count + 1):
                for kt in range(KP // SUB):
                    ks = range(kt * SUB, kt * SUB + SUB)
                    if min(ks) > min(l, count - 1):
                        continue
                    parts = [pair_ref[c, l, k] if k <= min(l, count - 1) else zero for k in ks]
                    g_ref[l, h, pl.ds(kt * SUB, SUB), :] = merge_rows(parts)
        row = lax.broadcasted_iota(jnp.int32, (SUB, LANES), 0)
        for c, g_ref in ((0, gr_ref), (1, gi_ref)):
            for l in range(count):
                for kt in range(KP // SUB):
                    ks = list(range(kt * SUB, kt * SUB + SUB))
                    if max(ks) <= l:
                        continue
                    other = jnp.concatenate(
                        [g_ref[k, h, pl.ds(l, 1), :] if l < k < count else zero[0:1] for k in ks], axis=0
                    )
                    if c:
                        other = -other
                    if min(ks) <= l:
                        other = jnp.where(row + ks[0] <= l, g_ref[l, h, pl.ds(kt * SUB, SUB), :], other)
                    g_ref[l, h, pl.ds(kt * SUB, SUB), :] = other
        for c in range(2):
            tiles = []
            for k in range(KP):
                total = None
                if k <= count:
                    for r in range(0, rows, SUB):
                        v = load(k, r)[c]
                        total = v if total is None else total + v
                tiles.append(zero if total is None else total)
            for kt in range(KP // SUB):
                sum_ref[c, h, pl.ds(kt * SUB, SUB), :] = merge_rows(tiles[kt * SUB : kt * SUB + SUB])


def turns(gr_ref, gi_ref, g0, count):
    halves = gr_ref.shape[1]

    def product(b, g):
        acc = [list(x) for x in g]
        for l in range(count):
            for h in range(halves):
                br = jnp.broadcast_to(b[h][0][l : l + 1], (KP, LANES))
                bi = jnp.broadcast_to(b[h][1][l : l + 1], (KP, LANES))
                gr = gr_ref[l, h]
                gi = gi_ref[l, h]
                acc[h][0] = acc[h][0] + (gr * br - gi * bi)
                acc[h][1] = acc[h][1] + (gr * bi + gi * br)
        return acc

    def step(_, carry):
        b, g = carry
        t = product(b, g)
        return tuple((b[h][0] + t[h][0], b[h][1] + t[h][1]) for h in range(halves)), g

    g = tuple(g0)
    b = g
    b, g = lax.fori_loop(0, ITERS // 2 - 1, step, (b, g))
    b = tuple((x * SHRINK, y * SHRINK) for x, y in b)
    g = tuple((x * SHRINK, y * SHRINK) for x, y in g)
    b, g = lax.fori_loop(0, ITERS - ITERS // 2, step, (b, g))
    return b, g, product(b, g)


def solve(virtual, gr_ref, gi_ref, hr, hi, sum_ref, stack, beta_ref, state_ref):
    halves = gr_ref.shape[1]
    count = gr_ref.shape[0]
    first = 1.0 / math.sqrt(stack)
    g0 = []
    for h in range(halves):
        zr, zi = sum_ref[0, h], sum_ref[1, h]
        row = lax.broadcasted_iota(jnp.int32, (KP, LANES), 0)
        zr = jnp.where(row < count, zr, 0.0)
        zi = jnp.where(row < count, zi, 0.0)
        if virtual is not None:
            zr = zr + virtual[h][1][0]
            zi = zi + virtual[h][1][1]
        g0.append((zr * first, zi * -first))
    b, g, t = turns(gr_ref, gi_ref, g0, count)
    for h in range(halves):
        norm = colsum(b[h][0] * (g[h][0] + t[h][0]) + b[h][1] * (g[h][1] + t[h][1]))
        inv = lax.rsqrt(SHRINK * SHRINK + norm)
        br, bi = b[h][0] * inv, b[h][1] * inv
        a = inv * (SHRINK * first)
        xr, xi = hr[h], hi[h]
        sr, si = sum_ref[0, h][count : count + 1], sum_ref[1, h][count : count + 1]
        fr, fi = a, jnp.zeros_like(a)
        if virtual is not None:
            (wr, wi), (zr, zi) = virtual[h]
            xr, xi = xr + (zr * wr + zi * wi), xi + (zr * wi - zi * wr)
            sr, si = sr + wr, si + wi
            fr = a + colsum(zr * br - zi * bi)
            fi = colsum(zr * bi + zi * br)
        beta_ref[0, h] = br
        beta_ref[1, h] = bi
        fr, fi = unit(fr, fi)
        state_ref[0:1, half(h)] = a * sr + colsum(br * xr + bi * xi)
        state_ref[1:2, half(h)] = a * si + colsum(br * xi - bi * xr)
        state_ref[2:3, half(h)] = fr
        state_ref[3:4, half(h)] = fi
        state_ref[4:5, half(h)] = a
        state_ref[5:8, half(h)] = jnp.zeros((3, LANES), jnp.float32)


def own_kernel(idx_hbm, slc_hbm, zr_ref, zi_ref, own_ref, idx_ref, slc_ref, hl_ref, sems):
    copies = [
        pltpu.make_async_copy(slc_hbm, slc_ref, sems.at[0]),
        pltpu.make_async_copy(idx_hbm, idx_ref, sems.at[1]),
    ]
    for copy in copies:
        copy.start()
    for copy in copies:
        copy.wait()
    start = seat(slc_ref.shape[2], 0)[3]
    gather(start, idx_ref, ((slc_ref, 0),), own_ref, hl_ref, zr_ref, zi_ref, False)


def prepare_kernel(stack, first, idx_ref, near_ref, far_ref, own_ref, *refs):
    refs = refs[2 if first else 7 :]
    zr_ref, zi_ref, gr_ref, gi_ref, sum_ref, beta_ref, state_ref = refs[:7]
    xs_ref, hl_ref, pair_ref = refs[-3:]

    section, _, _, start, near_at, far_at = seat(zr_ref.shape[2], near_ref.shape[2])

    @pl.when(section == 0 if first else section != 0)
    def _():
        count = zr_ref.shape[0]
        pieces = ((near_ref, near_at), (far_ref, far_at))
        gather(start, idx_ref, pieces, xs_ref, hl_ref, zr_ref, zi_ref, True)
        scale_dates(zr_ref, zi_ref)
        gram(pair_ref, zr_ref, zi_ref, own_ref, gr_ref, gi_ref, sum_ref)
        if first:
            halves = gr_ref.shape[1]
            hr = [gr_ref[count, h] for h in range(halves)]
            hi = [gi_ref[count, h] for h in range(halves)]
            solve(None, gr_ref.at[0:count], gi_ref.at[0:count], hr, hi, sum_ref, stack, beta_ref, state_ref)
            refs[7][...] = state_ref[0:2]


def lane_take(x, i):
    return jnp.take_along_axis(x, i, axis=1, mode="promise_in_bounds")


def round_kernel(
    rnd, stack, idx_ref, low_ref, own_ref, high_ref,
    gr_ref, gi_ref, sum_ref, beta0_ref, state0_ref, *refs,
):
    last = len(refs) > 5
    if last:
        late, (comp_ref, *made), refs = refs[:3], refs[3:6], refs[6:]
        fr_ref, fi_ref, beta_ref, state_ref, turned_ref = refs
    else:
        beta_ref, state_ref, comp_ref, fr_ref, fi_ref = refs
    count = gr_ref.shape[0] - 1
    halves = gr_ref.shape[1]
    reach = low_ref.shape[1]
    beta_ref[...] = beta0_ref[...]
    state_ref[...] = state0_ref[...]
    section, _, _, start, _, _ = seat(own_ref.shape[1], reach)

    @pl.when(section == rnd)
    def _():
        tiles = []
        for ref in (low_ref, own_ref, high_ref):
            for t in range(ref.shape[1] // LANES):
                tiles.append([ref[c : c + 1, half(t)] for c in range(2)])
        virtual = []
        for h in range(halves):
            parts = []
            for kt in range(KP // SUB):
                rows = min(SUB, count - kt * SUB)
                raw = idx_ref[pl.ds(kt * SUB, rows), half(h)] - (start - reach)
                if rows < SUB:
                    raw = jnp.concatenate([raw, jnp.full((SUB - rows, LANES), -1, jnp.int32)], axis=0)
                lane = jnp.bitwise_and(raw, LANES - 1)
                tile = jnp.right_shift(raw, 7)
                both = []
                for c in range(2):
                    out = jnp.zeros((SUB, LANES), jnp.float32)
                    for n in range(h, h + 2 * reach // LANES + 1):
                        got = lane_take(jnp.broadcast_to(tiles[n][c], (SUB, LANES)), lane)
                        out = jnp.where(tile == n, got, out)
                    both.append(out)
                parts.append(both)
            zr = jnp.concatenate([p[0] for p in parts], axis=0)
            zi = jnp.concatenate([p[1] for p in parts], axis=0)
            scale = lax.rsqrt(jnp.maximum(colsum(zr * zr + zi * zi), 1.0))
            zr, zi = zr * scale, zi * scale
            own = tiles[reach // LANES + h]
            virtual.append((own, (zr, zi)))
            for l in range(count):
                br = jnp.broadcast_to(zr[l : l + 1], (KP, LANES))
                bi = jnp.broadcast_to(zi[l : l + 1], (KP, LANES))
                fr_ref[l, h] = gr_ref[l, h] + (zr * br + zi * bi)
                fi_ref[l, h] = gi_ref[l, h] + (zr * bi - zi * br)
        hr = [gr_ref[count, h] for h in range(halves)]
        hi = [gi_ref[count, h] for h in range(halves)]
        solve(virtual, fr_ref, fi_ref, hr, hi, sum_ref, stack, beta_ref, state_ref)

    comp_ref[...] = state_ref[0:2]
    if last:
        vectors(*late, beta_ref, state_ref, *made, turned_ref)


def vectors(at_ref, zr_ref, zi_ref, beta_ref, state_ref, vec_ref, slot_ref, turned_ref):
    count, rows, pixels = zr_ref.shape
    dates = vec_ref.shape[1]
    local = at_ref[0]
    for h in range(pixels // LANES):
        a = state_ref[4:5, half(h)]
        acc_r = [jnp.broadcast_to(a, (SUB, LANES)) for _ in range(0, rows, SUB)]
        acc_i = [jnp.zeros((SUB, LANES), jnp.float32) for _ in range(0, rows, SUB)]
        for k in range(count):
            br = jnp.broadcast_to(beta_ref[0, h, k : k + 1, :], (SUB, LANES))
            bi = jnp.broadcast_to(beta_ref[1, h, k : k + 1, :], (SUB, LANES))
            for n, r in enumerate(range(0, rows, SUB)):
                zr = zr_ref[k, pl.ds(r, SUB), half(h)]
                zi = zi_ref[k, pl.ds(r, SUB), half(h)]
                acc_r[n] = acc_r[n] + (zr * br - zi * bi)
                acc_i[n] = acc_i[n] + (zr * bi + zi * br)
        for c, acc in ((0, acc_r), (1, acc_i)):
            whole = jnp.concatenate(acc, axis=0)
            vec_ref[c, :, half(h)] = whole[0:dates]
            wide = jnp.concatenate([whole, jnp.zeros((up(rows, LANES) - rows, LANES), jnp.float32)], axis=0)
            turned_ref[c, half(h)] = jnp.transpose(wide)
    slot = [jnp.zeros((1, LANES), jnp.float32)] * slot_ref.shape[1]
    lane = lax.broadcasted_iota(jnp.int32, (1, LANES), 1)
    halves = pixels // LANES
    for c in range(2):
        for h in range(halves):
            slot[c * halves + h] = state_ref[2 + c : 3 + c, half(h)]
        slot[2 * halves + c] = turned_ref[c, pl.ds(local, 1), :]
        picked = jnp.zeros((1, LANES), jnp.float32)
        for h in range(halves):
            picked = picked + jnp.where(lane == local - h * LANES, state_ref[2 + c : 3 + c, half(h)], 0.0)
        slot[2 * halves + 2 + c] = jnp.broadcast_to(jnp.sum(picked, axis=1, keepdims=True), (1, LANES))
    slot = jnp.concatenate(slot, axis=0)
    for n in range(slot_ref.shape[0]):
        slot_ref[n] = slot


def finish_kernel(sections, at_ref, vec_ref, got_ref, comp_ref, out_ref, small_ref):
    small_ref[:, 0] = comp_ref[...]
    dates, pixels = vec_ref.shape[1:]
    section, mine, blocks, _, _, _ = seat(pixels, 0)
    root = at_ref[1]
    halves = pixels // LANES
    one = jnp.ones((1, LANES), jnp.float32)
    datum = [(one, 0.0 * one) for _ in range(halves)]
    at_root = (one, 0.0 * one)
    for s in range(sections - 1, 0, -1):
        later = section < s
        own = got_ref[s * blocks + mine]
        ref = got_ref[s * blocks + root]

        def times(d, fr, fi):
            fr = jnp.where(later, fr, 1.0)
            fi = jnp.where(later, fi, 0.0)
            return (d[0] * fr - d[1] * fi, d[0] * fi + d[1] * fr)

        for h in range(halves):
            datum[h] = times(datum[h], own[h : h + 1], own[halves + h : halves + h + 1])
        at_root = times(at_root, ref[2 * halves + 2 : 2 * halves + 3], ref[2 * halves + 3 : 2 * halves + 4])
    ref = got_ref[section * blocks + root]
    vr, vi = ref[2 * halves : 2 * halves + 1], ref[2 * halves + 1 : 2 * halves + 2]
    ur, ui = unit(vr * at_root[0] - vi * at_root[1], vr * at_root[1] + vi * at_root[0])
    gain = math.sqrt(dates + 1)
    ur = jnp.transpose(jnp.broadcast_to(ur * gain, (LANES, LANES)))[0:dates]
    ui = jnp.transpose(jnp.broadcast_to(ui * gain, (LANES, LANES)))[0:dates]
    for h in range(halves):
        wr = ur * datum[h][0] + ui * datum[h][1]
        wi = ur * datum[h][1] - ui * datum[h][0]
        vr = vec_ref[0, :, half(h)]
        vi = vec_ref[1, :, half(h)]
        out_ref[:, 0, half(h)] = vr * wr - vi * wi
        out_ref[:, 1, half(h)] = vr * wi + vi * wr


def on_device(slc, neighbours, reference_pixel):
    dates, pixels = slc.shape[1:]
    slc = jnp.transpose(slc, (1, 0, 2))
    count = neighbours.shape[0]
    reach = min(pixels, REACH_LIMIT)
    sections = lax.axis_size("section")
    blocks = lax.axis_size("pix")
    block = lax.axis_index("pix")
    stack = dates + 1
    halves = pixels // LANES
    rows = up(dates, SUB)

    even = block % 2 == 0

    def swap(first, upper):
        pairs = [(i, i + 1) for i in range(first, blocks - 1, 2)]
        pairs += [(j, i) for i, j in pairs]
        sent = slc
        if reach < pixels:
            sent = jnp.where(upper, slc[:, :, pixels - reach :], slc[:, :, :reach])
        return lax.ppermute(sent, "pix", pairs)

    near = swap(0, even)
    far = swap(1, ~even)

    made = [
        f32(count, rows, pixels), f32(count, rows, pixels),
        f32(count + 1, halves, KP, LANES), f32(count + 1, halves, KP, LANES),
        f32(2, halves, KP, LANES), f32(2, halves, KP, LANES), f32(SUB, pixels), f32(2, pixels),
    ]
    zr, zi, own, neighbours = pl.pallas_call(
        own_kernel,
        out_shape=made[:2] + [f32(2 * rows, pixels), jax.ShapeDtypeStruct(neighbours.shape, jnp.int32)],
        in_specs=[HBM, HBM],
        out_specs=[VMEM] * 4,
        scratch_shapes=[
            pltpu.VMEM((dates, 2, pixels), jnp.float32),
            pltpu.VMEM((4 * rows, pixels), jnp.bfloat16),
            pltpu.SemaphoreType.DMA((2,)),
        ],
        compiler_params=params(),
        cost_estimate=cost(2 * 4 * rows * pixels * pixels * count),
        name="own",
    )(pltpu.with_memory_space_constraint(neighbours, pltpu.HBM), pltpu.with_memory_space_constraint(slc, pltpu.HBM))

    def prepare(first, carried):
        return pl.pallas_call(
            functools.partial(prepare_kernel, stack, first),
            out_shape=made[: 8 if first else 7],
            in_specs=[VMEM] * (4 + len(carried)),
            out_specs=[VMEM] * (8 if first else 7),
            scratch_shapes=[
                pltpu.VMEM((2 * rows, 2 * reach), jnp.float32),
                pltpu.VMEM((4 * rows, 2 * reach), jnp.bfloat16),
                pltpu.VMEM((2, count + 1, count, SUB, LANES), jnp.float32),
            ],
            input_output_aliases={4 + n: n for n in range(len(carried))},
            compiler_params=params(),
            cost_estimate=cost(50 * 12 * rows * reach * pixels * count),
        )(neighbours, near, far, own, *carried)

    *made_0, comp = prepare(True, (zr, zi))
    zr, zi, gr, gi, sums, beta, state = prepare(False, made_0)

    for rnd in range(1, sections):
        def hop(shift):
            pairs = [
                ((rnd - 1) * blocks + q, rnd * blocks + q + shift)
                for q in range(blocks)
                if 0 <= q + shift < blocks
            ]
            return lax.ppermute(comp, ("section", "pix"), pairs)

        last = rnd == sections - 1
        late, specs = (), []
        scratch = [pltpu.VMEM((count, halves, KP, LANES), jnp.float32)] * 2
        outs = [f32(2, halves, KP, LANES), f32(SUB, pixels), f32(2, pixels)]
        if last:
            late, specs = (ref_at, zr, zi), [SMEM, VMEM, VMEM]
            scratch += [pltpu.VMEM(o.shape, o.dtype) for o in outs[:2]] + [pltpu.VMEM((2, pixels, LANES), jnp.float32)]
            outs = outs[2:] + [f32(2, dates, pixels), f32(sections * blocks, up(2 * halves + 4, SUB), LANES)]
        made = pl.pallas_call(
            functools.partial(round_kernel, rnd, stack),
            out_shape=outs,
            in_specs=[VMEM] * 9 + specs,
            out_specs=[VMEM] * 3,
            scratch_shapes=scratch,
            compiler_params=params(),
        )(neighbours, hop(1)[:, pixels - reach :], hop(0), hop(-1)[:, :reach], gr, gi, sums, beta, state, *late)
        if last:
            comp, vec, sent = made
        else:
            beta, state, comp = made
        if rnd == 1:
            pixel = lax.optimization_barrier((reference_pixel, comp))[0][0]
            ref_at = jnp.stack([pixel % pixels, pixel // pixels]).astype(jnp.int32)

    got = lax.all_to_all(sent, ("section", "pix"), 0, 0, tiled=True)
    out, small = pl.pallas_call(
        functools.partial(finish_kernel, sections),
        out_shape=[f32(dates, 2, pixels), f32(2, 1, pixels)],
        in_specs=[SMEM] + [VMEM] * 3,
        out_specs=[VMEM] * 2,
        compiler_params=params(),
        name="finish",
    )(ref_at, vec, got, comp)
    return (jnp.transpose(out, (1, 0, 2)), small)


def solution(mesh):
    return jax.shard_map(
        on_device,
        mesh=mesh,
        in_specs=(P(None, "section", "pix"), P(None, "pix"), P()),
        out_specs=(P(None, "section", "pix"), P(None, "section", "pix")),
        check_vma=False,
    )
```

```python
import functools
import math

import jax
import jax.numpy as jnp
from jax import lax
from jax.experimental import pallas as pl
from jax.experimental.pallas import tpu as pltpu
from jax.sharding import PartitionSpec as P


ITERS = 16
FLOOR = 0.05
REACH_LIMIT = 256
LANES = 128
SUB = 8
KP = 16
SHRINK = 2.0**-35

VMEM = pl.BlockSpec(memory_space=pltpu.VMEM)
HBM = pl.BlockSpec(memory_space=pltpu.HBM)


def f32(*shape):
    return jax.ShapeDtypeStruct(shape, jnp.float32)


def params():
    return pltpu.CompilerParams(vmem_limit_bytes=20 * 1024 * 1024)


def cost(flops):
    return pl.CostEstimate(flops=flops, bytes_accessed=0, transcendentals=0)


def up(n, m):
    return -(-n // m) * m


def colsum(x):
    return jnp.sum(x, axis=0, keepdims=True)


def unit(real, imag):
    scale = 1.0 / jnp.maximum(jnp.sqrt(real * real + imag * imag), FLOOR)
    return (real * scale, imag * scale)


def seat(pixels, reach):
    section, block = lax.axis_index("section"), lax.axis_index("pix")
    even = block % 2 == 0
    return (
        section, block, lax.axis_size("pix"), block * pixels,
        jnp.where(even, pixels, -reach), jnp.where(even, -reach, pixels),
    )


def half(h):
    return pl.ds(h * LANES, LANES)


def gather(start, idx_ref, pieces, xs_ref, hl_ref, zr_ref, zi_ref, add):
    count, rows, pixels = zr_ref.shape
    xs_ref[...] = jnp.zeros_like(xs_ref)
    at = 0
    place = []
    for piece, first in pieces:
        dates, _, width = piece.shape
        for c in range(2):
            xs_ref[pl.ds(c * rows, dates), pl.ds(at, width)] = piece[:, c]
        place.append(lax.broadcasted_iota(jnp.int32, (width, pixels), 0) + first)
        at += width
    place = jnp.concatenate(place, axis=0)
    high = xs_ref[...].astype(jnp.bfloat16)
    hl_ref[0 : 2 * rows] = high
    hl_ref[2 * rows : 4 * rows] = (xs_ref[...] - high.astype(jnp.float32)).astype(jnp.bfloat16)
    for k in range(count):
        near = idx_ref[k : k + 1, :] - start
        hot = jnp.where(place == near, 1.0, 0.0).astype(jnp.bfloat16)
        got = jnp.dot(hl_ref[...], hot, preferred_element_type=jnp.float32)
        zr = got[0:rows] + got[2 * rows : 3 * rows]
        zi = got[rows : 2 * rows] + got[3 * rows : 4 * rows]
        zr_ref[k] = zr_ref[k] + zr if add else zr
        zi_ref[k] = zi_ref[k] + zi if add else zi


def scale_dates(zr_ref, zi_ref):
    count, rows, pixels = zr_ref.shape
    for h in range(pixels // LANES):
        for r in range(0, rows, SUB):
            power = None
            for k in range(count):
                a = zr_ref[k, pl.ds(r, SUB), half(h)]
                b = zi_ref[k, pl.ds(r, SUB), half(h)]
                power = a * a + b * b if power is None else power + (a * a + b * b)
            scale = lax.rsqrt(jnp.maximum(power, 1.0))
            for k in range(count):
                zr_ref[k, pl.ds(r, SUB), half(h)] *= scale
                zi_ref[k, pl.ds(r, SUB), half(h)] *= scale


def merge_rows(parts):
    row = lax.broadcasted_iota(jnp.int32, (SUB, LANES), 0)
    for step in (4, 2, 1):
        low = jnp.bitwise_and(row, step) == 0
        other = jnp.bitwise_xor(row, step)
        n = len(parts) // 2
        out = []
        for i in range(n):
            a, b = parts[i], parts[i + n]
            far = jnp.take_along_axis(jnp.where(low, b, a), other, axis=0, mode="promise_in_bounds")
            out.append(jnp.where(low, a, b) + far)
        parts = out
    return parts[0]


def gram(pair_ref, zr_ref, zi_ref, own_ref, gr_ref, gi_ref, sum_ref, block=3):
    count, rows, pixels = zr_ref.shape
    zero = jnp.zeros((SUB, LANES), jnp.float32)
    for h in range(pixels // LANES):
        def load(k, r):
            if k == count:
                return (own_ref[pl.ds(r, SUB), half(h)], own_ref[pl.ds(rows + r, SUB), half(h)])
            return (zr_ref[k, pl.ds(r, SUB), half(h)], zi_ref[k, pl.ds(r, SUB), half(h)])

        for k0 in range(0, count, block):
            for l0 in range(k0, count + 1, block):
                pairs = [
                    (k, l)
                    for k in range(k0, min(k0 + block, count))
                    for l in range(l0, min(l0 + block, count + 1))
                    if l >= k
                ]
                acc = {}
                for r in range(0, rows, SUB):
                    val = {n: load(n, r) for n in sorted({n for p in pairs for n in p})}
                    minus = {k: val[k][0] - val[k][1] for k in {k for k, l in pairs if k != l}}
                    plus = {l: val[l][0] + val[l][1] for l in {l for k, l in pairs if k != l}}
                    for k, l in pairs:
                        new = [val[k][0] * val[l][0], val[k][1] * val[l][1]]
                        if k != l:
                            new.append(minus[k] * plus[l])
                        acc[k, l] = [x + y for x, y in zip(acc[k, l], new)] if r else new
                for k, l in pairs:
                    pair_ref[0, l, k] = acc[k, l][0] + acc[k, l][1]
                    pair_ref[1, l, k] = zero if k == l else acc[k, l][2] - (acc[k, l][0] - acc[k, l][1])
        for c, g_ref in ((0, gr_ref), (1, gi_ref)):
            for l in range(count + 1):
                for kt in range(KP // SUB):
                    ks = range(kt * SUB, kt * SUB + SUB)
                    if min(ks) > min(l, count - 1):
                        continue
                    parts = [pair_ref[c, l, k] if k <= min(l, count - 1) else zero for k in ks]
                    g_ref[l, h, pl.ds(kt * SUB, SUB), :] = merge_rows(parts)
        row = lax.broadcasted_iota(jnp.int32, (SUB, LANES), 0)
        for c, g_ref in ((0, gr_ref), (1, gi_ref)):
            for l in range(count):
                for kt in range(KP // SUB):
                    ks = list(range(kt * SUB, kt * SUB + SUB))
                    if max(ks) <= l:
                        continue
                    other = jnp.concatenate(
                        [g_ref[k, h, pl.ds(l, 1), :] if l < k < count else zero[0:1] for k in ks], axis=0
                    )
                    if c:
                        other = -other
                    if min(ks) <= l:
                        other = jnp.where(row + ks[0] <= l, g_ref[l, h, pl.ds(kt * SUB, SUB), :], other)
                    g_ref[l, h, pl.ds(kt * SUB, SUB), :] = other
        for c in range(2):
            tiles = []
            for k in range(KP):
                total = None
                if k <= count:
                    for r in range(0, rows, SUB):
                        v = load(k, r)[c]
                        total = v if total is None else total + v
                tiles.append(zero if total is None else total)
            for kt in range(KP // SUB):
                sum_ref[c, h, pl.ds(kt * SUB, SUB), :] = merge_rows(tiles[kt * SUB : kt * SUB + SUB])


def turns(gr_ref, gi_ref, g0, count):
    halves = gr_ref.shape[1]

    def product(b, g):
        acc = [list(x) for x in g]
        for l in range(count):
            for h in range(halves):
                br = jnp.broadcast_to(b[h][0][l : l + 1], (KP, LANES))
                bi = jnp.broadcast_to(b[h][1][l : l + 1], (KP, LANES))
                gr = gr_ref[l, h]
                gi = gi_ref[l, h]
                acc[h][0] = acc[h][0] + (gr * br - gi * bi)
                acc[h][1] = acc[h][1] + (gr * bi + gi * br)
        return acc

    def step(_, carry):
        b, g = carry
        t = product(b, g)
        return tuple((b[h][0] + t[h][0], b[h][1] + t[h][1]) for h in range(halves)), g

    g = tuple(g0)
    b = g
    b, g = lax.fori_loop(0, ITERS // 2 - 1, step, (b, g))
    b = tuple((x * SHRINK, y * SHRINK) for x, y in b)
    g = tuple((x * SHRINK, y * SHRINK) for x, y in g)
    b, g = lax.fori_loop(0, ITERS - ITERS // 2, step, (b, g))
    return b, g, product(b, g)


def solve(virtual, gr_ref, gi_ref, hr, hi, sum_ref, stack, beta_ref, state_ref):
    halves = gr_ref.shape[1]
    count = gr_ref.shape[0]
    first = 1.0 / math.sqrt(stack)
    g0 = []
    for h in range(halves):
        zr, zi = sum_ref[0, h], sum_ref[1, h]
        row = lax.broadcasted_iota(jnp.int32, (KP, LANES), 0)
        zr = jnp.where(row < count, zr, 0.0)
        zi = jnp.where(row < count, zi, 0.0)
        if virtual is not None:
            zr = zr + virtual[h][1][0]
            zi = zi + virtual[h][1][1]
        g0.append((zr * first, zi * -first))
    b, g, t = turns(gr_ref, gi_ref, g0, count)
    for h in range(halves):
        norm = colsum(b[h][0] * (g[h][0] + t[h][0]) + b[h][1] * (g[h][1] + t[h][1]))
        inv = lax.rsqrt(SHRINK * SHRINK + norm)
        br, bi = b[h][0] * inv, b[h][1] * inv
        a = inv * (SHRINK * first)
        xr, xi = hr[h], hi[h]
        sr, si = sum_ref[0, h][count : count + 1], sum_ref[1, h][count : count + 1]
        fr, fi = a, jnp.zeros_like(a)
        if virtual is not None:
            (wr, wi), (zr, zi) = virtual[h]
            xr, xi = xr + (zr * wr + zi * wi), xi + (zr * wi - zi * wr)
            sr, si = sr + wr, si + wi
            fr = a + colsum(zr * br - zi * bi)
            fi = colsum(zr * bi + zi * br)
        beta_ref[0, h] = br
        beta_ref[1, h] = bi
        fr, fi = unit(fr, fi)
        state_ref[0:1, half(h)] = a * sr + colsum(br * xr + bi * xi)
        state_ref[1:2, half(h)] = a * si + colsum(br * xi - bi * xr)
        state_ref[2:3, half(h)] = fr
        state_ref[3:4, half(h)] = fi
        state_ref[4:5, half(h)] = a
        state_ref[5:8, half(h)] = jnp.zeros((3, LANES), jnp.float32)


def own_kernel(idx_hbm, slc_hbm, near_ref, zr_ref, zi_ref, own_ref, idx_ref, slc_ref, hl_ref, sems):
    copies = [
        pltpu.make_async_copy(slc_hbm, slc_ref, sems.at[0]),
        pltpu.make_async_copy(idx_hbm, idx_ref, sems.at[1]),
    ]
    for copy in copies:
        copy.start()
    for copy in copies:
        copy.wait()
    _, _, _, start, near_at, _ = seat(slc_ref.shape[2], near_ref.shape[2])
    gather(start, idx_ref, ((slc_ref, 0), (near_ref, near_at)), own_ref, hl_ref, zr_ref, zi_ref, False)


def prepare_kernel(stack, first, idx_ref, far_ref, own_ref, *refs):
    refs = refs[2 if first else 7 :]
    zr_ref, zi_ref, gr_ref, gi_ref, sum_ref, beta_ref, state_ref = refs[:7]
    xs_ref, hl_ref, pair_ref = refs[-3:]

    section, _, _, start, _, far_at = seat(zr_ref.shape[2], far_ref.shape[2])

    @pl.when(section == 0 if first else section != 0)
    def _():
        count = zr_ref.shape[0]
        gather(start, idx_ref, ((far_ref, far_at),), xs_ref, hl_ref, zr_ref, zi_ref, True)
        scale_dates(zr_ref, zi_ref)
        gram(pair_ref, zr_ref, zi_ref, own_ref, gr_ref, gi_ref, sum_ref)
        if first:
            halves = gr_ref.shape[1]
            hr = [gr_ref[count, h] for h in range(halves)]
            hi = [gi_ref[count, h] for h in range(halves)]
            solve(None, gr_ref.at[0:count], gi_ref.at[0:count], hr, hi, sum_ref, stack, beta_ref, state_ref)
            refs[7][...] = state_ref[0:2]


def lane_take(x, i):
    return jnp.take_along_axis(x, i, axis=1, mode="promise_in_bounds")


def round_kernel(
    rnd, stack, idx_ref, low_ref, own_ref, high_ref,
    gr_ref, gi_ref, sum_ref, beta0_ref, state0_ref, *refs,
):
    last = len(refs) > 5
    if last:
        late, (comp_ref, *made), refs = refs[:3], refs[3:6], refs[6:]
        fr_ref, fi_ref, beta_ref, state_ref = refs
    else:
        beta_ref, state_ref, comp_ref, fr_ref, fi_ref = refs
    count = gr_ref.shape[0] - 1
    halves = gr_ref.shape[1]
    reach = low_ref.shape[1]
    beta_ref[...] = beta0_ref[...]
    state_ref[...] = state0_ref[...]
    section, _, _, start, _, _ = seat(own_ref.shape[1], reach)

    @pl.when(section == rnd)
    def _():
        tiles = []
        for ref in (low_ref, own_ref, high_ref):
            for t in range(ref.shape[1] // LANES):
                tiles.append([ref[c : c + 1, half(t)] for c in range(2)])
        virtual = []
        for h in range(halves):
            parts = []
            for kt in range(KP // SUB):
                rows = min(SUB, count - kt * SUB)
                raw = idx_ref[pl.ds(kt * SUB, rows), half(h)] - (start - reach)
                if rows < SUB:
                    raw = jnp.concatenate([raw, jnp.full((SUB - rows, LANES), -1, jnp.int32)], axis=0)
                lane = jnp.bitwise_and(raw, LANES - 1)
                tile = jnp.right_shift(raw, 7)
                both = []
                for c in range(2):
                    out = jnp.zeros((SUB, LANES), jnp.float32)
                    for n in range(h, h + 2 * reach // LANES + 1):
                        got = lane_take(jnp.broadcast_to(tiles[n][c], (SUB, LANES)), lane)
                        out = jnp.where(tile == n, got, out)
                    both.append(out)
                parts.append(both)
            zr = jnp.concatenate([p[0] for p in parts], axis=0)
            zi = jnp.concatenate([p[1] for p in parts], axis=0)
            scale = lax.rsqrt(jnp.maximum(colsum(zr * zr + zi * zi), 1.0))
            zr, zi = zr * scale, zi * scale
            own = tiles[reach // LANES + h]
            virtual.append((own, (zr, zi)))
            for l in range(count):
                br = jnp.broadcast_to(zr[l : l + 1], (KP, LANES))
                bi = jnp.broadcast_to(zi[l : l + 1], (KP, LANES))
                fr_ref[l, h] = gr_ref[l, h] + (zr * br + zi * bi)
                fi_ref[l, h] = gi_ref[l, h] + (zr * bi - zi * br)
        hr = [gr_ref[count, h] for h in range(halves)]
        hi = [gi_ref[count, h] for h in range(halves)]
        solve(virtual, fr_ref, fi_ref, hr, hi, sum_ref, stack, beta_ref, state_ref)

    comp_ref[...] = state_ref[0:2]
    if last:
        vectors(*late, beta_ref, state_ref, *made)


def slot_rows(halves):
    return 2 * halves + 1


def vectors(pixel_ref, zr_ref, zi_ref, beta_ref, state_ref, vec_ref, slot_ref):
    count, rows, pixels = zr_ref.shape
    dates = vec_ref.shape[1]
    halves = pixels // LANES
    _, _, _, start, _, _ = seat(pixels, 0)
    local = pixel_ref[...] - start
    lane = lax.broadcasted_iota(jnp.int32, (SUB, LANES), 1)
    row = lax.broadcasted_iota(jnp.int32, (SUB, LANES), 0)
    at_pixel = [jnp.zeros((SUB, LANES), jnp.float32) for _ in range(2)]
    for h in range(halves):
        a = state_ref[4:5, half(h)]
        acc_r = [jnp.broadcast_to(a, (SUB, LANES)) for _ in range(0, rows, SUB)]
        acc_i = [jnp.zeros((SUB, LANES), jnp.float32) for _ in range(0, rows, SUB)]
        for k in range(count):
            br = jnp.broadcast_to(beta_ref[0, h, k : k + 1, :], (SUB, LANES))
            bi = jnp.broadcast_to(beta_ref[1, h, k : k + 1, :], (SUB, LANES))
            for n, r in enumerate(range(0, rows, SUB)):
                zr = zr_ref[k, pl.ds(r, SUB), half(h)]
                zi = zi_ref[k, pl.ds(r, SUB), half(h)]
                acc_r[n] = acc_r[n] + (zr * br - zi * bi)
                acc_i[n] = acc_i[n] + (zr * bi + zi * br)
        for c, acc in ((0, acc_r), (1, acc_i)):
            whole = jnp.concatenate(acc, axis=0)
            vec_ref[c, :, half(h)] = whole[0:dates]
            wide = jnp.concatenate([whole, jnp.zeros((up(rows, LANES) - rows, LANES), jnp.float32)], axis=0)
            turned = jnp.transpose(wide)
            for r in range(0, LANES, SUB):
                at_pixel[c] = at_pixel[c] + jnp.where(row == local - (h * LANES + r), turned[r : r + SUB], 0.0)
    slot = [state_ref[2 + c : 3 + c, half(h)] for c in range(2) for h in range(halves)]
    mixed = colsum(at_pixel[0]) + pltpu.roll(jnp.broadcast_to(colsum(at_pixel[1]), (SUB, LANES)), LANES // 2, 1)[0:1]
    for c in range(2):
        picked = jnp.zeros((1, LANES), jnp.float32)
        for h in range(halves):
            picked = picked + jnp.where((lane == local - h * LANES)[0:1], state_ref[2 + c : 3 + c, half(h)], 0.0)
        f = jnp.sum(picked, axis=1, keepdims=True)
        mixed = jnp.where(lane[0:1] == LANES - 2 + c, jnp.broadcast_to(f, (1, LANES)), mixed)
    slot.append(mixed)
    for n in range(slot_ref.shape[0]):
        for m, one in enumerate(slot):
            slot_ref[n, m] = one


def finish_kernel(sections, pixel_ref, vec_ref, got_ref, comp_ref, out_ref, small_ref):
    small_ref[:, 0] = comp_ref[...]
    dates, pixels = vec_ref.shape[1:]
    section, mine, blocks, _, _, _ = seat(pixels, 0)
    halves = pixels // LANES
    one = jnp.ones((1, LANES), jnp.float32)
    lane = lax.broadcasted_iota(jnp.int32, (1, LANES), 1)

    def of_pixel(s):
        total = jnp.zeros((1, LANES), jnp.float32)
        for q in range(blocks):
            first = pixel_ref[0:1] - q * pixels
            here = jnp.logical_and(first >= 0, first < pixels)
            total = total + jnp.where(here, got_ref[s * blocks + q, 2 * halves], 0.0)
        return total

    datum = [(one, 0.0 * one) for _ in range(halves)]
    at_pixel = (one, 0.0 * one)
    for s in range(sections - 1, 0, -1):
        later = section < s
        own = [got_ref[s * blocks + mine, m] for m in range(2 * halves)]
        row = of_pixel(s)

        def times(d, fr, fi):
            fr = jnp.where(later, fr, 1.0)
            fi = jnp.where(later, fi, 0.0)
            return (d[0] * fr - d[1] * fi, d[0] * fi + d[1] * fr)

        for h in range(halves):
            datum[h] = times(datum[h], own[h], own[halves + h])
        f = [jnp.sum(jnp.where(lane == LANES - 2 + c, row, 0.0), axis=1, keepdims=True) for c in range(2)]
        at_pixel = times(at_pixel, *[jnp.broadcast_to(x, (1, LANES)) for x in f])
    vr = of_pixel(section)
    vi = pltpu.roll(jnp.broadcast_to(vr, (SUB, LANES)), LANES // 2, 1)[0:1]
    ur, ui = unit(vr * at_pixel[0] - vi * at_pixel[1], vr * at_pixel[1] + vi * at_pixel[0])
    gain = math.sqrt(dates + 1)
    ur = jnp.transpose(jnp.broadcast_to(ur * gain, (LANES, LANES)))[0:dates]
    ui = jnp.transpose(jnp.broadcast_to(ui * gain, (LANES, LANES)))[0:dates]
    for h in range(halves):
        wr = ur * datum[h][0] + ui * datum[h][1]
        wi = ur * datum[h][1] - ui * datum[h][0]
        vr = vec_ref[0, :, half(h)]
        vi = vec_ref[1, :, half(h)]
        out_ref[:, 0, half(h)] = vr * wr - vi * wi
        out_ref[:, 1, half(h)] = vr * wi + vi * wr


def on_device(slc, neighbours, reference_pixel):
    dates, pixels = slc.shape[1:]
    slc = jnp.transpose(slc, (1, 0, 2))
    count = neighbours.shape[0]
    reach = min(pixels, REACH_LIMIT)
    sections = lax.axis_size("section")
    blocks = lax.axis_size("pix")
    block = lax.axis_index("pix")
    stack = dates + 1
    halves = pixels // LANES
    rows = up(dates, SUB)

    even = block % 2 == 0

    def swap(first, upper):
        pairs = [(i, i + 1) for i in range(first, blocks - 1, 2)]
        pairs += [(j, i) for i, j in pairs]
        sent = slc
        if reach < pixels:
            sent = jnp.where(upper, slc[:, :, pixels - reach :], slc[:, :, :reach])
        return lax.ppermute(sent, "pix", pairs)

    near = swap(0, even)
    far = swap(1, ~even)

    made = [
        f32(count, rows, pixels), f32(count, rows, pixels),
        f32(count + 1, halves, KP, LANES), f32(count + 1, halves, KP, LANES),
        f32(2, halves, KP, LANES), f32(2, halves, KP, LANES), f32(SUB, pixels), f32(2, pixels),
    ]
    zr, zi, own, neighbours = pl.pallas_call(
        own_kernel,
        out_shape=made[:2] + [f32(2 * rows, pixels + reach), jax.ShapeDtypeStruct(neighbours.shape, jnp.int32)],
        in_specs=[HBM, HBM, VMEM],
        out_specs=[VMEM] * 4,
        scratch_shapes=[
            pltpu.VMEM((dates, 2, pixels), jnp.float32),
            pltpu.VMEM((4 * rows, pixels + reach), jnp.bfloat16),
            pltpu.SemaphoreType.DMA((2,)),
        ],
        compiler_params=params(),
        cost_estimate=cost(2 * 4 * rows * pixels * (pixels + reach) * count),
        name="own",
    )(pltpu.with_memory_space_constraint(neighbours, pltpu.HBM), pltpu.with_memory_space_constraint(slc, pltpu.HBM), near)

    def prepare(first, carried):
        return pl.pallas_call(
            functools.partial(prepare_kernel, stack, first),
            out_shape=made[: 8 if first else 7],
            in_specs=[VMEM] * (3 + len(carried)),
            out_specs=[VMEM] * (8 if first else 7),
            scratch_shapes=[
                pltpu.VMEM((2 * rows, reach), jnp.float32),
                pltpu.VMEM((4 * rows, reach), jnp.bfloat16),
                pltpu.VMEM((2, count + 1, count, SUB, LANES), jnp.float32),
            ],
            input_output_aliases={3 + n: n for n in range(len(carried))},
            compiler_params=params(),
            cost_estimate=cost(50 * 12 * rows * reach * pixels * count),
        )(neighbours, far, own, *carried)

    *made_0, comp = prepare(True, (zr, zi))
    zr, zi, gr, gi, sums, beta, state = prepare(False, made_0)

    for rnd in range(1, sections):
        def hop(shift):
            pairs = [
                ((rnd - 1) * blocks + q, rnd * blocks + q + shift)
                for q in range(blocks)
                if 0 <= q + shift < blocks
            ]
            return lax.ppermute(comp, ("section", "pix"), pairs)

        last = rnd == sections - 1
        late, specs = (), []
        scratch = [pltpu.VMEM((count, halves, KP, LANES), jnp.float32)] * 2
        outs = [f32(2, halves, KP, LANES), f32(SUB, pixels), f32(2, pixels)]
        if last:
            late, specs = (ref_at, zr, zi), [VMEM] * 3
            scratch += [pltpu.VMEM(o.shape, o.dtype) for o in outs[:2]]
            outs = outs[2:] + [f32(2, dates, pixels), f32(sections * blocks, slot_rows(halves), 1, LANES)]
        made = pl.pallas_call(
            functools.partial(round_kernel, rnd, stack),
            out_shape=outs,
            in_specs=[VMEM] * 9 + specs,
            out_specs=[VMEM] * 3,
            scratch_shapes=scratch,
            compiler_params=params(),
        )(neighbours, hop(1)[:, pixels - reach :], hop(0), hop(-1)[:, :reach], gr, gi, sums, beta, state, *late)
        if last:
            comp, vec, sent = made
        else:
            beta, state, comp = made
        if rnd == 1:
            pixel = lax.optimization_barrier((reference_pixel, comp))[0][0]
            ref_at = jnp.full((SUB, LANES), pixel, jnp.int32)

    got = lax.all_to_all(sent, ("section", "pix"), 0, 0, tiled=True)
    out, small = pl.pallas_call(
        functools.partial(finish_kernel, sections),
        out_shape=[f32(dates, 2, pixels), f32(2, 1, pixels)],
        in_specs=[VMEM] * 4,
        out_specs=[VMEM] * 2,
        compiler_params=params(),
        name="finish",
    )(ref_at, vec, got, comp)
    return (jnp.transpose(out, (1, 0, 2)), small)


def solution(mesh):
    return jax.shard_map(
        on_device,
        mesh=mesh,
        in_specs=(P(None, "section", "pix"), P(None, "pix"), P()),
        out_specs=(P(None, "section", "pix"), P(None, "section", "pix")),
        check_vma=False,
    )
```

```python
import functools
import math

import jax
import jax.numpy as jnp
from jax import lax
from jax.experimental import pallas as pl
from jax.experimental.pallas import tpu as pltpu
from jax.sharding import PartitionSpec as P


ITERS = 16
FLOOR = 0.05
REACH_LIMIT = 256
LANES = 128
SUB = 8
KP = 16
Z_LANE, Z_STEP = 20, 54
SHRINK = 2.0**-35

VMEM = pl.BlockSpec(memory_space=pltpu.VMEM)
HBM = pl.BlockSpec(memory_space=pltpu.HBM)


def f32(*shape):
    return jax.ShapeDtypeStruct(shape, jnp.float32)


def params():
    return pltpu.CompilerParams(vmem_limit_bytes=20 * 1024 * 1024)


def cost(flops):
    return pl.CostEstimate(flops=flops, bytes_accessed=0, transcendentals=0)


def up(n, m):
    return -(-n // m) * m


def colsum(x):
    return jnp.sum(x, axis=0, keepdims=True)


def unit(real, imag):
    scale = 1.0 / jnp.maximum(jnp.sqrt(real * real + imag * imag), FLOOR)
    return (real * scale, imag * scale)


def seat(pixels, reach):
    section, block = lax.axis_index("section"), lax.axis_index("pix")
    even = block % 2 == 0
    return (
        section, block, lax.axis_size("pix"), block * pixels,
        jnp.where(even, pixels, -reach), jnp.where(even, -reach, pixels),
    )


def half(h):
    return pl.ds(h * LANES, LANES)


def gather(start, idx_ref, pieces, xs_ref, hl_ref, zr_ref, zi_ref, add):
    count, rows, pixels = zr_ref.shape
    xs_ref[...] = jnp.zeros_like(xs_ref)
    at = 0
    place = []
    for piece, first in pieces:
        dates, _, width = piece.shape
        for c in range(2):
            xs_ref[pl.ds(c * rows, dates), pl.ds(at, width)] = piece[:, c]
        place.append(lax.broadcasted_iota(jnp.int32, (width, pixels), 0) + first)
        at += width
    place = jnp.concatenate(place, axis=0)
    high = xs_ref[...].astype(jnp.bfloat16)
    hl_ref[0 : 2 * rows] = high
    hl_ref[2 * rows : 4 * rows] = (xs_ref[...] - high.astype(jnp.float32)).astype(jnp.bfloat16)
    for k in range(count):
        near = idx_ref[k : k + 1, :] - start
        hot = jnp.where(place == near, 1.0, 0.0).astype(jnp.bfloat16)
        got = jnp.dot(hl_ref[...], hot, preferred_element_type=jnp.float32)
        zr = got[0:rows] + got[2 * rows : 3 * rows]
        zi = got[rows : 2 * rows] + got[3 * rows : 4 * rows]
        zr_ref[k] = zr_ref[k] + zr if add else zr
        zi_ref[k] = zi_ref[k] + zi if add else zi


def scale_dates(zr_ref, zi_ref):
    count, rows, pixels = zr_ref.shape
    for h in range(pixels // LANES):
        for r in range(0, rows, SUB):
            power = None
            for k in range(count):
                a = zr_ref[k, pl.ds(r, SUB), half(h)]
                b = zi_ref[k, pl.ds(r, SUB), half(h)]
                power = a * a + b * b if power is None else power + (a * a + b * b)
            scale = lax.rsqrt(jnp.maximum(power, 1.0))
            for k in range(count):
                zr_ref[k, pl.ds(r, SUB), half(h)] *= scale
                zi_ref[k, pl.ds(r, SUB), half(h)] *= scale


def merge_rows(parts):
    row = lax.broadcasted_iota(jnp.int32, (SUB, LANES), 0)
    for step in (4, 2, 1):
        low = jnp.bitwise_and(row, step) == 0
        other = jnp.bitwise_xor(row, step)
        n = len(parts) // 2
        out = []
        for i in range(n):
            a, b = parts[i], parts[i + n]
            far = jnp.take_along_axis(jnp.where(low, b, a), other, axis=0, mode="promise_in_bounds")
            out.append(jnp.where(low, a, b) + far)
        parts = out
    return parts[0]


def gram(pair_ref, zr_ref, zi_ref, own_ref, gr_ref, gi_ref, sum_ref, block=3):
    count, rows, pixels = zr_ref.shape
    zero = jnp.zeros((SUB, LANES), jnp.float32)
    for h in range(pixels // LANES):
        def load(k, r):
            if k == count:
                return (own_ref[pl.ds(r, SUB), half(h)], own_ref[pl.ds(rows + r, SUB), half(h)])
            return (zr_ref[k, pl.ds(r, SUB), half(h)], zi_ref[k, pl.ds(r, SUB), half(h)])

        for k0 in range(0, count, block):
            for l0 in range(k0, count + 1, block):
                pairs = [
                    (k, l)
                    for k in range(k0, min(k0 + block, count))
                    for l in range(l0, min(l0 + block, count + 1))
                    if l >= k
                ]
                acc = {}
                for r in range(0, rows, SUB):
                    val = {n: load(n, r) for n in sorted({n for p in pairs for n in p})}
                    minus = {k: val[k][0] - val[k][1] for k in {k for k, l in pairs if k != l}}
                    plus = {l: val[l][0] + val[l][1] for l in {l for k, l in pairs if k != l}}
                    for k, l in pairs:
                        new = [val[k][0] * val[l][0], val[k][1] * val[l][1]]
                        if k != l:
                            new.append(minus[k] * plus[l])
                        acc[k, l] = [x + y for x, y in zip(acc[k, l], new)] if r else new
                for k, l in pairs:
                    pair_ref[0, l, k] = acc[k, l][0] + acc[k, l][1]
                    pair_ref[1, l, k] = zero if k == l else acc[k, l][2] - (acc[k, l][0] - acc[k, l][1])
        for c, g_ref in ((0, gr_ref), (1, gi_ref)):
            for l in range(count + 1):
                for kt in range(KP // SUB):
                    ks = range(kt * SUB, kt * SUB + SUB)
                    if min(ks) > min(l, count - 1):
                        continue
                    parts = [pair_ref[c, l, k] if k <= min(l, count - 1) else zero for k in ks]
                    g_ref[l, h, pl.ds(kt * SUB, SUB), :] = merge_rows(parts)
        row = lax.broadcasted_iota(jnp.int32, (SUB, LANES), 0)
        for c, g_ref in ((0, gr_ref), (1, gi_ref)):
            for l in range(count):
                for kt in range(KP // SUB):
                    ks = list(range(kt * SUB, kt * SUB + SUB))
                    if max(ks) <= l:
                        continue
                    other = jnp.concatenate(
                        [g_ref[k, h, pl.ds(l, 1), :] if l < k < count else zero[0:1] for k in ks], axis=0
                    )
                    if c:
                        other = -other
                    if min(ks) <= l:
                        other = jnp.where(row + ks[0] <= l, g_ref[l, h, pl.ds(kt * SUB, SUB), :], other)
                    g_ref[l, h, pl.ds(kt * SUB, SUB), :] = other
        for c in range(2):
            tiles = []
            for k in range(KP):
                total = None
                if k <= count:
                    for r in range(0, rows, SUB):
                        v = load(k, r)[c]
                        total = v if total is None else total + v
                tiles.append(zero if total is None else total)
            for kt in range(KP // SUB):
                sum_ref[c, h, pl.ds(kt * SUB, SUB), :] = merge_rows(tiles[kt * SUB : kt * SUB + SUB])


def turns(gr_ref, gi_ref, g0, count):
    halves = gr_ref.shape[1]

    def product(b, g):
        acc = [list(x) for x in g]
        for l in range(count):
            for h in range(halves):
                br = jnp.broadcast_to(b[h][0][l : l + 1], (KP, LANES))
                bi = jnp.broadcast_to(b[h][1][l : l + 1], (KP, LANES))
                gr = gr_ref[l, h]
                gi = gi_ref[l, h]
                acc[h][0] = acc[h][0] + (gr * br - gi * bi)
                acc[h][1] = acc[h][1] + (gr * bi + gi * br)
        return acc

    def step(_, carry):
        b, g = carry
        t = product(b, g)
        return tuple((b[h][0] + t[h][0], b[h][1] + t[h][1]) for h in range(halves)), g

    g = tuple(g0)
    b = g
    b, g = lax.fori_loop(0, ITERS // 2 - 1, step, (b, g))
    b = tuple((x * SHRINK, y * SHRINK) for x, y in b)
    g = tuple((x * SHRINK, y * SHRINK) for x, y in g)
    b, g = lax.fori_loop(0, ITERS - ITERS // 2, step, (b, g))
    return b, g, product(b, g)


def solve(virtual, gr_ref, gi_ref, hr, hi, sums, stack, beta_ref, state_ref):
    halves = gr_ref.shape[1]
    count = gr_ref.shape[0]
    first = 1.0 / math.sqrt(stack)
    g0 = []
    for h in range(halves):
        zr, zi = sums[h]
        row = lax.broadcasted_iota(jnp.int32, (KP, LANES), 0)
        zr = jnp.where(row < count, zr, 0.0)
        zi = jnp.where(row < count, zi, 0.0)
        if virtual is not None:
            zr = zr + virtual[h][1][0]
            zi = zi + virtual[h][1][1]
        g0.append((zr * first, zi * -first))
    b, g, t = turns(gr_ref, gi_ref, g0, count)
    for h in range(halves):
        norm = colsum(b[h][0] * (g[h][0] + t[h][0]) + b[h][1] * (g[h][1] + t[h][1]))
        inv = lax.rsqrt(SHRINK * SHRINK + norm)
        br, bi = b[h][0] * inv, b[h][1] * inv
        a = inv * (SHRINK * first)
        xr, xi = hr[h], hi[h]
        sr, si = (x[count : count + 1] for x in sums[h])
        fr, fi = a, jnp.zeros_like(a)
        if virtual is not None:
            (wr, wi), (zr, zi) = virtual[h]
            xr, xi = xr + (zr * wr + zi * wi), xi + (zr * wi - zi * wr)
            sr, si = sr + wr, si + wi
            fr = a + colsum(zr * br - zi * bi)
            fi = colsum(zr * bi + zi * br)
        beta_ref[0, h] = br
        beta_ref[1, h] = bi
        fr, fi = unit(fr, fi)
        state_ref[0:1, half(h)] = a * sr + colsum(br * xr + bi * xi)
        state_ref[1:2, half(h)] = a * si + colsum(br * xi - bi * xr)
        state_ref[2:3, half(h)] = fr
        state_ref[3:4, half(h)] = fi
        state_ref[4:5, half(h)] = a
        state_ref[5:8, half(h)] = jnp.zeros((3, LANES), jnp.float32)


def own_kernel(idx_hbm, slc_hbm, near_ref, zr_ref, zi_ref, own_ref, idx_ref, slc_ref, hl_ref, sems):
    copies = [
        pltpu.make_async_copy(slc_hbm, slc_ref, sems.at[0]),
        pltpu.make_async_copy(idx_hbm, idx_ref, sems.at[1]),
    ]
    for copy in copies:
        copy.start()
    for copy in copies:
        copy.wait()
    _, _, _, start, near_at, _ = seat(slc_ref.shape[2], near_ref.shape[2])
    gather(start, idx_ref, ((slc_ref, 0), (near_ref, near_at)), own_ref, hl_ref, zr_ref, zi_ref, False)


def prepare_kernel(stack, first, idx_ref, far_ref, own_ref, *refs):
    if not first:
        pixel_ref, refs = refs[0], refs[1:]
    refs = refs[2 if first else 7 :]
    zr_ref, zi_ref, gr_ref, gi_ref, sum_ref, beta_ref, state_ref = refs[:7]
    xs_ref, hl_ref, pair_ref = refs[-3:]

    section, _, _, start, _, far_at = seat(zr_ref.shape[2], far_ref.shape[2])

    @pl.when(section == 0 if first else section != 0)
    def _():
        count = zr_ref.shape[0]
        gather(start, idx_ref, ((far_ref, far_at),), xs_ref, hl_ref, zr_ref, zi_ref, True)
        scale_dates(zr_ref, zi_ref)
        gram(pair_ref, zr_ref, zi_ref, own_ref, gr_ref, gi_ref, sum_ref)
        if first:
            halves = gr_ref.shape[1]
            hr = [gr_ref[count, h] for h in range(halves)]
            hi = [gi_ref[count, h] for h in range(halves)]
            sums = [(sum_ref[0, h], sum_ref[1, h]) for h in range(halves)]
            solve(None, gr_ref.at[0:count], gi_ref.at[0:count], hr, hi, sums, stack, beta_ref, state_ref)
            refs[7][...] = state_ref[0:2]

    if not first:

        @pl.when(section == lax.axis_size("section") - 1)
        def _():
            fold(start, pixel_ref, idx_ref, zr_ref, zi_ref, gr_ref, gi_ref, sum_ref, refs[7], refs[8])


def fold(start, pixel_ref, idx_ref, zr_ref, zi_ref, gr_ref, gi_ref, sum_ref, fold_ref, tile_ref):
    count, rows, pixels = zr_ref.shape
    halves = pixels // LANES
    k_row = lax.broadcasted_iota(jnp.int32, (KP, LANES), 0)
    lane = lax.broadcasted_iota(jnp.int32, (KP, LANES), 1)
    local = pixel_ref[...] - start
    hit = [lax.broadcasted_iota(jnp.int32, (SUB, LANES), 1) == local - h * LANES for h in range(halves)]

    def column(parts):
        total = None
        for h, part in enumerate(parts):
            mask = jnp.concatenate([hit[h]] * (part.shape[0] // SUB), axis=0)
            part = jnp.where(mask, part, 0.0)
            total = part if total is None else total + part
        return jnp.broadcast_to(jnp.sum(total, axis=1, keepdims=True), total.shape)

    tile = jnp.zeros((KP, LANES), jnp.float32)
    for l in range(count + 2):
        parts = []
        for h in range(halves):
            if l < count:
                part = jnp.where(k_row <= l, gr_ref[l, h], gi_ref[l, h])
            else:
                part = sum_ref[l - count, h]
            fold_ref[l, h] = part
            parts.append(part)
        tile = jnp.where(lane == (l if l < count else KP + l - count), column(parts), tile)
    pad = jnp.zeros((KP - count, LANES), jnp.float32)
    near = [jnp.concatenate([idx_ref[:, half(h)].astype(jnp.float32), pad], axis=0) for h in range(halves)]
    tile = jnp.where(lane == KP + 2, column(near), tile)
    wide = lax.broadcasted_iota(jnp.int32, (rows, LANES), 1)
    empty = jnp.zeros((LANES - rows, LANES), jnp.float32)
    for c, ref in ((0, zr_ref), (1, zi_ref)):
        both = jnp.zeros((rows, LANES), jnp.float32)
        for k in range(count):
            both = jnp.where(wide == k, column([ref[k, :, half(h)] for h in range(halves)]), both)
        turned = jnp.transpose(jnp.concatenate([both, empty], axis=0))[0:KP]
        at = Z_LANE + c * Z_STEP
        tile = jnp.where(jnp.logical_and(lane >= at, lane < at + Z_STEP), pltpu.roll(turned, at, 1), tile)
    tile_ref[...] = tile


def lane_take(x, i):
    return jnp.take_along_axis(x, i, axis=1, mode="promise_in_bounds")


def scaled(own, zr, zi):
    scale = lax.rsqrt(jnp.maximum(colsum(zr * zr + zi * zi), 1.0))
    return own, (zr * scale, zi * scale)


def take_virtual(idx_ref, base, reach, tiles, halves, count):
    virtual = []
    for h in range(halves):
        parts = []
        for kt in range(KP // SUB):
            rows = min(SUB, count - kt * SUB)
            raw = idx_ref[pl.ds(kt * SUB, rows), half(h)] - base
            if rows < SUB:
                raw = jnp.concatenate([raw, jnp.full((SUB - rows, LANES), -1, jnp.int32)], axis=0)
            lane = jnp.bitwise_and(raw, LANES - 1)
            tile = jnp.right_shift(raw, 7)
            both = []
            for c in range(2):
                out = jnp.zeros((SUB, LANES), jnp.float32)
                for n in range(h, h + 2 * reach // LANES + 1):
                    got = lane_take(jnp.broadcast_to(tiles[n][c], (SUB, LANES)), lane)
                    out = jnp.where(tile == n, got, out)
                both.append(out)
            parts.append(both)
        zr = jnp.concatenate([p[0] for p in parts], axis=0)
        zi = jnp.concatenate([p[1] for p in parts], axis=0)
        virtual.append(scaled(tiles[reach // LANES + h], zr, zi))
    return virtual


def update(virtual, gr_ref, gi_ref, fr_ref, fi_ref):
    for h, (_, (zr, zi)) in enumerate(virtual):
        for l in range(fr_ref.shape[0]):
            br = jnp.broadcast_to(zr[l : l + 1], (KP, LANES))
            bi = jnp.broadcast_to(zi[l : l + 1], (KP, LANES))
            fr_ref[l, h] = gr_ref[l, h] + (zr * br + zi * bi)
            fi_ref[l, h] = gi_ref[l, h] + (zr * bi - zi * br)


def round_kernel(
    rnd, stack, idx_ref, low_ref, own_ref, high_ref,
    gr_ref, gi_ref, sum_ref, beta0_ref, state0_ref, *refs,
):
    last = len(refs) > 5
    if last:
        late, (comp_ref, *made), refs = refs[:4], refs[4:7], refs[7:]
        fr_ref, fi_ref, beta_ref, state_ref = refs
    else:
        beta_ref, state_ref, comp_ref, fr_ref, fi_ref = refs
    count = gr_ref.shape[0] - 1
    halves = gr_ref.shape[1]
    reach = low_ref.shape[1]
    beta_ref[...] = beta0_ref[...]
    state_ref[...] = state0_ref[...]
    section, _, _, start, _, _ = seat(own_ref.shape[1], reach)

    @pl.when(section == rnd)
    def _():
        tiles = []
        for ref in (low_ref, own_ref, high_ref):
            for t in range(ref.shape[1] // LANES):
                tiles.append([ref[c : c + 1, half(t)] for c in range(2)])
        virtual = take_virtual(idx_ref, start - reach, reach, tiles, halves, count)
        update(virtual, gr_ref, gi_ref, fr_ref, fi_ref)
        hr = [gr_ref[count, h] for h in range(halves)]
        hi = [gi_ref[count, h] for h in range(halves)]
        sums = [(sum_ref[0, h], sum_ref[1, h]) for h in range(halves)]
        solve(virtual, fr_ref, fi_ref, hr, hi, sums, stack, beta_ref, state_ref)

    comp_ref[...] = state_ref[0:2]
    if last:
        vectors(*late, beta_ref, state_ref, *made)


def slot_rows(halves):
    return 4 * halves + 1


def make_vectors(zr_ref, zi_ref, beta_ref, state_ref, vec_ref):
    count, rows, pixels = zr_ref.shape
    dates = vec_ref.shape[1]
    out = [[], []]
    for h in range(pixels // LANES):
        a = state_ref[4:5, half(h)]
        acc_r = [jnp.broadcast_to(a, (SUB, LANES)) for _ in range(0, rows, SUB)]
        acc_i = [jnp.zeros((SUB, LANES), jnp.float32) for _ in range(0, rows, SUB)]
        for k in range(count):
            br = jnp.broadcast_to(beta_ref[0, h, k : k + 1, :], (SUB, LANES))
            bi = jnp.broadcast_to(beta_ref[1, h, k : k + 1, :], (SUB, LANES))
            for n, r in enumerate(range(0, rows, SUB)):
                zr = zr_ref[k, pl.ds(r, SUB), half(h)]
                zi = zi_ref[k, pl.ds(r, SUB), half(h)]
                acc_r[n] = acc_r[n] + (zr * br - zi * bi)
                acc_i[n] = acc_i[n] + (zr * bi + zi * br)
        for c, acc in ((0, acc_r), (1, acc_i)):
            whole = jnp.concatenate(acc, axis=0)
            vec_ref[c, :, half(h)] = whole[0:dates]
            out[c].append(whole)
    return out


def vectors(pixel_ref, zr_ref, zi_ref, tile_ref, beta_ref, state_ref, vec_ref, slot_ref):
    _, rows, pixels = zr_ref.shape
    halves = pixels // LANES
    section, block, blocks, start, _, _ = seat(pixels, 0)

    @pl.when(section < lax.axis_size("section") - 1)
    def _():
        local = pixel_ref[...] - start
        lane = lax.broadcasted_iota(jnp.int32, (SUB, LANES), 1)
        row = lax.broadcasted_iota(jnp.int32, (SUB, LANES), 0)
        at_pixel = [jnp.zeros((SUB, LANES), jnp.float32) for _ in range(2)]
        vecs = make_vectors(zr_ref, zi_ref, beta_ref, state_ref, vec_ref)
        for c in range(2):
            for h in range(halves):
                empty = jnp.zeros((LANES - rows, LANES), jnp.float32)
                turned = jnp.transpose(jnp.concatenate([vecs[c][h], empty], axis=0))
                for r in range(0, LANES, SUB):
                    at_pixel[c] = at_pixel[c] + jnp.where(row == local - (h * LANES + r), turned[r : r + SUB], 0.0)
        slot = [state_ref[c : c + 1, half(h)] for c in range(4) for h in range(halves)]
        mixed = colsum(at_pixel[0]) + pltpu.roll(jnp.broadcast_to(colsum(at_pixel[1]), (SUB, LANES)), LANES // 2, 1)[0:1]
        for c in range(2):
            picked = jnp.zeros((1, LANES), jnp.float32)
            for h in range(halves):
                picked = picked + jnp.where((lane == local - h * LANES)[0:1], state_ref[2 + c : 3 + c, half(h)], 0.0)
            f = jnp.sum(picked, axis=1, keepdims=True)
            mixed = jnp.where(lane[0:1] == LANES - 2 + c, jnp.broadcast_to(f, (1, LANES)), mixed)
        slot.append(mixed)
        for n in range(slot_ref.shape[0]):
            for m, one in enumerate(slot):
                slot_ref[n, m] = one

    @pl.when(section == lax.axis_size("section") - 1)
    def _():
        piece = up(KP, blocks) // blocks
        for i in range(piece):
            at = jnp.minimum(block * piece + i, KP - 1)
            one = tile_ref[pl.ds(at, 1), :]
            for n in range(slot_ref.shape[0]):
                slot_ref[n, i] = one


def unfold(fold_ref, fr_ref, fi_ref):
    count = fr_ref.shape[0]
    k_row = lax.broadcasted_iota(jnp.int32, (KP, LANES), 0)
    for h in range(fold_ref.shape[1]):
        for l in range(count):
            straight = fold_ref[l, h]
            turned = jnp.concatenate(
                [fold_ref[k, h, pl.ds(l, 1), :] for k in range(count)] + [jnp.zeros((KP - count, LANES), jnp.float32)], axis=0
            )
            fr_ref[l, h] = jnp.where(k_row <= l, straight, turned)
            fi_ref[l, h] = jnp.where(k_row > l, straight, jnp.where(k_row < l, -turned, 0.0))


def finish_kernel(
    sections, stack, pixel_ref, idx_ref, got_ref, vec0_ref, comp0_ref, zr_ref, zi_ref, gr_ref, gi_ref, sum_ref, *refs
):
    folds, (out_ref, small_ref), refs = refs[:sections], refs[sections : sections + 2], refs[sections + 2 :]
    fr_ref, fi_ref, add_ref, beta_ref, state_ref, vec_ref = refs
    dates, pixels = vec_ref.shape[1:]
    count = zr_ref.shape[0]
    section, mine, blocks, start, _, _ = seat(pixels, 0)
    halves = pixels // LANES
    final = sections - 1
    reach = min(pixels, REACH_LIMIT)

    for s in range(sections):

        @pl.when(section == s)
        def _(s=s):
            unfold(folds[s], fr_ref, fi_ref)
            for c in range(2):
                for h in range(halves):
                    add_ref[c, h] = folds[s][count + c, h]

    piece = up(KP, blocks) // blocks
    tile = [got_ref[final * blocks + n // piece, n % piece] for n in range(KP)]
    tile = jnp.concatenate(tile, axis=0)
    k_row = lax.broadcasted_iota(jnp.int32, (KP, LANES), 0)
    lane = lax.broadcasted_iota(jnp.int32, (KP, LANES), 1)
    turned = jnp.transpose(jnp.concatenate([tile, jnp.zeros((LANES - KP, LANES), jnp.float32)], axis=0))[0:KP]
    real = jnp.where(k_row <= lane, tile, turned)
    imag = jnp.where(k_row > lane, tile, jnp.where(k_row < lane, -turned, 0.0))

    def spread(x, l):
        return jnp.broadcast_to(x[:, l : l + 1], (KP, LANES))

    for l in range(count):
        fr_ref[l, halves] = spread(real, l)
        fi_ref[l, halves] = spread(imag, l)
    sums = [(add_ref[0, h], add_ref[1, h]) for h in range(halves)] + [(spread(tile, KP), spread(tile, KP + 1))]

    before = final - 1
    tiles = []
    per = reach // LANES
    low, high = jnp.maximum(mine - 1, 0), jnp.minimum(mine + 1, blocks - 1)
    for at, which in ((low, range(halves - per, halves)), (mine, range(halves)), (high, range(per))):
        for h in which:
            tiles.append([got_ref[before * blocks + at, c * halves + h] for c in range(2)])
    virtual = take_virtual(idx_ref, start - reach, reach, tiles, halves, count)
    near = spread(tile, KP + 2).astype(jnp.int32)
    total = [jnp.zeros((KP, LANES), jnp.float32) for _ in range(2)]
    for q in range(blocks):
        for h in range(halves):
            hit = lane == near - (q * pixels + h * LANES)
            for c in range(2):
                total[c] = total[c] + jnp.where(hit, got_ref[before * blocks + q, c * halves + h], 0.0)
    total = [jnp.broadcast_to(jnp.sum(x, axis=1, keepdims=True), (KP, LANES)) for x in total]
    total = [jnp.where(k_row < count, x, 0.0) for x in total]
    virtual.append(scaled([x[0:1] for x in total], *total))
    update(virtual, fr_ref, fi_ref, fr_ref, fi_ref)

    zero = jnp.zeros((KP, LANES), jnp.float32)
    hr = [gr_ref[count, h] for h in range(halves)] + [zero]
    hi = [gi_ref[count, h] for h in range(halves)] + [zero]
    solve(virtual, fr_ref, fi_ref, hr, hi, sums, stack, beta_ref, state_ref)
    is_final = section == final
    for c in range(2):
        small_ref[c] = jnp.where(is_final, state_ref[c : c + 1, 0:pixels], comp0_ref[c : c + 1])

    def of_pixel(s):
        total = jnp.zeros((1, LANES), jnp.float32)
        for q in range(blocks):
            first = pixel_ref[0:1] - q * pixels
            here = jnp.logical_and(first >= 0, first < pixels)
            total = total + jnp.where(here, got_ref[s * blocks + q, 4 * halves], 0.0)
        return total

    def times(d, later, fr, fi):
        fr = jnp.where(later, fr, 1.0)
        fi = jnp.where(later, fi, 0.0)
        return (d[0] * fr - d[1] * fi, d[0] * fi + d[1] * fr)

    one = jnp.ones((1, LANES), jnp.float32)
    datum = [(one, 0.0 * one) for _ in range(halves + 1)]
    for h in range(halves + 1):
        datum[h] = times(datum[h], section < final, state_ref[2:3, half(h)], state_ref[3:4, half(h)])
    for s in range(final - 1, 0, -1):
        later = section < s
        own = [got_ref[s * blocks + mine, 2 * halves + m] for m in range(2 * halves)]
        row = of_pixel(s)
        for h in range(halves):
            datum[h] = times(datum[h], later, own[h], own[halves + h])
        f = [jnp.sum(jnp.where(lane[0:1] == LANES - 2 + c, row, 0.0), axis=1, keepdims=True) for c in range(2)]
        datum[halves] = times(datum[halves], later, *[jnp.broadcast_to(x, (1, LANES)) for x in f])

    zr = pltpu.roll(tile, LANES - Z_LANE, 1)
    zi = pltpu.roll(tile, LANES - Z_LANE - Z_STEP, 1)
    br, bi = beta_ref[0, halves], beta_ref[1, halves]
    zr, zi = jnp.where(k_row < count, zr, 0.0), jnp.where(k_row < count, zi, 0.0)
    last_r = state_ref[4:5, half(halves)] + colsum(zr * br - zi * bi)
    last_i = colsum(zr * bi + zi * br)
    row = of_pixel(jnp.minimum(section, final - 1))
    vr = jnp.where(is_final, last_r, row)
    vi = jnp.where(is_final, last_i, pltpu.roll(jnp.broadcast_to(row, (SUB, LANES)), LANES // 2, 1)[0:1])
    dr, di = datum[halves]
    ur, ui = unit(vr * dr - vi * di, vr * di + vi * dr)
    gain = math.sqrt(dates + 1)
    ur = jnp.transpose(jnp.broadcast_to(ur * gain, (LANES, LANES)))[0:dates]
    ui = jnp.transpose(jnp.broadcast_to(ui * gain, (LANES, LANES)))[0:dates]

    @pl.when(is_final)
    def _():
        make_vectors(zr_ref, zi_ref, beta_ref, state_ref, vec_ref)

    for h in range(halves):
        wr = ur * datum[h][0] + ui * datum[h][1]
        wi = ur * datum[h][1] - ui * datum[h][0]
        vr = jnp.where(is_final, vec_ref[0, :, half(h)], vec0_ref[0, :, half(h)])
        vi = jnp.where(is_final, vec_ref[1, :, half(h)], vec0_ref[1, :, half(h)])
        out_ref[:, 0, half(h)] = vr * wr - vi * wi
        out_ref[:, 1, half(h)] = vr * wi + vi * wr


def on_device(slc, neighbours, reference_pixel):
    dates, pixels = slc.shape[1:]
    slc = jnp.transpose(slc, (1, 0, 2))
    count = neighbours.shape[0]
    reach = min(pixels, REACH_LIMIT)
    sections = lax.axis_size("section")
    blocks = lax.axis_size("pix")
    block = lax.axis_index("pix")
    stack = dates + 1
    halves = pixels // LANES
    rows = up(dates, SUB)

    even = block % 2 == 0

    def swap(first, upper):
        pairs = [(i, i + 1) for i in range(first, blocks - 1, 2)]
        pairs += [(j, i) for i, j in pairs]
        sent = slc
        if reach < pixels:
            sent = jnp.where(upper, slc[:, :, pixels - reach :], slc[:, :, :reach])
        return lax.ppermute(sent, "pix", pairs)

    near = swap(0, even)
    far = swap(1, ~even)

    made = [
        f32(count, rows, pixels), f32(count, rows, pixels),
        f32(count + 1, halves, KP, LANES), f32(count + 1, halves, KP, LANES),
        f32(2, halves, KP, LANES), f32(2, halves, KP, LANES), f32(SUB, pixels), f32(2, pixels),
    ]
    zr, zi, own, neighbours = pl.pallas_call(
        own_kernel,
        out_shape=made[:2] + [f32(2 * rows, pixels + reach), jax.ShapeDtypeStruct(neighbours.shape, jnp.int32)],
        in_specs=[HBM, HBM, VMEM],
        out_specs=[VMEM] * 4,
        scratch_shapes=[
            pltpu.VMEM((dates, 2, pixels), jnp.float32),
            pltpu.VMEM((4 * rows, pixels + reach), jnp.bfloat16),
            pltpu.SemaphoreType.DMA((2,)),
        ],
        compiler_params=params(),
        cost_estimate=cost(2 * 4 * rows * pixels * (pixels + reach) * count),
        name="own",
    )(pltpu.with_memory_space_constraint(neighbours, pltpu.HBM), pltpu.with_memory_space_constraint(slc, pltpu.HBM), near)

    pixel = jnp.full((SUB, LANES), reference_pixel[0], jnp.int32)

    def prepare(first, carried):
        more = [] if first else [pixel]
        outs = made if first else made[:7] + [f32(count + 2, halves, KP, LANES), f32(KP, LANES)]
        return pl.pallas_call(
            functools.partial(prepare_kernel, stack, first),
            out_shape=outs,
            in_specs=[VMEM] * (3 + len(more) + len(carried)),
            out_specs=[VMEM] * len(outs),
            scratch_shapes=[
                pltpu.VMEM((2 * rows, reach), jnp.float32),
                pltpu.VMEM((4 * rows, reach), jnp.bfloat16),
                pltpu.VMEM((2, count + 1, count, SUB, LANES), jnp.float32),
            ],
            input_output_aliases={3 + len(more) + n: n for n in range(len(carried))},
            compiler_params=params(),
            cost_estimate=cost(50 * 12 * rows * reach * pixels * count),
        )(neighbours, far, own, *more, *carried)

    *made_0, comp = prepare(True, (zr, zi))
    zr, zi, gr, gi, sums, beta, state, folded, tile = prepare(False, made_0)

    final = sections - 1
    step = 1
    while step < blocks:
        pairs = [(final * blocks + q, final * blocks + (q + step) % blocks) for q in range(blocks)]
        tile = tile + lax.ppermute(tile, ("section", "pix"), pairs)
        step *= 2

    for rnd in range(1, final):
        def hop(shift):
            pairs = [
                ((rnd - 1) * blocks + q, rnd * blocks + q + shift)
                for q in range(blocks)
                if 0 <= q + shift < blocks
            ]
            return lax.ppermute(comp, ("section", "pix"), pairs)

        last = rnd == final - 1
        late = (pixel, zr, zi, tile) if last else ()
        scratch = [pltpu.VMEM((count, halves, KP, LANES), jnp.float32)] * 2
        outs = [f32(2, halves, KP, LANES), f32(SUB, pixels), f32(2, pixels)]
        if last:
            scratch += [pltpu.VMEM(o.shape, o.dtype) for o in outs[:2]]
            outs = outs[2:] + [f32(2, dates, pixels), f32(sections * blocks, slot_rows(halves), 1, LANES)]
        call = pl.pallas_call(
            functools.partial(round_kernel, rnd, stack),
            out_shape=outs,
            in_specs=[VMEM] * (9 + len(late)),
            out_specs=[VMEM] * 3,
            scratch_shapes=scratch,
            compiler_params=params(),
        )
        near = (hop(1)[:, pixels - reach :], hop(0), hop(-1)[:, :reach])
        made = call(neighbours, *near, gr, gi, sums, beta, state, *late)
        if last:
            comp, vec, sent = made
        else:
            beta, state, comp = made
        if rnd == 1:
            later = lax.optimization_barrier((folded, comp))[0]
            folds = []
            for s in range(final):
                pairs = [(final * blocks + q, s * blocks + q) for q in range(blocks)]
                folds.append(lax.ppermute(later, ("section", "pix"), pairs))
            folds.append(folded)

    sent, *folds = lax.optimization_barrier((sent, *folds))
    got = lax.all_to_all(sent, ("section", "pix"), 0, 0, tiled=True)
    out, small = pl.pallas_call(
        functools.partial(finish_kernel, sections, stack),
        out_shape=[f32(dates, 2, pixels), f32(2, 1, pixels)],
        in_specs=[VMEM] * (10 + sections),
        out_specs=[VMEM] * 2,
        scratch_shapes=[
            pltpu.VMEM((count, halves + 1, KP, LANES), jnp.float32),
            pltpu.VMEM((count, halves + 1, KP, LANES), jnp.float32),
            pltpu.VMEM((2, halves, KP, LANES), jnp.float32),
            pltpu.VMEM((2, halves + 1, KP, LANES), jnp.float32),
            pltpu.VMEM((SUB, pixels + LANES), jnp.float32),
            pltpu.VMEM((2, dates, pixels), jnp.float32),
        ],
        compiler_params=params(),
        name="finish",
    )(pixel, neighbours, got, vec, comp, zr, zi, gr, gi, sums, *folds)
    return (jnp.transpose(out, (1, 0, 2)), small)


def solution(mesh):
    return jax.shard_map(
        on_device,
        mesh=mesh,
        in_specs=(P(None, "section", "pix"), P(None, "pix"), P()),
        out_specs=(P(None, "section", "pix"), P(None, "section", "pix")),
        check_vma=False,
    )
```

```python
import functools
import math

import jax
import jax.numpy as jnp
from jax import lax
from jax.experimental import pallas as pl
from jax.experimental.pallas import tpu as pltpu
from jax.sharding import PartitionSpec as P


ITERS = 16
FLOOR = 0.05
REACH_LIMIT = 256
LANES = 128
SUB = 8
KP = 16
Z_LANE, Z_STEP = 20, 54
SHRINK = 2.0**-35

VMEM = pl.BlockSpec(memory_space=pltpu.VMEM)
HBM = pl.BlockSpec(memory_space=pltpu.HBM)


def f32(*shape):
    return jax.ShapeDtypeStruct(shape, jnp.float32)


def params():
    return pltpu.CompilerParams(vmem_limit_bytes=20 * 1024 * 1024)


def cost(flops):
    return pl.CostEstimate(flops=flops, bytes_accessed=0, transcendentals=0)


def up(n, m):
    return -(-n // m) * m


def colsum(x):
    return jnp.sum(x, axis=0, keepdims=True)


def unit(real, imag):
    scale = 1.0 / jnp.maximum(jnp.sqrt(real * real + imag * imag), FLOOR)
    return (real * scale, imag * scale)


def seat(pixels, reach):
    section, block = lax.axis_index("section"), lax.axis_index("pix")
    even = block % 2 == 0
    return (
        section, block, lax.axis_size("pix"), block * pixels,
        jnp.where(even, pixels, -reach), jnp.where(even, -reach, pixels),
    )


def half(h):
    return pl.ds(h * LANES, LANES)


def gather(start, idx_ref, pieces, xs_ref, hl_ref, zr_ref, zi_ref, add):
    count, rows, pixels = zr_ref.shape
    xs_ref[...] = jnp.zeros_like(xs_ref)
    at = 0
    place = []
    for piece, first in pieces:
        dates, _, width = piece.shape
        for c in range(2):
            xs_ref[pl.ds(c * rows, dates), pl.ds(at, width)] = piece[:, c]
        place.append(lax.broadcasted_iota(jnp.int32, (width, pixels), 0) + first)
        at += width
    place = jnp.concatenate(place, axis=0)
    high = xs_ref[...].astype(jnp.bfloat16)
    hl_ref[0 : 2 * rows] = high
    hl_ref[2 * rows : 4 * rows] = (xs_ref[...] - high.astype(jnp.float32)).astype(jnp.bfloat16)
    for k in range(count):
        near = idx_ref[k : k + 1, :] - start
        hot = jnp.where(place == near, 1.0, 0.0).astype(jnp.bfloat16)
        got = jnp.dot(hl_ref[...], hot, preferred_element_type=jnp.float32)
        zr = got[0:rows] + got[2 * rows : 3 * rows]
        zi = got[rows : 2 * rows] + got[3 * rows : 4 * rows]
        zr_ref[k] = zr_ref[k] + zr if add else zr
        zi_ref[k] = zi_ref[k] + zi if add else zi


def scale_dates(zr_ref, zi_ref):
    count, rows, pixels = zr_ref.shape
    for h in range(pixels // LANES):
        for r in range(0, rows, SUB):
            power = None
            for k in range(count):
                a = zr_ref[k, pl.ds(r, SUB), half(h)]
                b = zi_ref[k, pl.ds(r, SUB), half(h)]
                power = a * a + b * b if power is None else power + (a * a + b * b)
            scale = lax.rsqrt(jnp.maximum(power, 1.0))
            for k in range(count):
                zr_ref[k, pl.ds(r, SUB), half(h)] *= scale
                zi_ref[k, pl.ds(r, SUB), half(h)] *= scale


def merge_rows(parts):
    row = lax.broadcasted_iota(jnp.int32, (SUB, LANES), 0)
    for step in (4, 2, 1):
        low = jnp.bitwise_and(row, step) == 0
        other = jnp.bitwise_xor(row, step)
        n = len(parts) // 2
        out = []
        for i in range(n):
            a, b = parts[i], parts[i + n]
            far = jnp.take_along_axis(jnp.where(low, b, a), other, axis=0, mode="promise_in_bounds")
            out.append(jnp.where(low, a, b) + far)
        parts = out
    return parts[0]


def gram(pair_ref, zr_ref, zi_ref, own_ref, gr_ref, gi_ref, sum_ref, block=3):
    count, rows, pixels = zr_ref.shape
    zero = jnp.zeros((SUB, LANES), jnp.float32)
    for h in range(pixels // LANES):
        def load(k, r):
            if k == count:
                return (own_ref[pl.ds(r, SUB), half(h)], own_ref[pl.ds(rows + r, SUB), half(h)])
            return (zr_ref[k, pl.ds(r, SUB), half(h)], zi_ref[k, pl.ds(r, SUB), half(h)])

        for k0 in range(0, count, block):
            for l0 in range(k0, count + 1, block):
                pairs = [
                    (k, l)
                    for k in range(k0, min(k0 + block, count))
                    for l in range(l0, min(l0 + block, count + 1))
                    if l >= k
                ]
                acc = {}
                for r in range(0, rows, SUB):
                    val = {n: load(n, r) for n in sorted({n for p in pairs for n in p})}
                    minus = {k: val[k][0] - val[k][1] for k in {k for k, l in pairs if k != l}}
                    plus = {l: val[l][0] + val[l][1] for l in {l for k, l in pairs if k != l}}
                    for k, l in pairs:
                        new = [val[k][0] * val[l][0], val[k][1] * val[l][1]]
                        if k != l:
                            new.append(minus[k] * plus[l])
                        acc[k, l] = [x + y for x, y in zip(acc[k, l], new)] if r else new
                for k, l in pairs:
                    pair_ref[0, l, k] = acc[k, l][0] + acc[k, l][1]
                    pair_ref[1, l, k] = zero if k == l else acc[k, l][2] - (acc[k, l][0] - acc[k, l][1])
        for c, g_ref in ((0, gr_ref), (1, gi_ref)):
            for l in range(count + 1):
                for kt in range(KP // SUB):
                    ks = range(kt * SUB, kt * SUB + SUB)
                    if min(ks) > min(l, count - 1):
                        continue
                    parts = [pair_ref[c, l, k] if k <= min(l, count - 1) else zero for k in ks]
                    g_ref[l, h, pl.ds(kt * SUB, SUB), :] = merge_rows(parts)
        row = lax.broadcasted_iota(jnp.int32, (SUB, LANES), 0)
        for c, g_ref in ((0, gr_ref), (1, gi_ref)):
            for l in range(count):
                for kt in range(KP // SUB):
                    ks = list(range(kt * SUB, kt * SUB + SUB))
                    if max(ks) <= l:
                        continue
                    other = jnp.concatenate(
                        [g_ref[k, h, pl.ds(l, 1), :] if l < k < count else zero[0:1] for k in ks], axis=0
                    )
                    if c:
                        other = -other
                    if min(ks) <= l:
                        other = jnp.where(row + ks[0] <= l, g_ref[l, h, pl.ds(kt * SUB, SUB), :], other)
                    g_ref[l, h, pl.ds(kt * SUB, SUB), :] = other
        for c in range(2):
            tiles = []
            for k in range(KP):
                total = None
                if k <= count:
                    for r in range(0, rows, SUB):
                        v = load(k, r)[c]
                        total = v if total is None else total + v
                tiles.append(zero if total is None else total)
            for kt in range(KP // SUB):
                sum_ref[c, h, pl.ds(kt * SUB, SUB), :] = merge_rows(tiles[kt * SUB : kt * SUB + SUB])


def turns(gr_ref, gi_ref, g0, count):
    halves = gr_ref.shape[1]

    def product(b, g):
        acc = [list(x) for x in g]
        for l in range(count):
            for h in range(halves):
                br = jnp.broadcast_to(b[h][0][l : l + 1], (KP, LANES))
                bi = jnp.broadcast_to(b[h][1][l : l + 1], (KP, LANES))
                gr = gr_ref[l, h]
                gi = gi_ref[l, h]
                acc[h][0] = acc[h][0] + (gr * br - gi * bi)
                acc[h][1] = acc[h][1] + (gr * bi + gi * br)
        return acc

    def step(_, carry):
        b, g = carry
        t = product(b, g)
        return tuple((b[h][0] + t[h][0], b[h][1] + t[h][1]) for h in range(halves)), g

    g = tuple(g0)
    b = g
    b, g = lax.fori_loop(0, ITERS // 2 - 1, step, (b, g))
    b = tuple((x * SHRINK, y * SHRINK) for x, y in b)
    g = tuple((x * SHRINK, y * SHRINK) for x, y in g)
    b, g = lax.fori_loop(0, ITERS - ITERS // 2, step, (b, g))
    return b, g, product(b, g)


def solve(virtual, gr_ref, gi_ref, hr, hi, sums, stack, beta_ref, state_ref):
    halves = gr_ref.shape[1]
    count = gr_ref.shape[0]
    first = 1.0 / math.sqrt(stack)
    g0 = []
    for h in range(halves):
        zr, zi = sums[h]
        row = lax.broadcasted_iota(jnp.int32, (KP, LANES), 0)
        zr = jnp.where(row < count, zr, 0.0)
        zi = jnp.where(row < count, zi, 0.0)
        if virtual is not None:
            zr = zr + virtual[h][1][0]
            zi = zi + virtual[h][1][1]
        g0.append((zr * first, zi * -first))
    b, g, t = turns(gr_ref, gi_ref, g0, count)
    for h in range(halves):
        norm = colsum(b[h][0] * (g[h][0] + t[h][0]) + b[h][1] * (g[h][1] + t[h][1]))
        inv = lax.rsqrt(SHRINK * SHRINK + norm)
        br, bi = b[h][0] * inv, b[h][1] * inv
        a = inv * (SHRINK * first)
        xr, xi = hr[h], hi[h]
        sr, si = (x[count : count + 1] for x in sums[h])
        fr, fi = a, jnp.zeros_like(a)
        if virtual is not None:
            (wr, wi), (zr, zi) = virtual[h]
            xr, xi = xr + (zr * wr + zi * wi), xi + (zr * wi - zi * wr)
            sr, si = sr + wr, si + wi
            fr = a + colsum(zr * br - zi * bi)
            fi = colsum(zr * bi + zi * br)
        beta_ref[0, h] = br
        beta_ref[1, h] = bi
        fr, fi = unit(fr, fi)
        state_ref[0:1, half(h)] = a * sr + colsum(br * xr + bi * xi)
        state_ref[1:2, half(h)] = a * si + colsum(br * xi - bi * xr)
        state_ref[2:3, half(h)] = fr
        state_ref[3:4, half(h)] = fi
        state_ref[4:5, half(h)] = a
        state_ref[5:8, half(h)] = jnp.zeros((3, LANES), jnp.float32)


def own_kernel(idx_hbm, slc_hbm, near_ref, zr_ref, zi_ref, own_ref, idx_ref, slc_ref, hl_ref, sems):
    copies = [
        pltpu.make_async_copy(slc_hbm, slc_ref, sems.at[0]),
        pltpu.make_async_copy(idx_hbm, idx_ref, sems.at[1]),
    ]
    for copy in copies:
        copy.start()
    for copy in copies:
        copy.wait()
    _, _, _, start, near_at, _ = seat(slc_ref.shape[2], near_ref.shape[2])
    gather(start, idx_ref, ((slc_ref, 0), (near_ref, near_at)), own_ref, hl_ref, zr_ref, zi_ref, False)


def prepare_kernel(stack, first, idx_ref, far_ref, own_ref, *refs):
    if not first:
        pixel_ref, refs = refs[0], refs[1:]
    refs = refs[2 if first else 7 :]
    zr_ref, zi_ref, gr_ref, gi_ref, sum_ref, beta_ref, state_ref = refs[:7]
    xs_ref, hl_ref, pair_ref = refs[-3:]

    section, _, _, start, _, far_at = seat(zr_ref.shape[2], far_ref.shape[2])

    @pl.when(section == 0 if first else section != 0)
    def _():
        count = zr_ref.shape[0]
        gather(start, idx_ref, ((far_ref, far_at),), xs_ref, hl_ref, zr_ref, zi_ref, True)
        scale_dates(zr_ref, zi_ref)
        gram(pair_ref, zr_ref, zi_ref, own_ref, gr_ref, gi_ref, sum_ref)
        if first:
            halves = gr_ref.shape[1]
            hr = [gr_ref[count, h] for h in range(halves)]
            hi = [gi_ref[count, h] for h in range(halves)]
            sums = [(sum_ref[0, h], sum_ref[1, h]) for h in range(halves)]
            solve(None, gr_ref.at[0:count], gi_ref.at[0:count], hr, hi, sums, stack, beta_ref, state_ref)
            refs[7][...] = state_ref[0:2]

    if not first:

        @pl.when(section == lax.axis_size("section") - 1)
        def _():
            fold(start, pixel_ref, idx_ref, zr_ref, zi_ref, gr_ref, gi_ref, sum_ref, refs[7], refs[8])


def fold(start, pixel_ref, idx_ref, zr_ref, zi_ref, gr_ref, gi_ref, sum_ref, fold_ref, tile_ref):
    count, rows, pixels = zr_ref.shape
    halves = pixels // LANES
    k_row = lax.broadcasted_iota(jnp.int32, (KP, LANES), 0)
    lane = lax.broadcasted_iota(jnp.int32, (KP, LANES), 1)
    local = pixel_ref[...] - start
    hit = [lax.broadcasted_iota(jnp.int32, (SUB, LANES), 1) == local - h * LANES for h in range(halves)]

    def column(parts):
        total = None
        for h, part in enumerate(parts):
            mask = jnp.concatenate([hit[h]] * (part.shape[0] // SUB), axis=0)
            part = jnp.where(mask, part, 0.0)
            total = part if total is None else total + part
        return jnp.broadcast_to(jnp.sum(total, axis=1, keepdims=True), total.shape)

    tile = jnp.zeros((KP, LANES), jnp.float32)
    for l in range(count + 2):
        parts = []
        for h in range(halves):
            if l < count:
                part = jnp.where(k_row <= l, gr_ref[l, h], gi_ref[l, h])
            else:
                part = sum_ref[l - count, h]
            fold_ref[l, h] = part
            parts.append(part)
        tile = jnp.where(lane == (l if l < count else KP + l - count), column(parts), tile)
    pad = jnp.zeros((KP - count, LANES), jnp.float32)
    near = [jnp.concatenate([idx_ref[:, half(h)].astype(jnp.float32), pad], axis=0) for h in range(halves)]
    tile = jnp.where(lane == KP + 2, column(near), tile)
    wide = lax.broadcasted_iota(jnp.int32, (rows, LANES), 1)
    empty = jnp.zeros((LANES - rows, LANES), jnp.float32)
    for c, ref in ((0, zr_ref), (1, zi_ref)):
        both = jnp.zeros((rows, LANES), jnp.float32)
        for k in range(count):
            both = jnp.where(wide == k, column([ref[k, :, half(h)] for h in range(halves)]), both)
        turned = jnp.transpose(jnp.concatenate([both, empty], axis=0))[0:KP]
        at = Z_LANE + c * Z_STEP
        tile = jnp.where(jnp.logical_and(lane >= at, lane < at + Z_STEP), pltpu.roll(turned, at, 1), tile)
    tile_ref[...] = tile


def lane_take(x, i):
    return jnp.take_along_axis(x, i, axis=1, mode="promise_in_bounds")


def scaled(own, zr, zi):
    scale = lax.rsqrt(jnp.maximum(colsum(zr * zr + zi * zi), 1.0))
    return own, (zr * scale, zi * scale)


def take_virtual(idx_ref, base, reach, tiles, halves, count):
    virtual = []
    for h in range(halves):
        parts = []
        for kt in range(KP // SUB):
            rows = min(SUB, count - kt * SUB)
            raw = idx_ref[pl.ds(kt * SUB, rows), half(h)] - base
            if rows < SUB:
                raw = jnp.concatenate([raw, jnp.full((SUB - rows, LANES), -1, jnp.int32)], axis=0)
            lane = jnp.bitwise_and(raw, LANES - 1)
            tile = jnp.right_shift(raw, 7)
            both = []
            for c in range(2):
                out = jnp.zeros((SUB, LANES), jnp.float32)
                for n in range(h, h + 2 * reach // LANES + 1):
                    got = lane_take(jnp.broadcast_to(tiles[n][c], (SUB, LANES)), lane)
                    out = jnp.where(tile == n, got, out)
                both.append(out)
            parts.append(both)
        zr = jnp.concatenate([p[0] for p in parts], axis=0)
        zi = jnp.concatenate([p[1] for p in parts], axis=0)
        virtual.append(scaled(tiles[reach // LANES + h], zr, zi))
    return virtual


def update(virtual, gr_ref, gi_ref, fr_ref, fi_ref):
    for h, (_, (zr, zi)) in enumerate(virtual):
        for l in range(fr_ref.shape[0]):
            br = jnp.broadcast_to(zr[l : l + 1], (KP, LANES))
            bi = jnp.broadcast_to(zi[l : l + 1], (KP, LANES))
            fr_ref[l, h] = gr_ref[l, h] + (zr * br + zi * bi)
            fi_ref[l, h] = gi_ref[l, h] + (zr * bi - zi * br)


def round_kernel(
    rnd, stack, idx_ref, low_ref, own_ref, high_ref,
    gr_ref, gi_ref, sum_ref, beta0_ref, state0_ref, *refs,
):
    last = len(refs) > 5
    if last:
        late, (comp_ref, *made), refs = refs[:4], refs[4:7], refs[7:]
        fr_ref, fi_ref, beta_ref, state_ref = refs
    else:
        beta_ref, state_ref, comp_ref, fr_ref, fi_ref = refs
    count = gr_ref.shape[0] - 1
    halves = gr_ref.shape[1]
    reach = low_ref.shape[1]
    beta_ref[...] = beta0_ref[...]
    state_ref[...] = state0_ref[...]
    section, _, _, start, _, _ = seat(own_ref.shape[1], reach)

    @pl.when(section == rnd)
    def _():
        tiles = []
        for ref in (low_ref, own_ref, high_ref):
            for t in range(ref.shape[1] // LANES):
                tiles.append([ref[c : c + 1, half(t)] for c in range(2)])
        virtual = take_virtual(idx_ref, start - reach, reach, tiles, halves, count)
        update(virtual, gr_ref, gi_ref, fr_ref, fi_ref)
        hr = [gr_ref[count, h] for h in range(halves)]
        hi = [gi_ref[count, h] for h in range(halves)]
        sums = [(sum_ref[0, h], sum_ref[1, h]) for h in range(halves)]
        solve(virtual, fr_ref, fi_ref, hr, hi, sums, stack, beta_ref, state_ref)

    comp_ref[...] = state_ref[0:2]
    if last:
        vectors(*late, beta_ref, state_ref, *made)


def slot_rows(halves):
    return max(up(4 * halves + 1, SUB), KP)


def make_vectors(zr_ref, zi_ref, beta_ref, state_ref, vec_ref):
    count, rows, pixels = zr_ref.shape
    dates = vec_ref.shape[1]
    out = [[], []]
    for h in range(pixels // LANES):
        a = state_ref[4:5, half(h)]
        acc_r = [jnp.broadcast_to(a, (SUB, LANES)) for _ in range(0, rows, SUB)]
        acc_i = [jnp.zeros((SUB, LANES), jnp.float32) for _ in range(0, rows, SUB)]
        for k in range(count):
            br = jnp.broadcast_to(beta_ref[0, h, k : k + 1, :], (SUB, LANES))
            bi = jnp.broadcast_to(beta_ref[1, h, k : k + 1, :], (SUB, LANES))
            for n, r in enumerate(range(0, rows, SUB)):
                zr = zr_ref[k, pl.ds(r, SUB), half(h)]
                zi = zi_ref[k, pl.ds(r, SUB), half(h)]
                acc_r[n] = acc_r[n] + (zr * br - zi * bi)
                acc_i[n] = acc_i[n] + (zr * bi + zi * br)
        for c, acc in ((0, acc_r), (1, acc_i)):
            whole = jnp.concatenate(acc, axis=0)
            vec_ref[c, :, half(h)] = whole[0:dates]
            out[c].append(whole)
    return out


def vectors(pixel_ref, zr_ref, zi_ref, tile_ref, beta_ref, state_ref, vec_ref, slot_ref):
    _, rows, pixels = zr_ref.shape
    halves = pixels // LANES
    section, _, _, start, _, _ = seat(pixels, 0)

    @pl.when(section < lax.axis_size("section") - 1)
    def _():
        local = pixel_ref[...] - start
        lane = lax.broadcasted_iota(jnp.int32, (SUB, LANES), 1)
        row = lax.broadcasted_iota(jnp.int32, (SUB, LANES), 0)
        at_pixel = [jnp.zeros((SUB, LANES), jnp.float32) for _ in range(2)]
        vecs = make_vectors(zr_ref, zi_ref, beta_ref, state_ref, vec_ref)
        for c in range(2):
            for h in range(halves):
                empty = jnp.zeros((LANES - rows, LANES), jnp.float32)
                turned = jnp.transpose(jnp.concatenate([vecs[c][h], empty], axis=0))
                for r in range(0, LANES, SUB):
                    at_pixel[c] = at_pixel[c] + jnp.where(row == local - (h * LANES + r), turned[r : r + SUB], 0.0)
        slot = [state_ref[c : c + 1, half(h)] for c in range(4) for h in range(halves)]
        mixed = colsum(at_pixel[0]) + pltpu.roll(jnp.broadcast_to(colsum(at_pixel[1]), (SUB, LANES)), LANES // 2, 1)[0:1]
        for c in range(2):
            picked = jnp.zeros((1, LANES), jnp.float32)
            for h in range(halves):
                picked = picked + jnp.where((lane == local - h * LANES)[0:1], state_ref[2 + c : 3 + c, half(h)], 0.0)
            f = jnp.sum(picked, axis=1, keepdims=True)
            mixed = jnp.where(lane[0:1] == LANES - 2 + c, jnp.broadcast_to(f, (1, LANES)), mixed)
        slot.append(mixed)
        slot.append(jnp.zeros((slot_ref.shape[1] - len(slot), LANES), jnp.float32))
        slot = jnp.concatenate(slot, axis=0)
        for n in range(slot_ref.shape[0]):
            slot_ref[n] = slot

    @pl.when(section == lax.axis_size("section") - 1)
    def _():
        for n in range(slot_ref.shape[0]):
            slot_ref[n, 0:KP] = tile_ref[...]


def unfold(fold_ref, fr_ref, fi_ref):
    count = fr_ref.shape[0]
    k_row = lax.broadcasted_iota(jnp.int32, (KP, LANES), 0)
    for h in range(fold_ref.shape[1]):
        for l in range(count):
            straight = fold_ref[l, h]
            turned = jnp.concatenate(
                [fold_ref[k, h, pl.ds(l, 1), :] for k in range(count)] + [jnp.zeros((KP - count, LANES), jnp.float32)], axis=0
            )
            fr_ref[l, h] = jnp.where(k_row <= l, straight, turned)
            fi_ref[l, h] = jnp.where(k_row > l, straight, jnp.where(k_row < l, -turned, 0.0))


def finish_kernel(
    sections, stack, pixel_ref, idx_ref, got_ref, vec0_ref, comp0_ref, zr_ref, zi_ref, gr_ref, gi_ref, sum_ref, *refs
):
    folds, (out_ref, small_ref), refs = refs[:sections], refs[sections : sections + 2], refs[sections + 2 :]
    fr_ref, fi_ref, add_ref, beta_ref, state_ref, vec_ref = refs
    dates, pixels = vec_ref.shape[1:]
    count = zr_ref.shape[0]
    section, mine, blocks, start, _, _ = seat(pixels, 0)
    halves = pixels // LANES
    final = sections - 1
    reach = min(pixels, REACH_LIMIT)

    for s in range(sections):

        @pl.when(section == s)
        def _(s=s):
            unfold(folds[s], fr_ref, fi_ref)
            for c in range(2):
                for h in range(halves):
                    add_ref[c, h] = folds[s][count + c, h]

    tile = got_ref[final * blocks, 0:KP]
    for q in range(1, blocks):
        tile = tile + got_ref[final * blocks + q, 0:KP]
    k_row = lax.broadcasted_iota(jnp.int32, (KP, LANES), 0)
    lane = lax.broadcasted_iota(jnp.int32, (KP, LANES), 1)
    turned = jnp.transpose(jnp.concatenate([tile, jnp.zeros((LANES - KP, LANES), jnp.float32)], axis=0))[0:KP]
    real = jnp.where(k_row <= lane, tile, turned)
    imag = jnp.where(k_row > lane, tile, jnp.where(k_row < lane, -turned, 0.0))

    def spread(x, l):
        return jnp.broadcast_to(x[:, l : l + 1], (KP, LANES))

    for l in range(count):
        fr_ref[l, halves] = spread(real, l)
        fi_ref[l, halves] = spread(imag, l)
    sums = [(add_ref[0, h], add_ref[1, h]) for h in range(halves)] + [(spread(tile, KP), spread(tile, KP + 1))]

    before = final - 1
    tiles = []
    per = reach // LANES
    low, high = jnp.maximum(mine - 1, 0), jnp.minimum(mine + 1, blocks - 1)
    for at, which in ((low, range(halves - per, halves)), (mine, range(halves)), (high, range(per))):
        for h in which:
            tiles.append([got_ref[before * blocks + at, c * halves + h : c * halves + h + 1] for c in range(2)])
    virtual = take_virtual(idx_ref, start - reach, reach, tiles, halves, count)
    near = spread(tile, KP + 2).astype(jnp.int32)
    total = [jnp.zeros((KP, LANES), jnp.float32) for _ in range(2)]
    for q in range(blocks):
        for h in range(halves):
            hit = lane == near - (q * pixels + h * LANES)
            for c in range(2):
                row = got_ref[before * blocks + q, c * halves + h : c * halves + h + 1]
                total[c] = total[c] + jnp.where(hit, row, 0.0)
    total = [jnp.broadcast_to(jnp.sum(x, axis=1, keepdims=True), (KP, LANES)) for x in total]
    total = [jnp.where(k_row < count, x, 0.0) for x in total]
    virtual.append(scaled([x[0:1] for x in total], *total))
    update(virtual, fr_ref, fi_ref, fr_ref, fi_ref)

    zero = jnp.zeros((KP, LANES), jnp.float32)
    hr = [gr_ref[count, h] for h in range(halves)] + [zero]
    hi = [gi_ref[count, h] for h in range(halves)] + [zero]
    solve(virtual, fr_ref, fi_ref, hr, hi, sums, stack, beta_ref, state_ref)
    is_final = section == final
    for c in range(2):
        small_ref[c] = jnp.where(is_final, state_ref[c : c + 1, 0:pixels], comp0_ref[c : c + 1])

    def of_pixel(s):
        total = jnp.zeros((1, LANES), jnp.float32)
        for q in range(blocks):
            first = pixel_ref[0:1] - q * pixels
            here = jnp.logical_and(first >= 0, first < pixels)
            total = total + jnp.where(here, got_ref[s * blocks + q, 4 * halves : 4 * halves + 1], 0.0)
        return total

    def times(d, later, fr, fi):
        fr = jnp.where(later, fr, 1.0)
        fi = jnp.where(later, fi, 0.0)
        return (d[0] * fr - d[1] * fi, d[0] * fi + d[1] * fr)

    one = jnp.ones((1, LANES), jnp.float32)
    datum = [(one, 0.0 * one) for _ in range(halves + 1)]
    for h in range(halves + 1):
        datum[h] = times(datum[h], section < final, state_ref[2:3, half(h)], state_ref[3:4, half(h)])
    for s in range(final - 1, 0, -1):
        later = section < s
        own = [got_ref[s * blocks + mine, 2 * halves + m : 2 * halves + m + 1] for m in range(2 * halves)]
        row = of_pixel(s)
        for h in range(halves):
            datum[h] = times(datum[h], later, own[h], own[halves + h])
        f = [jnp.sum(jnp.where(lane[0:1] == LANES - 2 + c, row, 0.0), axis=1, keepdims=True) for c in range(2)]
        datum[halves] = times(datum[halves], later, *[jnp.broadcast_to(x, (1, LANES)) for x in f])

    zr = pltpu.roll(tile, LANES - Z_LANE, 1)
    zi = pltpu.roll(tile, LANES - Z_LANE - Z_STEP, 1)
    br, bi = beta_ref[0, halves], beta_ref[1, halves]
    zr, zi = jnp.where(k_row < count, zr, 0.0), jnp.where(k_row < count, zi, 0.0)
    last_r = state_ref[4:5, half(halves)] + colsum(zr * br - zi * bi)
    last_i = colsum(zr * bi + zi * br)
    row = of_pixel(jnp.minimum(section, final - 1))
    vr = jnp.where(is_final, last_r, row)
    vi = jnp.where(is_final, last_i, pltpu.roll(jnp.broadcast_to(row, (SUB, LANES)), LANES // 2, 1)[0:1])
    dr, di = datum[halves]
    ur, ui = unit(vr * dr - vi * di, vr * di + vi * dr)
    gain = math.sqrt(dates + 1)
    ur = jnp.transpose(jnp.broadcast_to(ur * gain, (LANES, LANES)))[0:dates]
    ui = jnp.transpose(jnp.broadcast_to(ui * gain, (LANES, LANES)))[0:dates]

    @pl.when(is_final)
    def _():
        make_vectors(zr_ref, zi_ref, beta_ref, state_ref, vec_ref)

    for h in range(halves):
        wr = ur * datum[h][0] + ui * datum[h][1]
        wi = ur * datum[h][1] - ui * datum[h][0]
        vr = jnp.where(is_final, vec_ref[0, :, half(h)], vec0_ref[0, :, half(h)])
        vi = jnp.where(is_final, vec_ref[1, :, half(h)], vec0_ref[1, :, half(h)])
        out_ref[:, 0, half(h)] = vr * wr - vi * wi
        out_ref[:, 1, half(h)] = vr * wi + vi * wr


def on_device(slc, neighbours, reference_pixel):
    dates, pixels = slc.shape[1:]
    slc = jnp.transpose(slc, (1, 0, 2))
    count = neighbours.shape[0]
    reach = min(pixels, REACH_LIMIT)
    sections = lax.axis_size("section")
    blocks = lax.axis_size("pix")
    block = lax.axis_index("pix")
    stack = dates + 1
    halves = pixels // LANES
    rows = up(dates, SUB)

    even = block % 2 == 0

    def swap(first, upper):
        pairs = [(i, i + 1) for i in range(first, blocks - 1, 2)]
        pairs += [(j, i) for i, j in pairs]
        sent = slc
        if reach < pixels:
            sent = jnp.where(upper, slc[:, :, pixels - reach :], slc[:, :, :reach])
        return lax.ppermute(sent, "pix", pairs)

    near = swap(0, even)
    far = swap(1, ~even)

    made = [
        f32(count, rows, pixels), f32(count, rows, pixels),
        f32(count + 1, halves, KP, LANES), f32(count + 1, halves, KP, LANES),
        f32(2, halves, KP, LANES), f32(2, halves, KP, LANES), f32(SUB, pixels), f32(2, pixels),
    ]
    zr, zi, own, neighbours = pl.pallas_call(
        own_kernel,
        out_shape=made[:2] + [f32(2 * rows, pixels + reach), jax.ShapeDtypeStruct(neighbours.shape, jnp.int32)],
        in_specs=[HBM, HBM, VMEM],
        out_specs=[VMEM] * 4,
        scratch_shapes=[
            pltpu.VMEM((dates, 2, pixels), jnp.float32),
            pltpu.VMEM((4 * rows, pixels + reach), jnp.bfloat16),
            pltpu.SemaphoreType.DMA((2,)),
        ],
        compiler_params=params(),
        cost_estimate=cost(2 * 4 * rows * pixels * (pixels + reach) * count),
        name="own",
    )(pltpu.with_memory_space_constraint(neighbours, pltpu.HBM), pltpu.with_memory_space_constraint(slc, pltpu.HBM), near)

    pixel = jnp.full((SUB, LANES), reference_pixel[0], jnp.int32)

    def prepare(first, carried):
        more = [] if first else [pixel]
        outs = made if first else made[:7] + [f32(count + 2, halves, KP, LANES), f32(KP, LANES)]
        return pl.pallas_call(
            functools.partial(prepare_kernel, stack, first),
            out_shape=outs,
            in_specs=[VMEM] * (3 + len(more) + len(carried)),
            out_specs=[VMEM] * len(outs),
            scratch_shapes=[
                pltpu.VMEM((2 * rows, reach), jnp.float32),
                pltpu.VMEM((4 * rows, reach), jnp.bfloat16),
                pltpu.VMEM((2, count + 1, count, SUB, LANES), jnp.float32),
            ],
            input_output_aliases={3 + len(more) + n: n for n in range(len(carried))},
            compiler_params=params(),
            cost_estimate=cost(50 * 12 * rows * reach * pixels * count),
        )(neighbours, far, own, *more, *carried)

    *made_0, comp = prepare(True, (zr, zi))
    zr, zi, gr, gi, sums, beta, state, folded, tile = prepare(False, made_0)

    final = sections - 1
    folds = []
    for s in range(final):
        pairs = [(final * blocks + q, s * blocks + q) for q in range(blocks)]
        folds.append(lax.ppermute(folded, ("section", "pix"), pairs))
    folds.append(folded)

    for rnd in range(1, final):
        def hop(shift):
            pairs = [
                ((rnd - 1) * blocks + q, rnd * blocks + q + shift)
                for q in range(blocks)
                if 0 <= q + shift < blocks
            ]
            return lax.ppermute(comp, ("section", "pix"), pairs)

        last = rnd == final - 1
        late = (pixel, zr, zi, tile) if last else ()
        scratch = [pltpu.VMEM((count, halves, KP, LANES), jnp.float32)] * 2
        outs = [f32(2, halves, KP, LANES), f32(SUB, pixels), f32(2, pixels)]
        if last:
            scratch += [pltpu.VMEM(o.shape, o.dtype) for o in outs[:2]]
            outs = outs[2:] + [f32(2, dates, pixels), f32(sections * blocks, slot_rows(halves), LANES)]
        call = pl.pallas_call(
            functools.partial(round_kernel, rnd, stack),
            out_shape=outs,
            in_specs=[VMEM] * (9 + len(late)),
            out_specs=[VMEM] * 3,
            scratch_shapes=scratch,
            compiler_params=params(),
        )
        near = (hop(1)[:, pixels - reach :], hop(0), hop(-1)[:, :reach])
        made = call(neighbours, *near, gr, gi, sums, beta, state, *late)
        if last:
            comp, vec, sent = made
        else:
            beta, state, comp = made

    sent, *folds = lax.optimization_barrier((sent, *folds))
    got = lax.all_to_all(sent, ("section", "pix"), 0, 0, tiled=True)
    out, small = pl.pallas_call(
        functools.partial(finish_kernel, sections, stack),
        out_shape=[f32(dates, 2, pixels), f32(2, 1, pixels)],
        in_specs=[VMEM] * (10 + sections),
        out_specs=[VMEM] * 2,
        scratch_shapes=[
            pltpu.VMEM((count, halves + 1, KP, LANES), jnp.float32),
            pltpu.VMEM((count, halves + 1, KP, LANES), jnp.float32),
            pltpu.VMEM((2, halves, KP, LANES), jnp.float32),
            pltpu.VMEM((2, halves + 1, KP, LANES), jnp.float32),
            pltpu.VMEM((SUB, pixels + LANES), jnp.float32),
            pltpu.VMEM((2, dates, pixels), jnp.float32),
        ],
        compiler_params=params(),
        name="finish",
    )(pixel, neighbours, got, vec, comp, zr, zi, gr, gi, sums, *folds)
    return (jnp.transpose(out, (1, 0, 2)), small)


def solution(mesh):
    return jax.shard_map(
        on_device,
        mesh=mesh,
        in_specs=(P(None, "section", "pix"), P(None, "pix"), P()),
        out_specs=(P(None, "section", "pix"), P(None, "section", "pix")),
        check_vma=False,
    )
```

```python
import functools
import math

import jax
import jax.numpy as jnp
from jax import lax
from jax.experimental import pallas as pl
from jax.experimental.pallas import tpu as pltpu
from jax.sharding import PartitionSpec as P


ITERS = 16
FLOOR = 0.05
REACH_LIMIT = 256
LANES = 128
SUB = 8
KP = 16
Z_LANE, Z_STEP = 20, 54
SHRINK = 2.0**-35

VMEM = pl.BlockSpec(memory_space=pltpu.VMEM)
HBM = pl.BlockSpec(memory_space=pltpu.HBM)


def f32(*shape):
    return jax.ShapeDtypeStruct(shape, jnp.float32)


def params():
    return pltpu.CompilerParams(vmem_limit_bytes=20 * 1024 * 1024)


def cost(flops):
    return pl.CostEstimate(flops=flops, bytes_accessed=0, transcendentals=0)


def up(n, m):
    return -(-n // m) * m


def colsum(x):
    return jnp.sum(x, axis=0, keepdims=True)


def unit(real, imag):
    scale = 1.0 / jnp.maximum(jnp.sqrt(real * real + imag * imag), FLOOR)
    return (real * scale, imag * scale)


def seat(pixels, reach):
    section, block = lax.axis_index("section"), lax.axis_index("pix")
    even = block % 2 == 0
    return (
        section, block, lax.axis_size("pix"), block * pixels,
        jnp.where(even, pixels, -reach), jnp.where(even, -reach, pixels),
    )


def half(h):
    return pl.ds(h * LANES, LANES)


def gather(start, idx_ref, pieces, xs_ref, hl_ref, zr_ref, zi_ref, add):
    count, rows, pixels = zr_ref.shape
    xs_ref[...] = jnp.zeros_like(xs_ref)
    at = 0
    place = []
    for piece, first in pieces:
        dates, _, width = piece.shape
        for c in range(2):
            xs_ref[pl.ds(c * rows, dates), pl.ds(at, width)] = piece[:, c]
        place.append(lax.broadcasted_iota(jnp.int32, (width, pixels), 0) + first)
        at += width
    place = jnp.concatenate(place, axis=0)
    high = xs_ref[...].astype(jnp.bfloat16)
    hl_ref[0 : 2 * rows] = high
    hl_ref[2 * rows : 4 * rows] = (xs_ref[...] - high.astype(jnp.float32)).astype(jnp.bfloat16)
    for k in range(count):
        near = idx_ref[k : k + 1, :] - start
        hot = jnp.where(place == near, 1.0, 0.0).astype(jnp.bfloat16)
        got = jnp.dot(hl_ref[...], hot, preferred_element_type=jnp.float32)
        zr = got[0:rows] + got[2 * rows : 3 * rows]
        zi = got[rows : 2 * rows] + got[3 * rows : 4 * rows]
        zr_ref[k] = zr_ref[k] + zr if add else zr
        zi_ref[k] = zi_ref[k] + zi if add else zi


def scale_dates(zr_ref, zi_ref):
    count, rows, pixels = zr_ref.shape
    for h in range(pixels // LANES):
        for r in range(0, rows, SUB):
            power = None
            for k in range(count):
                a = zr_ref[k, pl.ds(r, SUB), half(h)]
                b = zi_ref[k, pl.ds(r, SUB), half(h)]
                power = a * a + b * b if power is None else power + (a * a + b * b)
            scale = lax.rsqrt(jnp.maximum(power, 1.0))
            for k in range(count):
                zr_ref[k, pl.ds(r, SUB), half(h)] *= scale
                zi_ref[k, pl.ds(r, SUB), half(h)] *= scale


def merge_rows(parts):
    row = lax.broadcasted_iota(jnp.int32, (SUB, LANES), 0)
    for step in (4, 2, 1):
        low = jnp.bitwise_and(row, step) == 0
        other = jnp.bitwise_xor(row, step)
        n = len(parts) // 2
        out = []
        for i in range(n):
            a, b = parts[i], parts[i + n]
            far = jnp.take_along_axis(jnp.where(low, b, a), other, axis=0, mode="promise_in_bounds")
            out.append(jnp.where(low, a, b) + far)
        parts = out
    return parts[0]


def gram(pair_ref, zr_ref, zi_ref, own_ref, gr_ref, gi_ref, sum_ref, block=3):
    count, rows, pixels = zr_ref.shape
    zero = jnp.zeros((SUB, LANES), jnp.float32)
    for h in range(pixels // LANES):
        def load(k, r):
            if k == count:
                return (own_ref[pl.ds(r, SUB), half(h)], own_ref[pl.ds(rows + r, SUB), half(h)])
            return (zr_ref[k, pl.ds(r, SUB), half(h)], zi_ref[k, pl.ds(r, SUB), half(h)])

        for k0 in range(0, count, block):
            for l0 in range(k0, count + 1, block):
                pairs = [
                    (k, l)
                    for k in range(k0, min(k0 + block, count))
                    for l in range(l0, min(l0 + block, count + 1))
                    if l >= k
                ]
                acc = {}
                for r in range(0, rows, SUB):
                    val = {n: load(n, r) for n in sorted({n for p in pairs for n in p})}
                    minus = {k: val[k][0] - val[k][1] for k in {k for k, l in pairs if k != l}}
                    plus = {l: val[l][0] + val[l][1] for l in {l for k, l in pairs if k != l}}
                    for k, l in pairs:
                        new = [val[k][0] * val[l][0], val[k][1] * val[l][1]]
                        if k != l:
                            new.append(minus[k] * plus[l])
                        acc[k, l] = [x + y for x, y in zip(acc[k, l], new)] if r else new
                for k, l in pairs:
                    pair_ref[0, l, k] = acc[k, l][0] + acc[k, l][1]
                    pair_ref[1, l, k] = zero if k == l else acc[k, l][2] - (acc[k, l][0] - acc[k, l][1])
        for c, g_ref in ((0, gr_ref), (1, gi_ref)):
            for l in range(count + 1):
                for kt in range(KP // SUB):
                    ks = range(kt * SUB, kt * SUB + SUB)
                    if min(ks) > min(l, count - 1):
                        continue
                    parts = [pair_ref[c, l, k] if k <= min(l, count - 1) else zero for k in ks]
                    g_ref[l, h, pl.ds(kt * SUB, SUB), :] = merge_rows(parts)
        row = lax.broadcasted_iota(jnp.int32, (SUB, LANES), 0)
        for c, g_ref in ((0, gr_ref), (1, gi_ref)):
            for l in range(count):
                for kt in range(KP // SUB):
                    ks = list(range(kt * SUB, kt * SUB + SUB))
                    if max(ks) <= l:
                        continue
                    other = jnp.concatenate(
                        [g_ref[k, h, pl.ds(l, 1), :] if l < k < count else zero[0:1] for k in ks], axis=0
                    )
                    if c:
                        other = -other
                    if min(ks) <= l:
                        other = jnp.where(row + ks[0] <= l, g_ref[l, h, pl.ds(kt * SUB, SUB), :], other)
                    g_ref[l, h, pl.ds(kt * SUB, SUB), :] = other
        for c in range(2):
            tiles = []
            for k in range(KP):
                total = None
                if k <= count:
                    for r in range(0, rows, SUB):
                        v = load(k, r)[c]
                        total = v if total is None else total + v
                tiles.append(zero if total is None else total)
            for kt in range(KP // SUB):
                sum_ref[c, h, pl.ds(kt * SUB, SUB), :] = merge_rows(tiles[kt * SUB : kt * SUB + SUB])


def turns(gr_ref, gs_ref, gd_ref, g0, count):
    halves = gr_ref.shape[1]

    def product(b, g):
        acc = [None] * halves
        for l in range(count):
            for h in range(halves):
                br = jnp.broadcast_to(b[h][0][l : l + 1], (KP, LANES))
                bi = jnp.broadcast_to(b[h][1][l : l + 1], (KP, LANES))
                new = [gr_ref[l, h] * (br + bi), gs_ref[l, h] * bi, gd_ref[l, h] * br]
                acc[h] = new if l == 0 else [x + y for x, y in zip(acc[h], new)]
        return [(g[h][0] + (t - u), g[h][1] + (t + v)) for h, (t, u, v) in enumerate(acc)]

    def step(_, carry):
        b, g = carry
        t = product(b, g)
        return tuple((b[h][0] + t[h][0], b[h][1] + t[h][1]) for h in range(halves)), g

    g = tuple(g0)
    b = g
    b, g = lax.fori_loop(0, ITERS // 2 - 1, step, (b, g))
    b = tuple((x * SHRINK, y * SHRINK) for x, y in b)
    g = tuple((x * SHRINK, y * SHRINK) for x, y in g)
    b, g = lax.fori_loop(0, ITERS - ITERS // 2, step, (b, g))
    return b, g, product(b, g)


def solve(virtual, gr_ref, gs_ref, gd_ref, hr, hi, sums, stack, beta_ref, state_ref):
    halves = gr_ref.shape[1]
    count = gr_ref.shape[0]
    first = 1.0 / math.sqrt(stack)
    g0 = []
    for h in range(halves):
        zr, zi = sums[h]
        row = lax.broadcasted_iota(jnp.int32, (KP, LANES), 0)
        zr = jnp.where(row < count, zr, 0.0)
        zi = jnp.where(row < count, zi, 0.0)
        if virtual is not None:
            zr = zr + virtual[h][1][0]
            zi = zi + virtual[h][1][1]
        g0.append((zr * first, zi * -first))
    b, g, t = turns(gr_ref, gs_ref, gd_ref, g0, count)
    for h in range(halves):
        norm = colsum(b[h][0] * (g[h][0] + t[h][0]) + b[h][1] * (g[h][1] + t[h][1]))
        inv = lax.rsqrt(SHRINK * SHRINK + norm)
        br, bi = b[h][0] * inv, b[h][1] * inv
        a = inv * (SHRINK * first)
        xr, xi = hr[h], hi[h]
        sr, si = (x[count : count + 1] for x in sums[h])
        fr, fi = a, jnp.zeros_like(a)
        if virtual is not None:
            (wr, wi), (zr, zi) = virtual[h]
            xr, xi = xr + (zr * wr + zi * wi), xi + (zr * wi - zi * wr)
            sr, si = sr + wr, si + wi
            fr = a + colsum(zr * br - zi * bi)
            fi = colsum(zr * bi + zi * br)
        beta_ref[0, h] = br
        beta_ref[1, h] = bi
        fr, fi = unit(fr, fi)
        state_ref[0:1, half(h)] = a * sr + colsum(br * xr + bi * xi)
        state_ref[1:2, half(h)] = a * si + colsum(br * xi - bi * xr)
        state_ref[2:3, half(h)] = fr
        state_ref[3:4, half(h)] = fi
        state_ref[4:5, half(h)] = a
        state_ref[5:8, half(h)] = jnp.zeros((3, LANES), jnp.float32)


def own_kernel(idx_hbm, slc_hbm, near_ref, zr_ref, zi_ref, own_ref, idx_ref, slc_ref, hl_ref, sems):
    copies = [
        pltpu.make_async_copy(slc_hbm, slc_ref, sems.at[0]),
        pltpu.make_async_copy(idx_hbm, idx_ref, sems.at[1]),
    ]
    for copy in copies:
        copy.start()
    for copy in copies:
        copy.wait()
    _, _, _, start, near_at, _ = seat(slc_ref.shape[2], near_ref.shape[2])
    gather(start, idx_ref, ((slc_ref, 0), (near_ref, near_at)), own_ref, hl_ref, zr_ref, zi_ref, False)


def prepare_kernel(stack, first, idx_ref, far_ref, own_ref, *refs):
    refs = refs[2 if first else 7 :]
    zr_ref, zi_ref, gr_ref, gi_ref, sum_ref, beta_ref, state_ref = refs[:7]
    xs_ref, hl_ref, pair_ref = refs[-3:]

    section, _, _, start, _, far_at = seat(zr_ref.shape[2], far_ref.shape[2])

    @pl.when(section == 0 if first else section != 0)
    def _():
        count = zr_ref.shape[0]
        gather(start, idx_ref, ((far_ref, far_at),), xs_ref, hl_ref, zr_ref, zi_ref, True)
        scale_dates(zr_ref, zi_ref)
        gram(pair_ref, zr_ref, zi_ref, own_ref, gr_ref, gi_ref, sum_ref)
        if first:
            halves = gr_ref.shape[1]
            hr = [gr_ref[count, h] for h in range(halves)]
            hi = [gi_ref[count, h] for h in range(halves)]
            sums = [(sum_ref[0, h], sum_ref[1, h]) for h in range(halves)]
            gs_ref, gd_ref = refs[8:10]
            for l in range(count):
                for h in range(halves):
                    gs_ref[l, h] = gi_ref[l, h] + gr_ref[l, h]
                    gd_ref[l, h] = gi_ref[l, h] - gr_ref[l, h]
            solve(None, gr_ref.at[0:count], gs_ref, gd_ref, hr, hi, sums, stack, beta_ref, state_ref)
            refs[7][...] = state_ref[0:2]

    if not first:

        @pl.when(section == lax.axis_size("section") - 1)
        def _():
            fold(gr_ref, gi_ref, sum_ref, refs[7])


def folded_column(l, h, gr_ref, gi_ref, sum_ref):
    count = gr_ref.shape[0] - 1
    if l >= count:
        return sum_ref[l - count, h]
    k_row = lax.broadcasted_iota(jnp.int32, (KP, LANES), 0)
    return jnp.where(k_row <= l, gr_ref[l, h], gi_ref[l, h])


def fold(gr_ref, gi_ref, sum_ref, fold_ref):
    halves = gr_ref.shape[1]
    for l in range(gr_ref.shape[0] + 1):
        for h in range(halves):
            fold_ref[pl.ds((l * halves + h) * KP, KP), :] = folded_column(l, h, gr_ref, gi_ref, sum_ref)


def make_tile(start, pixel_ref, idx_ref, zr_ref, zi_ref, gr_ref, gi_ref, sum_ref):
    count, rows, pixels = zr_ref.shape
    halves = pixels // LANES
    lane = lax.broadcasted_iota(jnp.int32, (KP, LANES), 1)
    local = pixel_ref[...] - start
    hit = [lax.broadcasted_iota(jnp.int32, (SUB, LANES), 1) == local - h * LANES for h in range(halves)]

    def column(parts):
        total = None
        for h, part in enumerate(parts):
            mask = jnp.concatenate([hit[h]] * (part.shape[0] // SUB), axis=0)
            part = jnp.where(mask, part, 0.0)
            total = part if total is None else total + part
        return jnp.broadcast_to(jnp.sum(total, axis=1, keepdims=True), total.shape)

    tile = jnp.zeros((KP, LANES), jnp.float32)
    for l in range(count + 2):
        parts = [folded_column(l, h, gr_ref, gi_ref, sum_ref) for h in range(halves)]
        tile = jnp.where(lane == (l if l < count else KP + l - count), column(parts), tile)
    pad = jnp.zeros((KP - count, LANES), jnp.float32)
    near = [jnp.concatenate([idx_ref[:, half(h)].astype(jnp.float32), pad], axis=0) for h in range(halves)]
    tile = jnp.where(lane == KP + 2, column(near), tile)
    wide = lax.broadcasted_iota(jnp.int32, (rows, LANES), 1)
    empty = jnp.zeros((LANES - rows, LANES), jnp.float32)
    for c, ref in ((0, zr_ref), (1, zi_ref)):
        both = jnp.zeros((rows, LANES), jnp.float32)
        for k in range(count):
            both = jnp.where(wide == k, column([ref[k, :, half(h)] for h in range(halves)]), both)
        turned = jnp.transpose(jnp.concatenate([both, empty], axis=0))[0:KP]
        at = Z_LANE + c * Z_STEP
        tile = jnp.where(jnp.logical_and(lane >= at, lane < at + Z_STEP), pltpu.roll(turned, at, 1), tile)
    return tile


def lane_take(x, i):
    return jnp.take_along_axis(x, i, axis=1, mode="promise_in_bounds")


def scaled(own, zr, zi):
    scale = lax.rsqrt(jnp.maximum(colsum(zr * zr + zi * zi), 1.0))
    return own, (zr * scale, zi * scale)


def take_virtual(idx_ref, base, reach, tiles, halves, count):
    virtual = []
    for h in range(halves):
        parts = []
        for kt in range(KP // SUB):
            rows = min(SUB, count - kt * SUB)
            raw = idx_ref[pl.ds(kt * SUB, rows), half(h)] - base
            if rows < SUB:
                raw = jnp.concatenate([raw, jnp.full((SUB - rows, LANES), -1, jnp.int32)], axis=0)
            lane = jnp.bitwise_and(raw, LANES - 1)
            tile = jnp.right_shift(raw, 7)
            both = []
            for c in range(2):
                out = jnp.zeros((SUB, LANES), jnp.float32)
                for n in range(h, h + 2 * reach // LANES + 1):
                    got = lane_take(jnp.broadcast_to(tiles[n][c], (SUB, LANES)), lane)
                    out = jnp.where(tile == n, got, out)
                both.append(out)
            parts.append(both)
        zr = jnp.concatenate([p[0] for p in parts], axis=0)
        zi = jnp.concatenate([p[1] for p in parts], axis=0)
        virtual.append(scaled(tiles[reach // LANES + h], zr, zi))
    return virtual


def update(virtual, gram_of, fr_ref, fs_ref, fd_ref):
    for h, (_, (zr, zi)) in enumerate(virtual):
        for l in range(fr_ref.shape[0]):
            gr, gi = gram_of(l, h)
            br = jnp.broadcast_to(zr[l : l + 1], (KP, LANES))
            bi = jnp.broadcast_to(zi[l : l + 1], (KP, LANES))
            gr = gr + (zr * br + zi * bi)
            gi = gi + (zr * bi - zi * br)
            fr_ref[l, h] = gr
            fs_ref[l, h] = gi + gr
            fd_ref[l, h] = gi - gr


def round_kernel(
    rnd, stack, idx_ref, low_ref, own_ref, high_ref,
    gr_ref, gi_ref, sum_ref, beta0_ref, state0_ref, *refs,
):
    last = len(refs) > 6
    if last:
        late, (comp_ref, *made), refs = refs[:3], refs[3:6], refs[6:]
        fr_ref, fs_ref, fd_ref, beta_ref, state_ref = refs
    else:
        beta_ref, state_ref, comp_ref, fr_ref, fs_ref, fd_ref = refs
    count = gr_ref.shape[0] - 1
    halves = gr_ref.shape[1]
    reach = low_ref.shape[1]
    beta_ref[...] = beta0_ref[...]
    state_ref[...] = state0_ref[...]
    section, _, _, start, _, _ = seat(own_ref.shape[1], reach)

    @pl.when(section == rnd)
    def _():
        tiles = []
        for ref in (low_ref, own_ref, high_ref):
            for t in range(ref.shape[1] // LANES):
                tiles.append([ref[c : c + 1, half(t)] for c in range(2)])
        virtual = take_virtual(idx_ref, start - reach, reach, tiles, halves, count)
        update(virtual, lambda l, h: (gr_ref[l, h], gi_ref[l, h]), fr_ref, fs_ref, fd_ref)
        hr = [gr_ref[count, h] for h in range(halves)]
        hi = [gi_ref[count, h] for h in range(halves)]
        sums = [(sum_ref[0, h], sum_ref[1, h]) for h in range(halves)]
        solve(virtual, fr_ref, fs_ref, fd_ref, hr, hi, sums, stack, beta_ref, state_ref)

    comp_ref[...] = state_ref[0:2]
    if last:
        vectors(*late, idx_ref, gr_ref, gi_ref, sum_ref, beta_ref, state_ref, *made)


def slot_rows(halves):
    return max(up(4 * halves + 1, SUB), KP)


def make_vectors(zr_ref, zi_ref, beta_ref, state_ref, vec_ref):
    count, rows, pixels = zr_ref.shape
    dates = vec_ref.shape[1]
    out = [[], []]
    for h in range(pixels // LANES):
        a = state_ref[4:5, half(h)]
        acc_r = [jnp.broadcast_to(a, (SUB, LANES)) for _ in range(0, rows, SUB)]
        acc_i = [jnp.zeros((SUB, LANES), jnp.float32) for _ in range(0, rows, SUB)]
        for k in range(count):
            br = jnp.broadcast_to(beta_ref[0, h, k : k + 1, :], (SUB, LANES))
            bi = jnp.broadcast_to(beta_ref[1, h, k : k + 1, :], (SUB, LANES))
            for n, r in enumerate(range(0, rows, SUB)):
                zr = zr_ref[k, pl.ds(r, SUB), half(h)]
                zi = zi_ref[k, pl.ds(r, SUB), half(h)]
                acc_r[n] = acc_r[n] + (zr * br - zi * bi)
                acc_i[n] = acc_i[n] + (zr * bi + zi * br)
        for c, acc in ((0, acc_r), (1, acc_i)):
            whole = jnp.concatenate(acc, axis=0)
            vec_ref[c, :, half(h)] = whole[0:dates]
            out[c].append(whole)
    return out


def vectors(pixel_ref, zr_ref, zi_ref, idx_ref, gr_ref, gi_ref, sum_ref, beta_ref, state_ref, vec_ref, slot_ref):
    _, rows, pixels = zr_ref.shape
    halves = pixels // LANES
    section, _, _, start, _, _ = seat(pixels, 0)

    @pl.when(section < lax.axis_size("section") - 1)
    def _():
        local = pixel_ref[...] - start
        lane = lax.broadcasted_iota(jnp.int32, (SUB, LANES), 1)
        row = lax.broadcasted_iota(jnp.int32, (SUB, LANES), 0)
        at_pixel = [jnp.zeros((SUB, LANES), jnp.float32) for _ in range(2)]
        vecs = make_vectors(zr_ref, zi_ref, beta_ref, state_ref, vec_ref)
        for c in range(2):
            for h in range(halves):
                empty = jnp.zeros((LANES - rows, LANES), jnp.float32)
                turned = jnp.transpose(jnp.concatenate([vecs[c][h], empty], axis=0))
                for r in range(0, LANES, SUB):
                    at_pixel[c] = at_pixel[c] + jnp.where(row == local - (h * LANES + r), turned[r : r + SUB], 0.0)
        slot = [state_ref[c : c + 1, half(h)] for c in range(4) for h in range(halves)]
        mixed = colsum(at_pixel[0]) + pltpu.roll(jnp.broadcast_to(colsum(at_pixel[1]), (SUB, LANES)), LANES // 2, 1)[0:1]
        for c in range(2):
            picked = jnp.zeros((1, LANES), jnp.float32)
            for h in range(halves):
                picked = picked + jnp.where((lane == local - h * LANES)[0:1], state_ref[2 + c : 3 + c, half(h)], 0.0)
            f = jnp.sum(picked, axis=1, keepdims=True)
            mixed = jnp.where(lane[0:1] == LANES - 2 + c, jnp.broadcast_to(f, (1, LANES)), mixed)
        slot.append(mixed)
        slot.append(jnp.zeros((slot_ref.shape[1] - len(slot), LANES), jnp.float32))
        slot = jnp.concatenate(slot, axis=0)
        for n in range(slot_ref.shape[0]):
            slot_ref[n] = slot

    @pl.when(section == lax.axis_size("section") - 1)
    def _():
        tile = make_tile(start, pixel_ref, idx_ref, zr_ref, zi_ref, gr_ref, gi_ref, sum_ref)
        for n in range(slot_ref.shape[0]):
            slot_ref[n, 0:KP] = tile


def unfold(fold, l, h, k_row, count):
    straight, turned = fold[0](l, h), jnp.where(k_row < count, fold[1](l, h), 0.0)
    return (
        jnp.where(k_row <= l, straight, turned),
        jnp.where(k_row > l, straight, jnp.where(k_row < l, -turned, 0.0)),
    )


def finish_kernel(
    sections, stack, pixel_ref, idx_ref, got_ref, vec0_ref, comp0_ref, zr_ref, zi_ref, gr_ref, gi_ref, sum_ref, *refs
):
    folds, (out_ref, small_ref), refs = refs[:sections], refs[sections : sections + 2], refs[sections + 2 :]
    fold_ref, fr_ref, fs_ref, fd_ref, beta_ref, state_ref, vec_ref = refs
    dates, pixels = vec_ref.shape[1:]
    count = zr_ref.shape[0]
    section, mine, blocks, start, _, _ = seat(pixels, 0)
    halves = pixels // LANES
    final = sections - 1
    reach = min(pixels, REACH_LIMIT)

    for s in range(sections):

        @pl.when(section == s)
        def _(s=s):
            fold_ref[...] = folds[s][...]

    tile = got_ref[final * blocks, 0:KP]
    for q in range(1, blocks):
        tile = tile + got_ref[final * blocks + q, 0:KP]
    k_row = lax.broadcasted_iota(jnp.int32, (KP, LANES), 0)
    lane = lax.broadcasted_iota(jnp.int32, (KP, LANES), 1)
    turned = jnp.transpose(jnp.concatenate([tile, jnp.zeros((LANES - KP, LANES), jnp.float32)], axis=0))[0:KP]
    real = jnp.where(k_row <= lane, tile, turned)
    imag = jnp.where(k_row > lane, tile, jnp.where(k_row < lane, -turned, 0.0))

    def spread(x, l):
        return jnp.broadcast_to(x[:, l : l + 1], (KP, LANES))

    per_l = halves * KP

    def fold_of(l, h):
        return fold_ref[pl.ds(l * per_l + h * KP, KP), :]

    def fold_turned(l, h):
        return jnp.concatenate(
            [fold_ref[pl.ds(k0 * per_l + h * KP + l, SUB, stride=per_l), :] for k0 in range(0, KP, SUB)], axis=0
        )

    def gram_of(l, h):
        if h == halves:
            return spread(real, l), spread(imag, l)
        return unfold((fold_of, fold_turned), l, h, k_row, count)

    sums = [(fold_of(count, h), fold_of(count + 1, h)) for h in range(halves)]
    sums.append((spread(tile, KP), spread(tile, KP + 1)))

    before = final - 1
    tiles = []
    per = reach // LANES
    low, high = jnp.maximum(mine - 1, 0), jnp.minimum(mine + 1, blocks - 1)
    for at, which in ((low, range(halves - per, halves)), (mine, range(halves)), (high, range(per))):
        for h in which:
            tiles.append([got_ref[before * blocks + at, c * halves + h : c * halves + h + 1] for c in range(2)])
    virtual = take_virtual(idx_ref, start - reach, reach, tiles, halves, count)
    near = spread(tile, KP + 2).astype(jnp.int32)
    total = [jnp.zeros((KP, LANES), jnp.float32) for _ in range(2)]
    for q in range(blocks):
        for h in range(halves):
            hit = lane == near - (q * pixels + h * LANES)
            for c in range(2):
                row = got_ref[before * blocks + q, c * halves + h : c * halves + h + 1]
                total[c] = total[c] + jnp.where(hit, row, 0.0)
    total = [jnp.broadcast_to(jnp.sum(x, axis=1, keepdims=True), (KP, LANES)) for x in total]
    total = [jnp.where(k_row < count, x, 0.0) for x in total]
    virtual.append(scaled([x[0:1] for x in total], *total))
    update(virtual, gram_of, fr_ref, fs_ref, fd_ref)

    zero = jnp.zeros((KP, LANES), jnp.float32)
    hr = [gr_ref[count, h] for h in range(halves)] + [zero]
    hi = [gi_ref[count, h] for h in range(halves)] + [zero]
    solve(virtual, fr_ref, fs_ref, fd_ref, hr, hi, sums, stack, beta_ref, state_ref)
    is_final = section == final
    for c in range(2):
        small_ref[c] = jnp.where(is_final, state_ref[c : c + 1, 0:pixels], comp0_ref[c : c + 1])

    def of_pixel(s):
        total = jnp.zeros((1, LANES), jnp.float32)
        for q in range(blocks):
            first = pixel_ref[0:1] - q * pixels
            here = jnp.logical_and(first >= 0, first < pixels)
            total = total + jnp.where(here, got_ref[s * blocks + q, 4 * halves : 4 * halves + 1], 0.0)
        return total

    def times(d, later, fr, fi):
        fr = jnp.where(later, fr, 1.0)
        fi = jnp.where(later, fi, 0.0)
        return (d[0] * fr - d[1] * fi, d[0] * fi + d[1] * fr)

    one = jnp.ones((1, LANES), jnp.float32)
    datum = [(one, 0.0 * one) for _ in range(halves + 1)]
    for h in range(halves + 1):
        datum[h] = times(datum[h], section < final, state_ref[2:3, half(h)], state_ref[3:4, half(h)])
    for s in range(final - 1, 0, -1):
        later = section < s
        own = [got_ref[s * blocks + mine, 2 * halves + m : 2 * halves + m + 1] for m in range(2 * halves)]
        row = of_pixel(s)
        for h in range(halves):
            datum[h] = times(datum[h], later, own[h], own[halves + h])
        f = [jnp.sum(jnp.where(lane[0:1] == LANES - 2 + c, row, 0.0), axis=1, keepdims=True) for c in range(2)]
        datum[halves] = times(datum[halves], later, *[jnp.broadcast_to(x, (1, LANES)) for x in f])

    zr = pltpu.roll(tile, LANES - Z_LANE, 1)
    zi = pltpu.roll(tile, LANES - Z_LANE - Z_STEP, 1)
    br, bi = beta_ref[0, halves], beta_ref[1, halves]
    zr, zi = jnp.where(k_row < count, zr, 0.0), jnp.where(k_row < count, zi, 0.0)
    last_r = state_ref[4:5, half(halves)] + colsum(zr * br - zi * bi)
    last_i = colsum(zr * bi + zi * br)
    row = of_pixel(jnp.minimum(section, final - 1))
    vr = jnp.where(is_final, last_r, row)
    vi = jnp.where(is_final, last_i, pltpu.roll(jnp.broadcast_to(row, (SUB, LANES)), LANES // 2, 1)[0:1])
    dr, di = datum[halves]
    ur, ui = unit(vr * dr - vi * di, vr * di + vi * dr)
    gain = math.sqrt(dates + 1)
    ur = jnp.transpose(jnp.broadcast_to(ur * gain, (LANES, LANES)))[0:dates]
    ui = jnp.transpose(jnp.broadcast_to(ui * gain, (LANES, LANES)))[0:dates]

    @pl.when(is_final)
    def _():
        make_vectors(zr_ref, zi_ref, beta_ref, state_ref, vec_ref)

    for h in range(halves):
        wr = ur * datum[h][0] + ui * datum[h][1]
        wi = ur * datum[h][1] - ui * datum[h][0]
        vr = jnp.where(is_final, vec_ref[0, :, half(h)], vec0_ref[0, :, half(h)])
        vi = jnp.where(is_final, vec_ref[1, :, half(h)], vec0_ref[1, :, half(h)])
        out_ref[:, 0, half(h)] = vr * wr - vi * wi
        out_ref[:, 1, half(h)] = vr * wi + vi * wr


def on_device(slc, neighbours, reference_pixel):
    dates, pixels = slc.shape[1:]
    slc = jnp.transpose(slc, (1, 0, 2))
    count = neighbours.shape[0]
    reach = min(pixels, REACH_LIMIT)
    sections = lax.axis_size("section")
    blocks = lax.axis_size("pix")
    block = lax.axis_index("pix")
    stack = dates + 1
    halves = pixels // LANES
    rows = up(dates, SUB)

    even = block % 2 == 0

    def swap(first, upper):
        pairs = [(i, i + 1) for i in range(first, blocks - 1, 2)]
        pairs += [(j, i) for i, j in pairs]
        sent = slc
        if reach < pixels:
            sent = jnp.where(upper, slc[:, :, pixels - reach :], slc[:, :, :reach])
        return lax.ppermute(sent, "pix", pairs)

    near = swap(0, even)
    far = swap(1, ~even)

    made = [
        f32(count, rows, pixels), f32(count, rows, pixels),
        f32(count + 1, halves, KP, LANES), f32(count + 1, halves, KP, LANES),
        f32(2, halves, KP, LANES), f32(2, halves, KP, LANES), f32(SUB, pixels), f32(2, pixels),
    ]
    zr, zi, own, neighbours = pl.pallas_call(
        own_kernel,
        out_shape=made[:2]
        + [f32(2 * rows, pixels + reach)]
        + [jax.ShapeDtypeStruct(neighbours.shape, jnp.int32)],
        in_specs=[HBM, HBM, VMEM],
        out_specs=[VMEM] * 4,
        scratch_shapes=[
            pltpu.VMEM((dates, 2, pixels), jnp.float32),
            pltpu.VMEM((4 * rows, pixels + reach), jnp.bfloat16),
            pltpu.SemaphoreType.DMA((2,)),
        ],
        compiler_params=params(),
        cost_estimate=cost(2 * 4 * rows * pixels * (pixels + reach) * count),
        name="own",
    )(*[pltpu.with_memory_space_constraint(x, pltpu.HBM) for x in (neighbours, slc)], near)

    def prepare(first, carried):
        outs = made if first else made[:7] + [f32((count + 2) * halves * KP, LANES)]
        return pl.pallas_call(
            functools.partial(prepare_kernel, stack, first),
            out_shape=outs,
            in_specs=[VMEM] * (3 + len(carried)),
            out_specs=[VMEM] * len(outs),
            scratch_shapes=([pltpu.VMEM((count, halves, KP, LANES), jnp.float32)] * 2 if first else [])
            + [
                pltpu.VMEM((2 * rows, reach), jnp.float32),
                pltpu.VMEM((4 * rows, reach), jnp.bfloat16),
                pltpu.VMEM((2, count + 1, count, SUB, LANES), jnp.float32),
            ],
            input_output_aliases={3 + n: n for n in range(len(carried))},
            compiler_params=params(),
            cost_estimate=cost(50 * 12 * rows * reach * pixels * count),
        )(neighbours, far, own, *carried)

    *made_0, comp = prepare(True, (zr, zi))
    zr, zi, gr, gi, sums, beta, state, folded = prepare(False, made_0)

    final = sections - 1
    folds = []
    for s in range(final):
        pairs = [(final * blocks + q, s * blocks + q) for q in range(blocks)]
        folds.append(lax.ppermute(folded, ("section", "pix"), pairs))
    folds.append(folded)

    for rnd in range(1, final):
        def hop(shift):
            pairs = [
                ((rnd - 1) * blocks + q, rnd * blocks + q + shift)
                for q in range(blocks)
                if 0 <= q + shift < blocks
            ]
            return lax.ppermute(comp, ("section", "pix"), pairs)

        last = rnd == final - 1
        late = (pixel, zr, zi) if last else ()
        scratch = [pltpu.VMEM((count, halves, KP, LANES), jnp.float32)] * 3
        outs = [f32(2, halves, KP, LANES), f32(SUB, pixels), f32(2, pixels)]
        if last:
            scratch += [pltpu.VMEM(o.shape, o.dtype) for o in outs[:2]]
            outs = outs[2:] + [f32(2, dates, pixels), f32(sections * blocks, slot_rows(halves), LANES)]
        call = pl.pallas_call(
            functools.partial(round_kernel, rnd, stack),
            out_shape=outs,
            in_specs=[VMEM] * (9 + len(late)),
            out_specs=[VMEM] * 3,
            scratch_shapes=scratch,
            compiler_params=params(),
        )
        near = (hop(1)[:, pixels - reach :], hop(0), hop(-1)[:, :reach])
        made = call(neighbours, *near, gr, gi, sums, beta, state, *late)
        if last:
            comp, vec, sent = made
        else:
            beta, state, comp = made
        if rnd == 1:
            pixel = lax.optimization_barrier((reference_pixel, comp))[0][0]
            pixel = jnp.full((SUB, LANES), pixel, jnp.int32)

    sent, *folds = lax.optimization_barrier((sent, *folds))
    got = lax.all_to_all(sent, ("section", "pix"), 0, 0, tiled=True)
    out, small = pl.pallas_call(
        functools.partial(finish_kernel, sections, stack),
        out_shape=[f32(dates, 2, pixels), f32(2, 1, pixels)],
        in_specs=[VMEM] * (10 + sections),
        out_specs=[VMEM] * 2,
        scratch_shapes=[
            pltpu.VMEM(folded.shape, jnp.float32),
            pltpu.VMEM((count, halves + 1, KP, LANES), jnp.float32),
            pltpu.VMEM((count, halves + 1, KP, LANES), jnp.float32),
            pltpu.VMEM((count, halves + 1, KP, LANES), jnp.float32),
            pltpu.VMEM((2, halves + 1, KP, LANES), jnp.float32),
            pltpu.VMEM((SUB, pixels + LANES), jnp.float32),
            pltpu.VMEM((2, dates, pixels), jnp.float32),
        ],
        compiler_params=params(),
        name="finish",
    )(pixel, neighbours, got, vec, comp, zr, zi, gr, gi, sums, *folds)
    return (jnp.transpose(out, (1, 0, 2)), small)


def solution(mesh):
    return jax.shard_map(
        on_device,
        mesh=mesh,
        in_specs=(P(None, "section", "pix"), P(None, "pix"), P()),
        out_specs=(P(None, "section", "pix"), P(None, "section", "pix")),
        check_vma=False,
    )
```

```python
import functools
import math

import jax
import jax.numpy as jnp
from jax import lax
from jax.experimental import pallas as pl
from jax.experimental.pallas import tpu as pltpu
from jax.sharding import PartitionSpec as P


ITERS = 16
FLOOR = 0.05
REACH_LIMIT = 256
LANES = 128
SUB = 8
KP = 16
Z_LANE, Z_STEP = 20, 54
SHRINK = 2.0**-35

VMEM = pl.BlockSpec(memory_space=pltpu.VMEM)
HBM = pl.BlockSpec(memory_space=pltpu.HBM)


def f32(*shape):
    return jax.ShapeDtypeStruct(shape, jnp.float32)


def params():
    return pltpu.CompilerParams(vmem_limit_bytes=20 * 1024 * 1024)


def cost(flops):
    return pl.CostEstimate(flops=flops, bytes_accessed=0, transcendentals=0)


def up(n, m):
    return -(-n // m) * m


def colsum(x):
    return jnp.sum(x, axis=0, keepdims=True)


def unit(real, imag):
    scale = 1.0 / jnp.maximum(jnp.sqrt(real * real + imag * imag), FLOOR)
    return (real * scale, imag * scale)


def seat(pixels, reach):
    section, block = lax.axis_index("section"), lax.axis_index("pix")
    even = block % 2 == 0
    return (
        section, block, lax.axis_size("pix"), block * pixels,
        jnp.where(even, pixels, -reach), jnp.where(even, -reach, pixels),
    )


def half(h):
    return pl.ds(h * LANES, LANES)


def gather(start, idx_ref, pieces, xs_ref, hl_ref, zr_ref, zi_ref, add):
    count, rows, pixels = zr_ref.shape
    xs_ref[...] = jnp.zeros_like(xs_ref)
    at = 0
    place = []
    for piece, first in pieces:
        dates, _, width = piece.shape
        for c in range(2):
            xs_ref[pl.ds(c * rows, dates), pl.ds(at, width)] = piece[:, c]
        place.append(lax.broadcasted_iota(jnp.int32, (width, pixels), 0) + first)
        at += width
    place = jnp.concatenate(place, axis=0)
    high = xs_ref[...].astype(jnp.bfloat16)
    hl_ref[0 : 2 * rows] = high
    hl_ref[2 * rows : 4 * rows] = (xs_ref[...] - high.astype(jnp.float32)).astype(jnp.bfloat16)
    for k in range(count):
        near = idx_ref[k : k + 1, :] - start
        hot = jnp.where(place == near, 1.0, 0.0).astype(jnp.bfloat16)
        got = jnp.dot(hl_ref[...], hot, preferred_element_type=jnp.float32)
        zr = got[0:rows] + got[2 * rows : 3 * rows]
        zi = got[rows : 2 * rows] + got[3 * rows : 4 * rows]
        zr_ref[k] = zr_ref[k] + zr if add else zr
        zi_ref[k] = zi_ref[k] + zi if add else zi


def scale_dates(zr_ref, zi_ref):
    count, rows, pixels = zr_ref.shape
    for h in range(pixels // LANES):
        for r in range(0, rows, SUB):
            power = None
            for k in range(count):
                a = zr_ref[k, pl.ds(r, SUB), half(h)]
                b = zi_ref[k, pl.ds(r, SUB), half(h)]
                power = a * a + b * b if power is None else power + (a * a + b * b)
            scale = lax.rsqrt(jnp.maximum(power, 1.0))
            for k in range(count):
                zr_ref[k, pl.ds(r, SUB), half(h)] *= scale
                zi_ref[k, pl.ds(r, SUB), half(h)] *= scale


def merge_rows(parts):
    row = lax.broadcasted_iota(jnp.int32, (SUB, LANES), 0)
    for step in (4, 2, 1):
        low = jnp.bitwise_and(row, step) == 0
        other = jnp.bitwise_xor(row, step)
        n = len(parts) // 2
        out = []
        for i in range(n):
            a, b = parts[i], parts[i + n]
            far = jnp.take_along_axis(jnp.where(low, b, a), other, axis=0, mode="promise_in_bounds")
            out.append(jnp.where(low, a, b) + far)
        parts = out
    return parts[0]


def gram(pair_ref, zr_ref, zi_ref, own_ref, gr_ref, gi_ref, sum_ref, block=3):
    count, rows, pixels = zr_ref.shape
    zero = jnp.zeros((SUB, LANES), jnp.float32)
    for h in range(pixels // LANES):
        def load(k, r):
            if k == count:
                return (own_ref[pl.ds(r, SUB), half(h)], own_ref[pl.ds(rows + r, SUB), half(h)])
            return (zr_ref[k, pl.ds(r, SUB), half(h)], zi_ref[k, pl.ds(r, SUB), half(h)])

        for k0 in range(0, count, block):
            for l0 in range(k0, count + 1, block):
                pairs = [
                    (k, l)
                    for k in range(k0, min(k0 + block, count))
                    for l in range(l0, min(l0 + block, count + 1))
                    if l >= k
                ]
                acc = {}
                for r in range(0, rows, SUB):
                    val = {n: load(n, r) for n in sorted({n for p in pairs for n in p})}
                    minus = {k: val[k][0] - val[k][1] for k in {k for k, l in pairs if k != l}}
                    plus = {l: val[l][0] + val[l][1] for l in {l for k, l in pairs if k != l}}
                    for k, l in pairs:
                        new = [val[k][0] * val[l][0], val[k][1] * val[l][1]]
                        if k != l:
                            new.append(minus[k] * plus[l])
                        acc[k, l] = [x + y for x, y in zip(acc[k, l], new)] if r else new
                for k, l in pairs:
                    pair_ref[0, l, k] = acc[k, l][0] + acc[k, l][1]
                    pair_ref[1, l, k] = zero if k == l else acc[k, l][2] - (acc[k, l][0] - acc[k, l][1])
        for c, g_ref in ((0, gr_ref), (1, gi_ref)):
            for l in range(count + 1):
                for kt in range(KP // SUB):
                    ks = range(kt * SUB, kt * SUB + SUB)
                    if min(ks) > min(l, count - 1):
                        continue
                    parts = [pair_ref[c, l, k] if k <= min(l, count - 1) else zero for k in ks]
                    g_ref[l, h, pl.ds(kt * SUB, SUB), :] = merge_rows(parts)
        row = lax.broadcasted_iota(jnp.int32, (SUB, LANES), 0)
        for c, g_ref in ((0, gr_ref), (1, gi_ref)):
            for l in range(count):
                for kt in range(KP // SUB):
                    ks = list(range(kt * SUB, kt * SUB + SUB))
                    if max(ks) <= l:
                        continue
                    other = jnp.concatenate(
                        [g_ref[k, h, pl.ds(l, 1), :] if l < k < count else zero[0:1] for k in ks], axis=0
                    )
                    if c:
                        other = -other
                    if min(ks) <= l:
                        other = jnp.where(row + ks[0] <= l, g_ref[l, h, pl.ds(kt * SUB, SUB), :], other)
                    g_ref[l, h, pl.ds(kt * SUB, SUB), :] = other
        for c in range(2):
            tiles = []
            for k in range(KP):
                total = None
                if k <= count:
                    for r in range(0, rows, SUB):
                        v = load(k, r)[c]
                        total = v if total is None else total + v
                tiles.append(zero if total is None else total)
            for kt in range(KP // SUB):
                sum_ref[c, h, pl.ds(kt * SUB, SUB), :] = merge_rows(tiles[kt * SUB : kt * SUB + SUB])


def turns(gr_ref, gs_ref, gd_ref, g0, count):
    halves = gr_ref.shape[1]

    def product(b, g):
        acc = [None] * halves
        for l in range(count):
            for h in range(halves):
                br = jnp.broadcast_to(b[h][0][l : l + 1], (KP, LANES))
                bi = jnp.broadcast_to(b[h][1][l : l + 1], (KP, LANES))
                new = [gr_ref[l, h] * (br + bi), gs_ref[l, h] * bi, gd_ref[l, h] * br]
                acc[h] = new if l == 0 else [x + y for x, y in zip(acc[h], new)]
        return [(g[h][0] + (t - u), g[h][1] + (t + v)) for h, (t, u, v) in enumerate(acc)]

    def step(_, carry):
        b, g = carry
        t = product(b, g)
        return tuple((b[h][0] + t[h][0], b[h][1] + t[h][1]) for h in range(halves)), g

    g = tuple(g0)
    b = g
    b, g = lax.fori_loop(0, ITERS // 2 - 1, step, (b, g))
    b = tuple((x * SHRINK, y * SHRINK) for x, y in b)
    g = tuple((x * SHRINK, y * SHRINK) for x, y in g)
    b, g = lax.fori_loop(0, ITERS - ITERS // 2, step, (b, g))
    return b, g, product(b, g)


def solve(virtual, gr_ref, gs_ref, gd_ref, hr, hi, sums, stack, beta_ref, state_ref):
    halves = gr_ref.shape[1]
    count = gr_ref.shape[0]
    first = 1.0 / math.sqrt(stack)
    g0 = []
    for h in range(halves):
        zr, zi = sums[h]
        row = lax.broadcasted_iota(jnp.int32, (KP, LANES), 0)
        zr = jnp.where(row < count, zr, 0.0)
        zi = jnp.where(row < count, zi, 0.0)
        if virtual is not None:
            zr = zr + virtual[h][1][0]
            zi = zi + virtual[h][1][1]
        g0.append((zr * first, zi * -first))
    b, g, t = turns(gr_ref, gs_ref, gd_ref, g0, count)
    for h in range(halves):
        norm = colsum(b[h][0] * (g[h][0] + t[h][0]) + b[h][1] * (g[h][1] + t[h][1]))
        inv = lax.rsqrt(SHRINK * SHRINK + norm)
        br, bi = b[h][0] * inv, b[h][1] * inv
        a = inv * (SHRINK * first)
        xr, xi = hr[h], hi[h]
        sr, si = (x[count : count + 1] for x in sums[h])
        fr, fi = a, jnp.zeros_like(a)
        if virtual is not None:
            (wr, wi), (zr, zi) = virtual[h]
            xr, xi = xr + (zr * wr + zi * wi), xi + (zr * wi - zi * wr)
            sr, si = sr + wr, si + wi
            fr = a + colsum(zr * br - zi * bi)
            fi = colsum(zr * bi + zi * br)
        beta_ref[0, h] = br
        beta_ref[1, h] = bi
        fr, fi = unit(fr, fi)
        state_ref[0:1, half(h)] = a * sr + colsum(br * xr + bi * xi)
        state_ref[1:2, half(h)] = a * si + colsum(br * xi - bi * xr)
        state_ref[2:3, half(h)] = fr
        state_ref[3:4, half(h)] = fi
        state_ref[4:5, half(h)] = a
        state_ref[5:8, half(h)] = jnp.zeros((3, LANES), jnp.float32)


def own_kernel(idx_hbm, slc_hbm, near_ref, zr_ref, zi_ref, own_ref, idx_ref, slc_ref, hl_ref, sems):
    copies = [
        pltpu.make_async_copy(slc_hbm, slc_ref, sems.at[0]),
        pltpu.make_async_copy(idx_hbm, idx_ref, sems.at[1]),
    ]
    for copy in copies:
        copy.start()
    for copy in copies:
        copy.wait()
    _, _, _, start, near_at, _ = seat(slc_ref.shape[2], near_ref.shape[2])
    gather(start, idx_ref, ((slc_ref, 0), (near_ref, near_at)), own_ref, hl_ref, zr_ref, zi_ref, False)


def prepare_kernel(stack, first, idx_ref, far_ref, own_ref, *refs):
    refs = refs[2 if first else 7 :]
    zr_ref, zi_ref, gr_ref, gi_ref, sum_ref, beta_ref, state_ref = refs[:7]
    xs_ref, hl_ref, pair_ref = refs[-3:]

    section, _, _, start, _, far_at = seat(zr_ref.shape[2], far_ref.shape[2])

    @pl.when(section == 0 if first else section != 0)
    def _():
        count = zr_ref.shape[0]
        gather(start, idx_ref, ((far_ref, far_at),), xs_ref, hl_ref, zr_ref, zi_ref, True)
        scale_dates(zr_ref, zi_ref)
        gram(pair_ref, zr_ref, zi_ref, own_ref, gr_ref, gi_ref, sum_ref)
        if first:
            halves = gr_ref.shape[1]
            hr = [gr_ref[count, h] for h in range(halves)]
            hi = [gi_ref[count, h] for h in range(halves)]
            sums = [(sum_ref[0, h], sum_ref[1, h]) for h in range(halves)]
            gs_ref, gd_ref = refs[8:10]
            for l in range(count):
                for h in range(halves):
                    gs_ref[l, h] = gi_ref[l, h] + gr_ref[l, h]
                    gd_ref[l, h] = gi_ref[l, h] - gr_ref[l, h]
            solve(None, gr_ref.at[0:count], gs_ref, gd_ref, hr, hi, sums, stack, beta_ref, state_ref)
            refs[7][...] = state_ref[0:2]

    if not first:

        @pl.when(section == lax.axis_size("section") - 1)
        def _():
            fold(gr_ref, gi_ref, sum_ref, refs[7])


def folded_column(l, h, gr_ref, gi_ref, sum_ref):
    count = gr_ref.shape[0] - 1
    if l >= count:
        return sum_ref[l - count, h]
    k_row = lax.broadcasted_iota(jnp.int32, (KP, LANES), 0)
    return jnp.where(k_row <= l, gr_ref[l, h], gi_ref[l, h])


def fold(gr_ref, gi_ref, sum_ref, fold_ref):
    halves = gr_ref.shape[1]
    for l in range(gr_ref.shape[0] + 1):
        for h in range(halves):
            fold_ref[pl.ds((l * halves + h) * KP, KP), :] = folded_column(l, h, gr_ref, gi_ref, sum_ref)


def make_tile(start, pixel_ref, idx_ref, zr_ref, zi_ref, gr_ref, gi_ref, sum_ref):
    count, rows, pixels = zr_ref.shape
    halves = pixels // LANES
    lane = lax.broadcasted_iota(jnp.int32, (KP, LANES), 1)
    local = pixel_ref[...] - start
    hit = [lax.broadcasted_iota(jnp.int32, (SUB, LANES), 1) == local - h * LANES for h in range(halves)]

    def column(parts):
        total = None
        for h, part in enumerate(parts):
            mask = jnp.concatenate([hit[h]] * (part.shape[0] // SUB), axis=0)
            part = jnp.where(mask, part, 0.0)
            total = part if total is None else total + part
        return jnp.broadcast_to(jnp.sum(total, axis=1, keepdims=True), total.shape)

    tile = jnp.zeros((KP, LANES), jnp.float32)
    for l in range(count + 2):
        parts = [folded_column(l, h, gr_ref, gi_ref, sum_ref) for h in range(halves)]
        tile = jnp.where(lane == (l if l < count else KP + l - count), column(parts), tile)
    pad = jnp.zeros((KP - count, LANES), jnp.float32)
    near = [jnp.concatenate([idx_ref[:, half(h)].astype(jnp.float32), pad], axis=0) for h in range(halves)]
    tile = jnp.where(lane == KP + 2, column(near), tile)
    wide = lax.broadcasted_iota(jnp.int32, (rows, LANES), 1)
    empty = jnp.zeros((LANES - rows, LANES), jnp.float32)
    for c, ref in ((0, zr_ref), (1, zi_ref)):
        both = jnp.zeros((rows, LANES), jnp.float32)
        for k in range(count):
            both = jnp.where(wide == k, column([ref[k, :, half(h)] for h in range(halves)]), both)
        turned = jnp.transpose(jnp.concatenate([both, empty], axis=0))[0:KP]
        at = Z_LANE + c * Z_STEP
        tile = jnp.where(jnp.logical_and(lane >= at, lane < at + Z_STEP), pltpu.roll(turned, at, 1), tile)
    return tile


def lane_take(x, i):
    return jnp.take_along_axis(x, i, axis=1, mode="promise_in_bounds")


def scaled(own, zr, zi):
    scale = lax.rsqrt(jnp.maximum(colsum(zr * zr + zi * zi), 1.0))
    return own, (zr * scale, zi * scale)


def take_virtual(idx_ref, base, reach, tiles, halves, count):
    virtual = []
    for h in range(halves):
        parts = []
        for kt in range(KP // SUB):
            rows = min(SUB, count - kt * SUB)
            raw = idx_ref[pl.ds(kt * SUB, rows), half(h)] - base
            if rows < SUB:
                raw = jnp.concatenate([raw, jnp.full((SUB - rows, LANES), -1, jnp.int32)], axis=0)
            lane = jnp.bitwise_and(raw, LANES - 1)
            tile = jnp.right_shift(raw, 7)
            both = []
            for c in range(2):
                out = jnp.zeros((SUB, LANES), jnp.float32)
                for n in range(h, h + 2 * reach // LANES + 1):
                    got = lane_take(jnp.broadcast_to(tiles[n][c], (SUB, LANES)), lane)
                    out = jnp.where(tile == n, got, out)
                both.append(out)
            parts.append(both)
        zr = jnp.concatenate([p[0] for p in parts], axis=0)
        zi = jnp.concatenate([p[1] for p in parts], axis=0)
        virtual.append(scaled(tiles[reach // LANES + h], zr, zi))
    return virtual


def update(virtual, gram_of, fr_ref, fs_ref, fd_ref):
    for h, (_, (zr, zi)) in enumerate(virtual):
        for l in range(fr_ref.shape[0]):
            gr, gi = gram_of(l, h)
            br = jnp.broadcast_to(zr[l : l + 1], (KP, LANES))
            bi = jnp.broadcast_to(zi[l : l + 1], (KP, LANES))
            gr = gr + (zr * br + zi * bi)
            gi = gi + (zr * bi - zi * br)
            fr_ref[l, h] = gr
            fs_ref[l, h] = gi + gr
            fd_ref[l, h] = gi - gr


def round_kernel(
    rnd, stack, idx_ref, low_ref, own_ref, high_ref,
    gr_ref, gi_ref, sum_ref, beta0_ref, state0_ref, *refs,
):
    last = len(refs) > 6
    if last:
        late, (comp_ref, *made), refs = refs[:5], refs[5:8], refs[8:]
        fr_ref, fs_ref, fd_ref, beta_ref, state_ref = refs
    else:
        beta_ref, state_ref, comp_ref, fr_ref, fs_ref, fd_ref = refs
    count = gr_ref.shape[0] - 1
    halves = gr_ref.shape[1]
    reach = low_ref.shape[1]
    beta_ref[...] = beta0_ref[...]
    state_ref[...] = state0_ref[...]
    section, _, _, start, _, _ = seat(own_ref.shape[1], reach)

    @pl.when(section == rnd)
    def _():
        tiles = []
        for ref in (low_ref, own_ref, high_ref):
            for t in range(ref.shape[1] // LANES):
                tiles.append([ref[c : c + 1, half(t)] for c in range(2)])
        virtual = take_virtual(idx_ref, start - reach, reach, tiles, halves, count)
        update(virtual, lambda l, h: (gr_ref[l, h], gi_ref[l, h]), fr_ref, fs_ref, fd_ref)
        hr = [gr_ref[count, h] for h in range(halves)]
        hi = [gi_ref[count, h] for h in range(halves)]
        sums = [(sum_ref[0, h], sum_ref[1, h]) for h in range(halves)]
        solve(virtual, fr_ref, fs_ref, fd_ref, hr, hi, sums, stack, beta_ref, state_ref)

    comp_ref[...] = state_ref[0:2]
    if last:
        vectors(*late, beta_ref, state_ref, *made)


def slot_rows(halves):
    return max(up(4 * halves, SUB), KP // 2)


def tile_kernel(pixel_ref, idx_ref, zr_ref, zi_ref, gr_ref, gi_ref, sum_ref, tile_ref):
    section, _, _, start, _, _ = seat(zr_ref.shape[2], 0)
    final = lax.axis_size("section") - 1

    @pl.when(section == final)
    def _():
        tile_ref[...] = make_tile(start, pixel_ref, idx_ref, zr_ref, zi_ref, gr_ref, gi_ref, sum_ref)

    @pl.when(section != final)
    def _():
        tile_ref[...] = jnp.zeros_like(tile_ref)


def make_vectors(zr_ref, zi_ref, beta_ref, state_ref, vec_ref):
    count, rows, pixels = zr_ref.shape
    dates = vec_ref.shape[1]
    out = [[], []]
    for h in range(pixels // LANES):
        a = state_ref[4:5, half(h)]
        acc_r = [jnp.broadcast_to(a, (SUB, LANES)) for _ in range(0, rows, SUB)]
        acc_i = [jnp.zeros((SUB, LANES), jnp.float32) for _ in range(0, rows, SUB)]
        for k in range(count):
            br = jnp.broadcast_to(beta_ref[0, h, k : k + 1, :], (SUB, LANES))
            bi = jnp.broadcast_to(beta_ref[1, h, k : k + 1, :], (SUB, LANES))
            for n, r in enumerate(range(0, rows, SUB)):
                zr = zr_ref[k, pl.ds(r, SUB), half(h)]
                zi = zi_ref[k, pl.ds(r, SUB), half(h)]
                acc_r[n] = acc_r[n] + (zr * br - zi * bi)
                acc_i[n] = acc_i[n] + (zr * bi + zi * br)
        for c, acc in ((0, acc_r), (1, acc_i)):
            whole = jnp.concatenate(acc, axis=0)
            vec_ref[c, :, half(h)] = whole[0:dates]
            out[c].append(whole)
    return out


def vectors(pixel_ref, zr_ref, zi_ref, tile_ref, other_ref, beta_ref, state_ref, vec_ref, slot_ref):
    _, rows, pixels = zr_ref.shape
    halves = pixels // LANES
    section, block, blocks, start, _, _ = seat(pixels, 0)

    @pl.when(section < lax.axis_size("section") - 1)
    def _():
        local = pixel_ref[...] - start
        lane = lax.broadcasted_iota(jnp.int32, (SUB, LANES), 1)
        row = lax.broadcasted_iota(jnp.int32, (SUB, LANES), 0)
        at_pixel = [jnp.zeros((SUB, LANES), jnp.float32) for _ in range(2)]
        vecs = make_vectors(zr_ref, zi_ref, beta_ref, state_ref, vec_ref)
        for c in range(2):
            for h in range(halves):
                empty = jnp.zeros((LANES - rows, LANES), jnp.float32)
                turned = jnp.transpose(jnp.concatenate([vecs[c][h], empty], axis=0))
                for r in range(0, LANES, SUB):
                    at_pixel[c] = at_pixel[c] + jnp.where(row == local - (h * LANES + r), turned[r : r + SUB], 0.0)
        virtual, f_rows = (
            [state_ref[c : c + 1, half(h)] for c in cs for h in range(halves)] for cs in ((0, 1), (2, 3))
        )
        mixed = colsum(at_pixel[0]) + pltpu.roll(jnp.broadcast_to(colsum(at_pixel[1]), (SUB, LANES)), LANES // 2, 1)[0:1]
        for c in range(2):
            picked = jnp.zeros((1, LANES), jnp.float32)
            for h in range(halves):
                picked = picked + jnp.where((lane == local - h * LANES)[0:1], state_ref[2 + c : 3 + c, half(h)], 0.0)
            f = jnp.sum(picked, axis=1, keepdims=True)
            mixed = jnp.where(lane[0:1] == LANES - 2 + c, jnp.broadcast_to(f, (1, LANES)), mixed)
        spare = slot_ref.shape[1] - 2 * halves
        kinds = []
        for more in (f_rows, [mixed]):
            empty = [jnp.zeros((1, LANES), jnp.float32)] * (spare - len(more))
            kinds.append(jnp.concatenate(virtual + more + empty, axis=0))
        for n in range(slot_ref.shape[0]):
            with_f = jnp.logical_and(block == n % blocks, n // blocks < section)
            slot_ref[n] = jnp.where(with_f, *kinds)

    @pl.when(section == lax.axis_size("section") - 1)
    def _():
        tile = tile_ref[...] + other_ref[...]
        tile = jnp.where(block % 2 == 0, tile[0 : KP // 2], tile[KP // 2 :])
        for n in range(slot_ref.shape[0]):
            slot_ref[n, 0 : KP // 2] = tile


def unfold(fold, l, h, k_row, count):
    straight, turned = fold[0](l, h), jnp.where(k_row < count, fold[1](l, h), 0.0)
    return (
        jnp.where(k_row <= l, straight, turned),
        jnp.where(k_row > l, straight, jnp.where(k_row < l, -turned, 0.0)),
    )


def finish_kernel(
    sections, stack, pixel_ref, idx_ref, got_ref, vec0_ref, comp0_ref, zr_ref, zi_ref, gr_ref, gi_ref, sum_ref, *refs
):
    folds, (out_ref, small_ref), refs = refs[:sections], refs[sections : sections + 2], refs[sections + 2 :]
    fold_ref, fr_ref, fs_ref, fd_ref, beta_ref, state_ref, vec_ref = refs
    dates, pixels = vec_ref.shape[1:]
    count = zr_ref.shape[0]
    section, mine, blocks, start, _, _ = seat(pixels, 0)
    halves = pixels // LANES
    final = sections - 1
    reach = min(pixels, REACH_LIMIT)

    for s in range(sections):

        @pl.when(section == s)
        def _(s=s):
            fold_ref[...] = folds[s][...]

    tile = [got_ref[final * blocks + q, 0 : KP // 2] for q in range(2)]
    for q in range(2, blocks):
        tile[q % 2] = tile[q % 2] + got_ref[final * blocks + q, 0 : KP // 2]
    tile = jnp.concatenate(tile, axis=0)
    k_row = lax.broadcasted_iota(jnp.int32, (KP, LANES), 0)
    lane = lax.broadcasted_iota(jnp.int32, (KP, LANES), 1)
    turned = jnp.transpose(jnp.concatenate([tile, jnp.zeros((LANES - KP, LANES), jnp.float32)], axis=0))[0:KP]
    real = jnp.where(k_row <= lane, tile, turned)
    imag = jnp.where(k_row > lane, tile, jnp.where(k_row < lane, -turned, 0.0))

    def spread(x, l):
        return jnp.broadcast_to(x[:, l : l + 1], (KP, LANES))

    per_l = halves * KP

    def fold_of(l, h):
        return fold_ref[pl.ds(l * per_l + h * KP, KP), :]

    def fold_turned(l, h):
        return jnp.concatenate(
            [fold_ref[pl.ds(k0 * per_l + h * KP + l, SUB, stride=per_l), :] for k0 in range(0, KP, SUB)], axis=0
        )

    def gram_of(l, h):
        if h == halves:
            return spread(real, l), spread(imag, l)
        return unfold((fold_of, fold_turned), l, h, k_row, count)

    sums = [(fold_of(count, h), fold_of(count + 1, h)) for h in range(halves)]
    sums.append((spread(tile, KP), spread(tile, KP + 1)))

    before = final - 1
    tiles = []
    per = reach // LANES
    low, high = jnp.maximum(mine - 1, 0), jnp.minimum(mine + 1, blocks - 1)
    for at, which in ((low, range(halves - per, halves)), (mine, range(halves)), (high, range(per))):
        for h in which:
            tiles.append([got_ref[before * blocks + at, c * halves + h : c * halves + h + 1] for c in range(2)])
    virtual = take_virtual(idx_ref, start - reach, reach, tiles, halves, count)
    near = spread(tile, KP + 2).astype(jnp.int32)
    total = [jnp.zeros((KP, LANES), jnp.float32) for _ in range(2)]
    for q in range(blocks):
        for h in range(halves):
            hit = lane == near - (q * pixels + h * LANES)
            for c in range(2):
                row = got_ref[before * blocks + q, c * halves + h : c * halves + h + 1]
                total[c] = total[c] + jnp.where(hit, row, 0.0)
    total = [jnp.broadcast_to(jnp.sum(x, axis=1, keepdims=True), (KP, LANES)) for x in total]
    total = [jnp.where(k_row < count, x, 0.0) for x in total]
    virtual.append(scaled([x[0:1] for x in total], *total))
    update(virtual, gram_of, fr_ref, fs_ref, fd_ref)

    zero = jnp.zeros((KP, LANES), jnp.float32)
    hr = [gr_ref[count, h] for h in range(halves)] + [zero]
    hi = [gi_ref[count, h] for h in range(halves)] + [zero]
    solve(virtual, fr_ref, fs_ref, fd_ref, hr, hi, sums, stack, beta_ref, state_ref)
    is_final = section == final
    for c in range(2):
        small_ref[c] = jnp.where(is_final, state_ref[c : c + 1, 0:pixels], comp0_ref[c : c + 1])

    def of_pixel(s, later):
        total = jnp.zeros((1, LANES), jnp.float32)
        for q in range(blocks):
            first = pixel_ref[0:1] - q * pixels
            here = jnp.logical_and(first >= 0, first < pixels)
            here = jnp.logical_and(here, jnp.logical_not(jnp.logical_and(later, mine == q)))
            total = total + jnp.where(here, got_ref[s * blocks + q, 2 * halves : 2 * halves + 1], 0.0)
        return total

    def times(d, later, fr, fi):
        fr = jnp.where(later, fr, 1.0)
        fi = jnp.where(later, fi, 0.0)
        return (d[0] * fr - d[1] * fi, d[0] * fi + d[1] * fr)

    one = jnp.ones((1, LANES), jnp.float32)
    datum = [(one, 0.0 * one) for _ in range(halves + 1)]
    for h in range(halves + 1):
        datum[h] = times(datum[h], section < final, state_ref[2:3, half(h)], state_ref[3:4, half(h)])
    for s in range(final - 1, 0, -1):
        later = section < s
        own = [got_ref[s * blocks + mine, 2 * halves + m : 2 * halves + m + 1] for m in range(2 * halves)]
        row = of_pixel(s, later)
        for h in range(halves):
            datum[h] = times(datum[h], later, own[h], own[halves + h])
        f = []
        for c in range(2):
            total = jnp.where(lane[0:1] == LANES - 2 + c, row, 0.0)
            for h in range(halves):
                total = total + jnp.where(lane[0:1] == pixel_ref[0:1] - start - h * LANES, own[c * halves + h], 0.0)
            f.append(jnp.sum(total, axis=1, keepdims=True))
        datum[halves] = times(datum[halves], later, *[jnp.broadcast_to(x, (1, LANES)) for x in f])

    zr = pltpu.roll(tile, LANES - Z_LANE, 1)
    zi = pltpu.roll(tile, LANES - Z_LANE - Z_STEP, 1)
    br, bi = beta_ref[0, halves], beta_ref[1, halves]
    zr, zi = jnp.where(k_row < count, zr, 0.0), jnp.where(k_row < count, zi, 0.0)
    last_r = state_ref[4:5, half(halves)] + colsum(zr * br - zi * bi)
    last_i = colsum(zr * bi + zi * br)
    row = of_pixel(jnp.minimum(section, final - 1), False)
    vr = jnp.where(is_final, last_r, row)
    vi = jnp.where(is_final, last_i, pltpu.roll(jnp.broadcast_to(row, (SUB, LANES)), LANES // 2, 1)[0:1])
    dr, di = datum[halves]
    ur, ui = unit(vr * dr - vi * di, vr * di + vi * dr)
    gain = math.sqrt(dates + 1)
    ur = jnp.transpose(jnp.broadcast_to(ur * gain, (LANES, LANES)))[0:dates]
    ui = jnp.transpose(jnp.broadcast_to(ui * gain, (LANES, LANES)))[0:dates]

    @pl.when(is_final)
    def _():
        make_vectors(zr_ref, zi_ref, beta_ref, state_ref, vec_ref)

    for h in range(halves):
        wr = ur * datum[h][0] + ui * datum[h][1]
        wi = ur * datum[h][1] - ui * datum[h][0]
        vr = jnp.where(is_final, vec_ref[0, :, half(h)], vec0_ref[0, :, half(h)])
        vi = jnp.where(is_final, vec_ref[1, :, half(h)], vec0_ref[1, :, half(h)])
        out_ref[:, 0, half(h)] = vr * wr - vi * wi
        out_ref[:, 1, half(h)] = vr * wi + vi * wr


def on_device(slc, neighbours, reference_pixel):
    dates, pixels = slc.shape[1:]
    slc = jnp.transpose(slc, (1, 0, 2))
    count = neighbours.shape[0]
    reach = min(pixels, REACH_LIMIT)
    sections = lax.axis_size("section")
    blocks = lax.axis_size("pix")
    block = lax.axis_index("pix")
    stack = dates + 1
    halves = pixels // LANES
    rows = up(dates, SUB)

    even = block % 2 == 0

    def swap(first, upper):
        pairs = [(i, i + 1) for i in range(first, blocks - 1, 2)]
        pairs += [(j, i) for i, j in pairs]
        sent = slc
        if reach < pixels:
            sent = jnp.where(upper, slc[:, :, pixels - reach :], slc[:, :, :reach])
        return lax.ppermute(sent, "pix", pairs)

    near = swap(0, even)
    far = swap(1, ~even)

    made = [
        f32(count, rows, pixels), f32(count, rows, pixels),
        f32(count + 1, halves, KP, LANES), f32(count + 1, halves, KP, LANES),
        f32(2, halves, KP, LANES), f32(2, halves, KP, LANES), f32(SUB, pixels), f32(2, pixels),
    ]
    zr, zi, own, neighbours = pl.pallas_call(
        own_kernel,
        out_shape=made[:2]
        + [f32(2 * rows, pixels + reach)]
        + [jax.ShapeDtypeStruct(neighbours.shape, jnp.int32)],
        in_specs=[HBM, HBM, VMEM],
        out_specs=[VMEM] * 4,
        scratch_shapes=[
            pltpu.VMEM((dates, 2, pixels), jnp.float32),
            pltpu.VMEM((4 * rows, pixels + reach), jnp.bfloat16),
            pltpu.SemaphoreType.DMA((2,)),
        ],
        compiler_params=params(),
        cost_estimate=cost(2 * 4 * rows * pixels * (pixels + reach) * count),
        name="own",
    )(*[pltpu.with_memory_space_constraint(x, pltpu.HBM) for x in (neighbours, slc)], near)

    def prepare(first, carried):
        outs = made if first else made[:7] + [f32((count + 2) * halves * KP, LANES)]
        return pl.pallas_call(
            functools.partial(prepare_kernel, stack, first),
            out_shape=outs,
            in_specs=[VMEM] * (3 + len(carried)),
            out_specs=[VMEM] * len(outs),
            scratch_shapes=([pltpu.VMEM((count, halves, KP, LANES), jnp.float32)] * 2 if first else [])
            + [
                pltpu.VMEM((2 * rows, reach), jnp.float32),
                pltpu.VMEM((4 * rows, reach), jnp.bfloat16),
                pltpu.VMEM((2, count + 1, count, SUB, LANES), jnp.float32),
            ],
            input_output_aliases={3 + n: n for n in range(len(carried))},
            compiler_params=params(),
            cost_estimate=cost(50 * 12 * rows * reach * pixels * count),
        )(neighbours, far, own, *carried)

    *made_0, comp = prepare(True, (zr, zi))
    zr, zi, gr, gi, sums, beta, state, folded = prepare(False, made_0)

    final = sections - 1
    folds = []
    for s in range(final):
        pairs = [(final * blocks + q, s * blocks + q) for q in range(blocks)]
        folds.append(lax.ppermute(folded, ("section", "pix"), pairs))
    folds.append(folded)

    for rnd in range(1, final):
        def hop(shift):
            pairs = [
                ((rnd - 1) * blocks + q, rnd * blocks + q + shift)
                for q in range(blocks)
                if 0 <= q + shift < blocks
            ]
            return lax.ppermute(comp, ("section", "pix"), pairs)

        last = rnd == final - 1
        late = (pixel, zr, zi, tile, other) if last else ()
        scratch = [pltpu.VMEM((count, halves, KP, LANES), jnp.float32)] * 3
        outs = [f32(2, halves, KP, LANES), f32(SUB, pixels), f32(2, pixels)]
        if last:
            scratch += [pltpu.VMEM(o.shape, o.dtype) for o in outs[:2]]
            outs = outs[2:] + [f32(2, dates, pixels), f32(sections * blocks, slot_rows(halves), LANES)]
        call = pl.pallas_call(
            functools.partial(round_kernel, rnd, stack),
            out_shape=outs,
            in_specs=[VMEM] * (9 + len(late)),
            out_specs=[VMEM] * 3,
            scratch_shapes=scratch,
            compiler_params=params(),
        )
        near = (hop(1)[:, pixels - reach :], hop(0), hop(-1)[:, :reach])
        made = call(neighbours, *near, gr, gi, sums, beta, state, *late)
        if last:
            comp, vec, sent = made
        else:
            beta, state, comp = made
        if rnd == 1:
            pixel = lax.optimization_barrier((reference_pixel, comp))[0][0]
            pixel = jnp.full((SUB, LANES), pixel, jnp.int32)
            tile = pl.pallas_call(
                tile_kernel,
                out_shape=f32(KP, LANES),
                in_specs=[VMEM] * 7,
                out_specs=VMEM,
                compiler_params=params(),
                name="tile",
            )(pixel, neighbours, zr, zi, gr, gi, sums)
            pairs = [(final * blocks + q, final * blocks + (q ^ 1)) for q in range(blocks)]
            other = lax.ppermute(tile, ("section", "pix"), pairs)

    sent, *folds = lax.optimization_barrier((sent, *folds))
    got = lax.all_to_all(sent, ("section", "pix"), 0, 0, tiled=True)
    out, small = pl.pallas_call(
        functools.partial(finish_kernel, sections, stack),
        out_shape=[f32(dates, 2, pixels), f32(2, 1, pixels)],
        in_specs=[VMEM] * (10 + sections),
        out_specs=[VMEM] * 2,
        scratch_shapes=[
            pltpu.VMEM(folded.shape, jnp.float32),
            pltpu.VMEM((count, halves + 1, KP, LANES), jnp.float32),
            pltpu.VMEM((count, halves + 1, KP, LANES), jnp.float32),
            pltpu.VMEM((count, halves + 1, KP, LANES), jnp.float32),
            pltpu.VMEM((2, halves + 1, KP, LANES), jnp.float32),
            pltpu.VMEM((SUB, pixels + LANES), jnp.float32),
            pltpu.VMEM((2, dates, pixels), jnp.float32),
        ],
        compiler_params=params(),
        name="finish",
    )(pixel, neighbours, got, vec, comp, zr, zi, gr, gi, sums, *folds)
    return (jnp.transpose(out, (1, 0, 2)), small)


def solution(mesh):
    return jax.shard_map(
        on_device,
        mesh=mesh,
        in_specs=(P(None, "section", "pix"), P(None, "pix"), P()),
        out_specs=(P(None, "section", "pix"), P(None, "section", "pix")),
        check_vma=False,
    )
```

```python
import functools
import math

import jax
import jax.numpy as jnp
from jax import lax
from jax.experimental import pallas as pl
from jax.experimental.pallas import tpu as pltpu
from jax.sharding import PartitionSpec as P


ITERS = 16
FLOOR = 0.05
REACH_LIMIT = 256
LANES = 128
SUB = 8
KP = 16
Z_LANE, Z_STEP = 20, 54
SHRINK = 2.0**-35

VMEM = pl.BlockSpec(memory_space=pltpu.VMEM)
HBM = pl.BlockSpec(memory_space=pltpu.HBM)


def f32(*shape):
    return jax.ShapeDtypeStruct(shape, jnp.float32)


def params():
    return pltpu.CompilerParams(vmem_limit_bytes=20 * 1024 * 1024)


def cost(flops):
    return pl.CostEstimate(flops=flops, bytes_accessed=0, transcendentals=0)


def up(n, m):
    return -(-n // m) * m


def colsum(x):
    return jnp.sum(x, axis=0, keepdims=True)


def unit(real, imag):
    scale = 1.0 / jnp.maximum(jnp.sqrt(real * real + imag * imag), FLOOR)
    return (real * scale, imag * scale)


def seat(pixels, reach):
    section, block = lax.axis_index("section"), lax.axis_index("pix")
    even = block % 2 == 0
    return (
        section, block, lax.axis_size("pix"), block * pixels,
        jnp.where(even, pixels, -reach), jnp.where(even, -reach, pixels),
    )


def half(h):
    return pl.ds(h * LANES, LANES)


def gather(start, idx_ref, pieces, xs_ref, hl_ref, zr_ref, zi_ref, add):
    count, rows, pixels = zr_ref.shape
    xs_ref[...] = jnp.zeros_like(xs_ref)
    at = 0
    place = []
    for piece, first in pieces:
        dates, _, width = piece.shape
        for c in range(2):
            xs_ref[pl.ds(c * rows, dates), pl.ds(at, width)] = piece[:, c]
        place.append(lax.broadcasted_iota(jnp.int32, (width, pixels), 0) + first)
        at += width
    place = jnp.concatenate(place, axis=0)
    high = xs_ref[...].astype(jnp.bfloat16)
    hl_ref[0 : 2 * rows] = high
    hl_ref[2 * rows : 4 * rows] = (xs_ref[...] - high.astype(jnp.float32)).astype(jnp.bfloat16)
    for k in range(count):
        near = idx_ref[k : k + 1, :] - start
        hot = jnp.where(place == near, 1.0, 0.0).astype(jnp.bfloat16)
        got = jnp.dot(hl_ref[...], hot, preferred_element_type=jnp.float32)
        zr = got[0:rows] + got[2 * rows : 3 * rows]
        zi = got[rows : 2 * rows] + got[3 * rows : 4 * rows]
        zr_ref[k] = zr_ref[k] + zr if add else zr
        zi_ref[k] = zi_ref[k] + zi if add else zi


def scale_dates(zr_ref, zi_ref):
    count, rows, pixels = zr_ref.shape
    for h in range(pixels // LANES):
        for r in range(0, rows, SUB):
            power = None
            for k in range(count):
                a = zr_ref[k, pl.ds(r, SUB), half(h)]
                b = zi_ref[k, pl.ds(r, SUB), half(h)]
                power = a * a + b * b if power is None else power + (a * a + b * b)
            scale = lax.rsqrt(jnp.maximum(power, 1.0))
            for k in range(count):
                zr_ref[k, pl.ds(r, SUB), half(h)] *= scale
                zi_ref[k, pl.ds(r, SUB), half(h)] *= scale


def merge_rows(parts):
    row = lax.broadcasted_iota(jnp.int32, (SUB, LANES), 0)
    for step in (4, 2, 1):
        low = jnp.bitwise_and(row, step) == 0
        other = jnp.bitwise_xor(row, step)
        n = len(parts) // 2
        out = []
        for i in range(n):
            a, b = parts[i], parts[i + n]
            far = jnp.take_along_axis(jnp.where(low, b, a), other, axis=0, mode="promise_in_bounds")
            out.append(jnp.where(low, a, b) + far)
        parts = out
    return parts[0]


def gram(pair_ref, zr_ref, zi_ref, own_ref, gr_ref, gi_ref, sum_ref, block=3):
    count, rows, pixels = zr_ref.shape
    zero = jnp.zeros((SUB, LANES), jnp.float32)
    for h in range(pixels // LANES):
        def load(k, r):
            if k == count:
                return (own_ref[pl.ds(r, SUB), half(h)], own_ref[pl.ds(rows + r, SUB), half(h)])
            return (zr_ref[k, pl.ds(r, SUB), half(h)], zi_ref[k, pl.ds(r, SUB), half(h)])

        for k0 in range(0, count, block):
            for l0 in range(k0, count + 1, block):
                pairs = [
                    (k, l)
                    for k in range(k0, min(k0 + block, count))
                    for l in range(l0, min(l0 + block, count + 1))
                    if l >= k
                ]
                acc = {}
                for r in range(0, rows, SUB):
                    val = {n: load(n, r) for n in sorted({n for p in pairs for n in p})}
                    minus = {k: val[k][0] - val[k][1] for k in {k for k, l in pairs if k != l}}
                    plus = {l: val[l][0] + val[l][1] for l in {l for k, l in pairs if k != l}}
                    for k, l in pairs:
                        new = [val[k][0] * val[l][0], val[k][1] * val[l][1]]
                        if k != l:
                            new.append(minus[k] * plus[l])
                        acc[k, l] = [x + y for x, y in zip(acc[k, l], new)] if r else new
                for k, l in pairs:
                    pair_ref[0, l, k] = acc[k, l][0] + acc[k, l][1]
                    pair_ref[1, l, k] = zero if k == l else acc[k, l][2] - (acc[k, l][0] - acc[k, l][1])
        for c, g_ref in ((0, gr_ref), (1, gi_ref)):
            for l in range(count + 1):
                for kt in range(KP // SUB):
                    ks = range(kt * SUB, kt * SUB + SUB)
                    if min(ks) > min(l, count - 1):
                        continue
                    parts = [pair_ref[c, l, k] if k <= min(l, count - 1) else zero for k in ks]
                    g_ref[l, h, pl.ds(kt * SUB, SUB), :] = merge_rows(parts)
        row = lax.broadcasted_iota(jnp.int32, (SUB, LANES), 0)
        for c, g_ref in ((0, gr_ref), (1, gi_ref)):
            for l in range(count):
                for kt in range(KP // SUB):
                    ks = list(range(kt * SUB, kt * SUB + SUB))
                    if max(ks) <= l:
                        continue
                    other = jnp.concatenate(
                        [g_ref[k, h, pl.ds(l, 1), :] if l < k < count else zero[0:1] for k in ks], axis=0
                    )
                    if c:
                        other = -other
                    if min(ks) <= l:
                        other = jnp.where(row + ks[0] <= l, g_ref[l, h, pl.ds(kt * SUB, SUB), :], other)
                    g_ref[l, h, pl.ds(kt * SUB, SUB), :] = other
        for c in range(2):
            tiles = []
            for k in range(KP):
                total = None
                if k <= count:
                    for r in range(0, rows, SUB):
                        v = load(k, r)[c]
                        total = v if total is None else total + v
                tiles.append(zero if total is None else total)
            for kt in range(KP // SUB):
                sum_ref[c, h, pl.ds(kt * SUB, SUB), :] = merge_rows(tiles[kt * SUB : kt * SUB + SUB])


def turns(gr_ref, gs_ref, gd_ref, g0, count):
    halves = gr_ref.shape[1]

    def product(b, g):
        acc = [None] * halves
        for l in range(count):
            for h in range(halves):
                br = jnp.broadcast_to(b[h][0][l : l + 1], (KP, LANES))
                bi = jnp.broadcast_to(b[h][1][l : l + 1], (KP, LANES))
                new = [gr_ref[l, h] * (br + bi), gs_ref[l, h] * bi, gd_ref[l, h] * br]
                acc[h] = new if l == 0 else [x + y for x, y in zip(acc[h], new)]
        return [(g[h][0] + (t - u), g[h][1] + (t + v)) for h, (t, u, v) in enumerate(acc)]

    def step(_, carry):
        b, g = carry
        t = product(b, g)
        return tuple((b[h][0] + t[h][0], b[h][1] + t[h][1]) for h in range(halves)), g

    g = tuple(g0)
    b = g
    b, g = lax.fori_loop(0, ITERS // 2 - 1, step, (b, g))
    b = tuple((x * SHRINK, y * SHRINK) for x, y in b)
    g = tuple((x * SHRINK, y * SHRINK) for x, y in g)
    b, g = lax.fori_loop(0, ITERS - ITERS // 2, step, (b, g))
    return b, g, product(b, g)


def solve(virtual, gr_ref, gs_ref, gd_ref, hr, hi, sums, stack, beta_ref, state_ref):
    halves = gr_ref.shape[1]
    count = gr_ref.shape[0]
    first = 1.0 / math.sqrt(stack)
    g0 = []
    for h in range(halves):
        zr, zi = sums[h]
        row = lax.broadcasted_iota(jnp.int32, (KP, LANES), 0)
        zr = jnp.where(row < count, zr, 0.0)
        zi = jnp.where(row < count, zi, 0.0)
        if virtual is not None:
            zr = zr + virtual[h][1][0]
            zi = zi + virtual[h][1][1]
        g0.append((zr * first, zi * -first))
    b, g, t = turns(gr_ref, gs_ref, gd_ref, g0, count)
    for h in range(halves):
        norm = colsum(b[h][0] * (g[h][0] + t[h][0]) + b[h][1] * (g[h][1] + t[h][1]))
        inv = lax.rsqrt(SHRINK * SHRINK + norm)
        br, bi = b[h][0] * inv, b[h][1] * inv
        a = inv * (SHRINK * first)
        xr, xi = hr[h], hi[h]
        sr, si = (x[count : count + 1] for x in sums[h])
        fr, fi = a, jnp.zeros_like(a)
        if virtual is not None:
            (wr, wi), (zr, zi) = virtual[h]
            xr, xi = xr + (zr * wr + zi * wi), xi + (zr * wi - zi * wr)
            sr, si = sr + wr, si + wi
            fr = a + colsum(zr * br - zi * bi)
            fi = colsum(zr * bi + zi * br)
        beta_ref[0, h] = br
        beta_ref[1, h] = bi
        fr, fi = unit(fr, fi)
        state_ref[0:1, half(h)] = a * sr + colsum(br * xr + bi * xi)
        state_ref[1:2, half(h)] = a * si + colsum(br * xi - bi * xr)
        state_ref[2:3, half(h)] = fr
        state_ref[3:4, half(h)] = fi
        state_ref[4:5, half(h)] = a
        state_ref[5:8, half(h)] = jnp.zeros((3, LANES), jnp.float32)


def own_kernel(idx_hbm, slc_hbm, near_ref, zr_ref, zi_ref, own_ref, idx_ref, slc_ref, hl_ref, sems):
    copies = [
        pltpu.make_async_copy(slc_hbm, slc_ref, sems.at[0]),
        pltpu.make_async_copy(idx_hbm, idx_ref, sems.at[1]),
    ]
    for copy in copies:
        copy.start()
    for copy in copies:
        copy.wait()
    _, _, _, start, near_at, _ = seat(slc_ref.shape[2], near_ref.shape[2])
    gather(start, idx_ref, ((slc_ref, 0), (near_ref, near_at)), own_ref, hl_ref, zr_ref, zi_ref, False)


def prepare_kernel(stack, first, idx_ref, far_ref, own_ref, *refs):
    refs = refs[2 if first else 7 :]
    zr_ref, zi_ref, gr_ref, gi_ref, sum_ref, beta_ref, state_ref = refs[:7]
    xs_ref, hl_ref, pair_ref = refs[-3:]

    section, _, _, start, _, far_at = seat(zr_ref.shape[2], far_ref.shape[2])

    final = lax.axis_size("section") - 1
    ends = jnp.logical_or(section == 0, section == final)

    @pl.when(ends if first else jnp.logical_not(ends))
    def _():
        gather(start, idx_ref, ((far_ref, far_at),), xs_ref, hl_ref, zr_ref, zi_ref, True)
        scale_dates(zr_ref, zi_ref)
        gram(pair_ref, zr_ref, zi_ref, own_ref, gr_ref, gi_ref, sum_ref)

    if first:
        count, halves = gr_ref.shape[0] - 1, gr_ref.shape[1]
        comp_ref, fold_ref, gs_ref, gd_ref = refs[7:11]

        @pl.when(section == final)
        def _():
            fold(gr_ref, gi_ref, sum_ref, fold_ref)

        @pl.when(section == 0)
        def _():
            hr = [gr_ref[count, h] for h in range(halves)]
            hi = [gi_ref[count, h] for h in range(halves)]
            sums = [(sum_ref[0, h], sum_ref[1, h]) for h in range(halves)]
            for l in range(count):
                for h in range(halves):
                    gs_ref[l, h] = gi_ref[l, h] + gr_ref[l, h]
                    gd_ref[l, h] = gi_ref[l, h] - gr_ref[l, h]
            solve(None, gr_ref.at[0:count], gs_ref, gd_ref, hr, hi, sums, stack, beta_ref, state_ref)
            comp_ref[...] = state_ref[0:2]


def folded_column(l, h, gr_ref, gi_ref, sum_ref):
    count = gr_ref.shape[0] - 1
    if l >= count:
        return sum_ref[l - count, h]
    k_row = lax.broadcasted_iota(jnp.int32, (KP, LANES), 0)
    return jnp.where(k_row <= l, gr_ref[l, h], gi_ref[l, h])


def fold(gr_ref, gi_ref, sum_ref, fold_ref):
    halves = gr_ref.shape[1]
    for l in range(gr_ref.shape[0] + 1):
        for h in range(halves):
            fold_ref[pl.ds((l * halves + h) * KP, KP), :] = folded_column(l, h, gr_ref, gi_ref, sum_ref)


def make_tile(start, pixel_ref, idx_ref, zr_ref, zi_ref, gr_ref, gi_ref, sum_ref):
    count, rows, pixels = zr_ref.shape
    halves = pixels // LANES
    lane = lax.broadcasted_iota(jnp.int32, (KP, LANES), 1)
    local = pixel_ref[...] - start
    hit = [lax.broadcasted_iota(jnp.int32, (SUB, LANES), 1) == local - h * LANES for h in range(halves)]

    def column(parts):
        total = None
        for h, part in enumerate(parts):
            mask = jnp.concatenate([hit[h]] * (part.shape[0] // SUB), axis=0)
            part = jnp.where(mask, part, 0.0)
            total = part if total is None else total + part
        return jnp.broadcast_to(jnp.sum(total, axis=1, keepdims=True), total.shape)

    tile = jnp.zeros((KP, LANES), jnp.float32)
    for l in range(count + 2):
        parts = [folded_column(l, h, gr_ref, gi_ref, sum_ref) for h in range(halves)]
        tile = jnp.where(lane == (l if l < count else KP + l - count), column(parts), tile)
    pad = jnp.zeros((KP - count, LANES), jnp.float32)
    near = [jnp.concatenate([idx_ref[:, half(h)].astype(jnp.float32), pad], axis=0) for h in range(halves)]
    tile = jnp.where(lane == KP + 2, column(near), tile)
    wide = lax.broadcasted_iota(jnp.int32, (rows, LANES), 1)
    empty = jnp.zeros((LANES - rows, LANES), jnp.float32)
    for c, ref in ((0, zr_ref), (1, zi_ref)):
        both = jnp.zeros((rows, LANES), jnp.float32)
        for k in range(count):
            both = jnp.where(wide == k, column([ref[k, :, half(h)] for h in range(halves)]), both)
        turned = jnp.transpose(jnp.concatenate([both, empty], axis=0))[0:KP]
        at = Z_LANE + c * Z_STEP
        tile = jnp.where(jnp.logical_and(lane >= at, lane < at + Z_STEP), pltpu.roll(turned, at, 1), tile)
    return tile


def lane_take(x, i):
    return jnp.take_along_axis(x, i, axis=1, mode="promise_in_bounds")


def scaled(own, zr, zi):
    scale = lax.rsqrt(jnp.maximum(colsum(zr * zr + zi * zi), 1.0))
    return own, (zr * scale, zi * scale)


def take_virtual(idx_ref, base, reach, tiles, halves, count):
    virtual = []
    for h in range(halves):
        parts = []
        for kt in range(KP // SUB):
            rows = min(SUB, count - kt * SUB)
            raw = idx_ref[pl.ds(kt * SUB, rows), half(h)] - base
            if rows < SUB:
                raw = jnp.concatenate([raw, jnp.full((SUB - rows, LANES), -1, jnp.int32)], axis=0)
            lane = jnp.bitwise_and(raw, LANES - 1)
            tile = jnp.right_shift(raw, 7)
            both = []
            for c in range(2):
                out = jnp.zeros((SUB, LANES), jnp.float32)
                for n in range(h, h + 2 * reach // LANES + 1):
                    got = lane_take(jnp.broadcast_to(tiles[n][c], (SUB, LANES)), lane)
                    out = jnp.where(tile == n, got, out)
                both.append(out)
            parts.append(both)
        zr = jnp.concatenate([p[0] for p in parts], axis=0)
        zi = jnp.concatenate([p[1] for p in parts], axis=0)
        virtual.append(scaled(tiles[reach // LANES + h], zr, zi))
    return virtual


def update(virtual, gram_of, fr_ref, fs_ref, fd_ref):
    for h, (_, (zr, zi)) in enumerate(virtual):
        for l in range(fr_ref.shape[0]):
            gr, gi = gram_of(l, h)
            br = jnp.broadcast_to(zr[l : l + 1], (KP, LANES))
            bi = jnp.broadcast_to(zi[l : l + 1], (KP, LANES))
            gr = gr + (zr * br + zi * bi)
            gi = gi + (zr * bi - zi * br)
            fr_ref[l, h] = gr
            fs_ref[l, h] = gi + gr
            fd_ref[l, h] = gi - gr


def round_kernel(
    rnd, stack, idx_ref, low_ref, own_ref, high_ref,
    gr_ref, gi_ref, sum_ref, beta0_ref, state0_ref, *refs,
):
    last = len(refs) > 6
    if last:
        late, (comp_ref, *made), refs = refs[:5], refs[5:8], refs[8:]
        fr_ref, fs_ref, fd_ref, beta_ref, state_ref = refs
    else:
        beta_ref, state_ref, comp_ref, fr_ref, fs_ref, fd_ref = refs
    count = gr_ref.shape[0] - 1
    halves = gr_ref.shape[1]
    reach = low_ref.shape[1]
    beta_ref[...] = beta0_ref[...]
    state_ref[...] = state0_ref[...]
    section, _, _, start, _, _ = seat(own_ref.shape[1], reach)

    @pl.when(section == rnd)
    def _():
        tiles = []
        for ref in (low_ref, own_ref, high_ref):
            for t in range(ref.shape[1] // LANES):
                tiles.append([ref[c : c + 1, half(t)] for c in range(2)])
        virtual = take_virtual(idx_ref, start - reach, reach, tiles, halves, count)
        update(virtual, lambda l, h: (gr_ref[l, h], gi_ref[l, h]), fr_ref, fs_ref, fd_ref)
        hr = [gr_ref[count, h] for h in range(halves)]
        hi = [gi_ref[count, h] for h in range(halves)]
        sums = [(sum_ref[0, h], sum_ref[1, h]) for h in range(halves)]
        solve(virtual, fr_ref, fs_ref, fd_ref, hr, hi, sums, stack, beta_ref, state_ref)

    comp_ref[...] = state_ref[0:2]
    if last:
        vectors(*late, beta_ref, state_ref, *made)


def slot_rows(halves):
    return max(up(4 * halves, SUB), KP // 2)


def tile_kernel(pixel_ref, idx_ref, zr_ref, zi_ref, gr_ref, gi_ref, sum_ref, tile_ref):
    section, _, _, start, _, _ = seat(zr_ref.shape[2], 0)
    final = lax.axis_size("section") - 1

    @pl.when(section == final)
    def _():
        tile_ref[...] = make_tile(start, pixel_ref, idx_ref, zr_ref, zi_ref, gr_ref, gi_ref, sum_ref)

    @pl.when(section != final)
    def _():
        tile_ref[...] = jnp.zeros_like(tile_ref)


def make_vectors(zr_ref, zi_ref, beta_ref, state_ref, vec_ref):
    count, rows, pixels = zr_ref.shape
    dates = vec_ref.shape[1]
    out = [[], []]
    for h in range(pixels // LANES):
        a = state_ref[4:5, half(h)]
        acc_r = [jnp.broadcast_to(a, (SUB, LANES)) for _ in range(0, rows, SUB)]
        acc_i = [jnp.zeros((SUB, LANES), jnp.float32) for _ in range(0, rows, SUB)]
        for k in range(count):
            br = jnp.broadcast_to(beta_ref[0, h, k : k + 1, :], (SUB, LANES))
            bi = jnp.broadcast_to(beta_ref[1, h, k : k + 1, :], (SUB, LANES))
            for n, r in enumerate(range(0, rows, SUB)):
                zr = zr_ref[k, pl.ds(r, SUB), half(h)]
                zi = zi_ref[k, pl.ds(r, SUB), half(h)]
                acc_r[n] = acc_r[n] + (zr * br - zi * bi)
                acc_i[n] = acc_i[n] + (zr * bi + zi * br)
        for c, acc in ((0, acc_r), (1, acc_i)):
            whole = jnp.concatenate(acc, axis=0)
            vec_ref[c, :, half(h)] = whole[0:dates]
            out[c].append(whole)
    return out


def vectors(pixel_ref, zr_ref, zi_ref, tile_ref, other_ref, beta_ref, state_ref, vec_ref, slot_ref):
    _, rows, pixels = zr_ref.shape
    halves = pixels // LANES
    section, block, blocks, start, _, _ = seat(pixels, 0)

    @pl.when(section < lax.axis_size("section") - 1)
    def _():
        local = pixel_ref[...] - start
        lane = lax.broadcasted_iota(jnp.int32, (SUB, LANES), 1)
        row = lax.broadcasted_iota(jnp.int32, (SUB, LANES), 0)
        at_pixel = [jnp.zeros((SUB, LANES), jnp.float32) for _ in range(2)]
        vecs = make_vectors(zr_ref, zi_ref, beta_ref, state_ref, vec_ref)
        for c in range(2):
            for h in range(halves):
                empty = jnp.zeros((LANES - rows, LANES), jnp.float32)
                turned = jnp.transpose(jnp.concatenate([vecs[c][h], empty], axis=0))
                for r in range(0, LANES, SUB):
                    at_pixel[c] = at_pixel[c] + jnp.where(row == local - (h * LANES + r), turned[r : r + SUB], 0.0)
        virtual, f_rows = (
            [state_ref[c : c + 1, half(h)] for c in cs for h in range(halves)] for cs in ((0, 1), (2, 3))
        )
        mixed = colsum(at_pixel[0]) + pltpu.roll(jnp.broadcast_to(colsum(at_pixel[1]), (SUB, LANES)), LANES // 2, 1)[0:1]
        for c in range(2):
            picked = jnp.zeros((1, LANES), jnp.float32)
            for h in range(halves):
                picked = picked + jnp.where((lane == local - h * LANES)[0:1], state_ref[2 + c : 3 + c, half(h)], 0.0)
            f = jnp.sum(picked, axis=1, keepdims=True)
            mixed = jnp.where(lane[0:1] == LANES - 2 + c, jnp.broadcast_to(f, (1, LANES)), mixed)
        spare = slot_ref.shape[1] - 2 * halves
        kinds = []
        for more in (f_rows, [mixed]):
            empty = [jnp.zeros((1, LANES), jnp.float32)] * (spare - len(more))
            kinds.append(jnp.concatenate(virtual + more + empty, axis=0))
        for n in range(slot_ref.shape[0]):
            with_f = jnp.logical_and(block == n % blocks, n // blocks < section)
            slot_ref[n] = jnp.where(with_f, *kinds)

    @pl.when(section == lax.axis_size("section") - 1)
    def _():
        tile = tile_ref[...] + other_ref[...]
        tile = jnp.where(block % 2 == 0, tile[0 : KP // 2], tile[KP // 2 :])
        for n in range(slot_ref.shape[0]):
            slot_ref[n, 0 : KP // 2] = tile


def unfold(fold, l, h, k_row, count):
    straight, turned = fold[0](l, h), jnp.where(k_row < count, fold[1](l, h), 0.0)
    return (
        jnp.where(k_row <= l, straight, turned),
        jnp.where(k_row > l, straight, jnp.where(k_row < l, -turned, 0.0)),
    )


def finish_kernel(
    sections, stack, pixel_ref, idx_ref, got_ref, vec0_ref, comp0_ref, zr_ref, zi_ref, gr_ref, gi_ref, sum_ref, *refs
):
    folds, (out_ref, small_ref), refs = refs[:sections], refs[sections : sections + 2], refs[sections + 2 :]
    fold_ref, fr_ref, fs_ref, fd_ref, beta_ref, state_ref, vec_ref = refs
    dates, pixels = vec_ref.shape[1:]
    count = zr_ref.shape[0]
    section, mine, blocks, start, _, _ = seat(pixels, 0)
    halves = pixels // LANES
    final = sections - 1
    reach = min(pixels, REACH_LIMIT)

    for s in range(sections):

        @pl.when(section == s)
        def _(s=s):
            fold_ref[...] = folds[s][...]

    tile = [got_ref[final * blocks + q, 0 : KP // 2] for q in range(2)]
    for q in range(2, blocks):
        tile[q % 2] = tile[q % 2] + got_ref[final * blocks + q, 0 : KP // 2]
    tile = jnp.concatenate(tile, axis=0)
    k_row = lax.broadcasted_iota(jnp.int32, (KP, LANES), 0)
    lane = lax.broadcasted_iota(jnp.int32, (KP, LANES), 1)
    turned = jnp.transpose(jnp.concatenate([tile, jnp.zeros((LANES - KP, LANES), jnp.float32)], axis=0))[0:KP]
    real = jnp.where(k_row <= lane, tile, turned)
    imag = jnp.where(k_row > lane, tile, jnp.where(k_row < lane, -turned, 0.0))

    def spread(x, l):
        return jnp.broadcast_to(x[:, l : l + 1], (KP, LANES))

    per_l = halves * KP

    def fold_of(l, h):
        return fold_ref[pl.ds(l * per_l + h * KP, KP), :]

    def fold_turned(l, h):
        return jnp.concatenate(
            [fold_ref[pl.ds(k0 * per_l + h * KP + l, SUB, stride=per_l), :] for k0 in range(0, KP, SUB)], axis=0
        )

    def gram_of(l, h):
        if h == halves:
            return spread(real, l), spread(imag, l)
        return unfold((fold_of, fold_turned), l, h, k_row, count)

    sums = [(fold_of(count, h), fold_of(count + 1, h)) for h in range(halves)]
    sums.append((spread(tile, KP), spread(tile, KP + 1)))

    before = final - 1
    tiles = []
    per = reach // LANES
    low, high = jnp.maximum(mine - 1, 0), jnp.minimum(mine + 1, blocks - 1)
    for at, which in ((low, range(halves - per, halves)), (mine, range(halves)), (high, range(per))):
        for h in which:
            tiles.append([got_ref[before * blocks + at, c * halves + h : c * halves + h + 1] for c in range(2)])
    virtual = take_virtual(idx_ref, start - reach, reach, tiles, halves, count)
    near = spread(tile, KP + 2).astype(jnp.int32)
    total = [jnp.zeros((KP, LANES), jnp.float32) for _ in range(2)]
    for q in range(blocks):
        for h in range(halves):
            hit = lane == near - (q * pixels + h * LANES)
            for c in range(2):
                row = got_ref[before * blocks + q, c * halves + h : c * halves + h + 1]
                total[c] = total[c] + jnp.where(hit, row, 0.0)
    total = [jnp.broadcast_to(jnp.sum(x, axis=1, keepdims=True), (KP, LANES)) for x in total]
    total = [jnp.where(k_row < count, x, 0.0) for x in total]
    virtual.append(scaled([x[0:1] for x in total], *total))
    update(virtual, gram_of, fr_ref, fs_ref, fd_ref)

    zero = jnp.zeros((KP, LANES), jnp.float32)
    hr = [gr_ref[count, h] for h in range(halves)] + [zero]
    hi = [gi_ref[count, h] for h in range(halves)] + [zero]
    solve(virtual, fr_ref, fs_ref, fd_ref, hr, hi, sums, stack, beta_ref, state_ref)
    is_final = section == final
    for c in range(2):
        small_ref[c] = jnp.where(is_final, state_ref[c : c + 1, 0:pixels], comp0_ref[c : c + 1])

    def of_pixel(s, later):
        total = jnp.zeros((1, LANES), jnp.float32)
        for q in range(blocks):
            first = pixel_ref[0:1] - q * pixels
            here = jnp.logical_and(first >= 0, first < pixels)
            here = jnp.logical_and(here, jnp.logical_not(jnp.logical_and(later, mine == q)))
            total = total + jnp.where(here, got_ref[s * blocks + q, 2 * halves : 2 * halves + 1], 0.0)
        return total

    def times(d, later, fr, fi):
        fr = jnp.where(later, fr, 1.0)
        fi = jnp.where(later, fi, 0.0)
        return (d[0] * fr - d[1] * fi, d[0] * fi + d[1] * fr)

    one = jnp.ones((1, LANES), jnp.float32)
    datum = [(one, 0.0 * one) for _ in range(halves + 1)]
    for h in range(halves + 1):
        datum[h] = times(datum[h], section < final, state_ref[2:3, half(h)], state_ref[3:4, half(h)])
    for s in range(final - 1, 0, -1):
        later = section < s
        own = [got_ref[s * blocks + mine, 2 * halves + m : 2 * halves + m + 1] for m in range(2 * halves)]
        row = of_pixel(s, later)
        for h in range(halves):
            datum[h] = times(datum[h], later, own[h], own[halves + h])
        f = []
        for c in range(2):
            total = jnp.where(lane[0:1] == LANES - 2 + c, row, 0.0)
            for h in range(halves):
                total = total + jnp.where(lane[0:1] == pixel_ref[0:1] - start - h * LANES, own[c * halves + h], 0.0)
            f.append(jnp.sum(total, axis=1, keepdims=True))
        datum[halves] = times(datum[halves], later, *[jnp.broadcast_to(x, (1, LANES)) for x in f])

    zr = pltpu.roll(tile, LANES - Z_LANE, 1)
    zi = pltpu.roll(tile, LANES - Z_LANE - Z_STEP, 1)
    br, bi = beta_ref[0, halves], beta_ref[1, halves]
    zr, zi = jnp.where(k_row < count, zr, 0.0), jnp.where(k_row < count, zi, 0.0)
    last_r = state_ref[4:5, half(halves)] + colsum(zr * br - zi * bi)
    last_i = colsum(zr * bi + zi * br)
    row = of_pixel(jnp.minimum(section, final - 1), False)
    vr = jnp.where(is_final, last_r, row)
    vi = jnp.where(is_final, last_i, pltpu.roll(jnp.broadcast_to(row, (SUB, LANES)), LANES // 2, 1)[0:1])
    dr, di = datum[halves]
    ur, ui = unit(vr * dr - vi * di, vr * di + vi * dr)
    gain = math.sqrt(dates + 1)
    ur = jnp.transpose(jnp.broadcast_to(ur * gain, (LANES, LANES)))[0:dates]
    ui = jnp.transpose(jnp.broadcast_to(ui * gain, (LANES, LANES)))[0:dates]

    @pl.when(is_final)
    def _():
        make_vectors(zr_ref, zi_ref, beta_ref, state_ref, vec_ref)

    for h in range(halves):
        wr = ur * datum[h][0] + ui * datum[h][1]
        wi = ur * datum[h][1] - ui * datum[h][0]
        vr = jnp.where(is_final, vec_ref[0, :, half(h)], vec0_ref[0, :, half(h)])
        vi = jnp.where(is_final, vec_ref[1, :, half(h)], vec0_ref[1, :, half(h)])
        out_ref[:, 0, half(h)] = vr * wr - vi * wi
        out_ref[:, 1, half(h)] = vr * wi + vi * wr


def on_device(slc, neighbours, reference_pixel):
    dates, pixels = slc.shape[1:]
    slc = jnp.transpose(slc, (1, 0, 2))
    count = neighbours.shape[0]
    reach = min(pixels, REACH_LIMIT)
    sections = lax.axis_size("section")
    blocks = lax.axis_size("pix")
    block = lax.axis_index("pix")
    stack = dates + 1
    halves = pixels // LANES
    rows = up(dates, SUB)

    even = block % 2 == 0

    def swap(first, upper):
        pairs = [(i, i + 1) for i in range(first, blocks - 1, 2)]
        pairs += [(j, i) for i, j in pairs]
        sent = slc
        if reach < pixels:
            sent = jnp.where(upper, slc[:, :, pixels - reach :], slc[:, :, :reach])
        return lax.ppermute(sent, "pix", pairs)

    near = swap(0, even)
    far = swap(1, ~even)

    made = [
        f32(count, rows, pixels), f32(count, rows, pixels),
        f32(count + 1, halves, KP, LANES), f32(count + 1, halves, KP, LANES),
        f32(2, halves, KP, LANES), f32(2, halves, KP, LANES), f32(SUB, pixels), f32(2, pixels),
    ]
    zr, zi, own, neighbours = pl.pallas_call(
        own_kernel,
        out_shape=made[:2]
        + [f32(2 * rows, pixels + reach)]
        + [jax.ShapeDtypeStruct(neighbours.shape, jnp.int32)],
        in_specs=[HBM, HBM, VMEM],
        out_specs=[VMEM] * 4,
        scratch_shapes=[
            pltpu.VMEM((dates, 2, pixels), jnp.float32),
            pltpu.VMEM((4 * rows, pixels + reach), jnp.bfloat16),
            pltpu.SemaphoreType.DMA((2,)),
        ],
        compiler_params=params(),
        cost_estimate=cost(2 * 4 * rows * pixels * (pixels + reach) * count),
        name="own",
    )(*[pltpu.with_memory_space_constraint(x, pltpu.HBM) for x in (neighbours, slc)], near)

    def prepare(first, carried):
        outs = made + [f32((count + 2) * halves * KP, LANES)] if first else made[:7]
        return pl.pallas_call(
            functools.partial(prepare_kernel, stack, first),
            out_shape=outs,
            in_specs=[VMEM] * (3 + len(carried)),
            out_specs=[VMEM] * len(outs),
            scratch_shapes=([pltpu.VMEM((count, halves, KP, LANES), jnp.float32)] * 2 if first else [])
            + [
                pltpu.VMEM((2 * rows, reach), jnp.float32),
                pltpu.VMEM((4 * rows, reach), jnp.bfloat16),
                pltpu.VMEM((2, count + 1, count, SUB, LANES), jnp.float32),
            ],
            input_output_aliases={3 + n: n for n in range(len(carried))},
            compiler_params=params(),
            cost_estimate=cost(50 * 12 * rows * reach * pixels * count),
        )(neighbours, far, own, *carried)

    *made_0, comp, folded = prepare(True, (zr, zi))
    zr, zi, gr, gi, sums, beta, state = prepare(False, made_0)

    final = sections - 1
    folds = []
    for s in range(final):
        pairs = [(final * blocks + q, s * blocks + q) for q in range(blocks)]
        folds.append(lax.ppermute(folded, ("section", "pix"), pairs))
    folds.append(folded)

    for rnd in range(1, final):
        def hop(shift):
            pairs = [
                ((rnd - 1) * blocks + q, rnd * blocks + q + shift)
                for q in range(blocks)
                if 0 <= q + shift < blocks
            ]
            return lax.ppermute(comp, ("section", "pix"), pairs)

        last = rnd == final - 1
        late = (pixel, zr, zi, tile, other) if last else ()
        scratch = [pltpu.VMEM((count, halves, KP, LANES), jnp.float32)] * 3
        outs = [f32(2, halves, KP, LANES), f32(SUB, pixels), f32(2, pixels)]
        if last:
            scratch += [pltpu.VMEM(o.shape, o.dtype) for o in outs[:2]]
            outs = outs[2:] + [f32(2, dates, pixels), f32(sections * blocks, slot_rows(halves), LANES)]
        call = pl.pallas_call(
            functools.partial(round_kernel, rnd, stack),
            out_shape=outs,
            in_specs=[VMEM] * (9 + len(late)),
            out_specs=[VMEM] * 3,
            scratch_shapes=scratch,
            compiler_params=params(),
        )
        near = (hop(1)[:, pixels - reach :], hop(0), hop(-1)[:, :reach])
        made = call(neighbours, *near, gr, gi, sums, beta, state, *late)
        if last:
            comp, vec, sent = made
        else:
            beta, state, comp = made
        if rnd == 1:
            pixel = lax.optimization_barrier((reference_pixel, comp))[0][0]
            pixel = jnp.full((SUB, LANES), pixel, jnp.int32)
            tile = pl.pallas_call(
                tile_kernel,
                out_shape=f32(KP, LANES),
                in_specs=[VMEM] * 7,
                out_specs=VMEM,
                compiler_params=params(),
                name="tile",
            )(pixel, neighbours, zr, zi, gr, gi, sums)
            pairs = [(final * blocks + q, final * blocks + (q ^ 1)) for q in range(blocks)]
            other = lax.ppermute(tile, ("section", "pix"), pairs)

    sent, *folds = lax.optimization_barrier((sent, *folds))
    got = lax.all_to_all(sent, ("section", "pix"), 0, 0, tiled=True)
    out, small = pl.pallas_call(
        functools.partial(finish_kernel, sections, stack),
        out_shape=[f32(dates, 2, pixels), f32(2, 1, pixels)],
        in_specs=[VMEM] * (10 + sections),
        out_specs=[VMEM] * 2,
        scratch_shapes=[
            pltpu.VMEM(folded.shape, jnp.float32),
            pltpu.VMEM((count, halves + 1, KP, LANES), jnp.float32),
            pltpu.VMEM((count, halves + 1, KP, LANES), jnp.float32),
            pltpu.VMEM((count, halves + 1, KP, LANES), jnp.float32),
            pltpu.VMEM((2, halves + 1, KP, LANES), jnp.float32),
            pltpu.VMEM((SUB, pixels + LANES), jnp.float32),
            pltpu.VMEM((2, dates, pixels), jnp.float32),
        ],
        compiler_params=params(),
        name="finish",
    )(pixel, neighbours, got, vec, comp, zr, zi, gr, gi, sums, *folds)
    return (jnp.transpose(out, (1, 0, 2)), small)


def solution(mesh):
    return jax.shard_map(
        on_device,
        mesh=mesh,
        in_specs=(P(None, "section", "pix"), P(None, "pix"), P()),
        out_specs=(P(None, "section", "pix"), P(None, "section", "pix")),
        check_vma=False,
    )
```
